16 devices in a mesh: replica: 2 (over y, z), stage: 8 (over x, core).
Axes of the slice: x: 4, y: 2, z: 1, core: 2. Of those that a mesh axis runs over, the one named last changes fastest.
The devices are a block of a 4x4x8 slice.
Arguments:
- x_dec: bfloat16 [8, 32, 896], P('replica'), parts along dimension 0
- x_pre: bfloat16 [8, 32, 896], P('replica'), parts along dimension 0
- dec_len: int32 [8, 32], P('replica'), parts along dimension 0
- pre_len: int32 [2], P('replica'), parts along dimension 0
- g_attn: bfloat16 [8, 896], P('stage')
- w_q: bfloat16 [8, 896, 896], P('stage')
- w_k: bfloat16 [8, 896, 128], P('stage')
- w_v: bfloat16 [8, 896, 128], P('stage')
- w_o: bfloat16 [8, 896, 896], P('stage')
- g_mlp: bfloat16 [8, 896], P('stage')
- w_gate: bfloat16 [8, 896, 4864], P('stage')
- w_up: bfloat16 [8, 896, 4864], P('stage')
- w_down: bfloat16 [8, 4864, 896], P('stage')
- g_final: bfloat16 [896], replicated
- w_head: bfloat16 [896, 8192], replicated
- k_dec: bfloat16 [8, 8, 32, 256, 2, 64], P('stage', 'replica'), parts along dimension 1
- v_dec: bfloat16 [8, 8, 32, 256, 2, 64], P('stage', 'replica'), parts along dimension 1
- k_pre: bfloat16 [8, 512, 2, 64], P('stage', 'replica'), parts along dimension 1
- v_pre: bfloat16 [8, 512, 2, 64], P('stage', 'replica'), parts along dimension 1
Outputs:
- output 1: float32 [8, 33, 8192], P('replica'), parts along dimension 0
- output 2: bfloat16 [8, 8, 32, 256, 2, 64], P('stage', 'replica'), parts along dimension 1
- output 3: bfloat16 [8, 8, 32, 256, 2, 64], P('stage', 'replica'), parts along dimension 1
- output 4: bfloat16 [8, 512, 2, 64], P('stage', 'replica'), parts along dimension 1
- output 5: bfloat16 [8, 512, 2, 64], P('stage', 'replica'), parts along dimension 1
There are 2 independent parts. The reference program is written for one: setup_inputs(seed, part) draws one part's arguments, and reference() takes and returns one part's arrays. A program takes and returns all parts, laid end to end along the dimension named above; an argument that names none is the same for every part.
All inputs are finite; a program needn't handle non-finite values.
Results may differ from the reference program's by a relative error of at most 0.02.
Values are sent between devices in bfloat16 or wider.
A program may use at most 768 MiB of HBM per device.

```python
import jax
import jax.numpy as jnp
from jax import lax

HIDDEN = 896
Q_HEADS = 14
KV_COUNT = 2
HEAD_DIM = 64
FFN_DIM = 4864
N_LAYERS = 8
N_MICRO = 4
DEC_ROWS = 32
SEG_LEN = 32
CACHE_LEN = 256
VOCAB_SIZE = 8192
NORM_EPS = 1e-6
ROPE_BASE = 10000.0
GROUP_SIZE = Q_HEADS // KV_COUNT
PRE_SPAN = CACHE_LEN - N_MICRO * SEG_LEN


def draw_lengths(base_key):
    key_list = jax.random.split(base_key, 4)
    n_slots = N_MICRO * DEC_ROWS
    min_len = CACHE_LEN // 8
    flat_len = jax.random.randint(key_list[0], (n_slots,), min_len, CACHE_LEN)
    top_at = jax.random.randint(key_list[1], (), 0, n_slots)
    low_at = (top_at + 1 + jax.random.randint(key_list[2], (), 0, n_slots - 1)) % n_slots
    slot_ids = jnp.arange(n_slots)
    flat_len = jnp.where(slot_ids == top_at, CACHE_LEN - 1, flat_len)
    flat_len = jnp.where(slot_ids == low_at, min_len, flat_len)
    pre_len = jax.random.randint(key_list[3], (1,), PRE_SPAN // 4 + 1, PRE_SPAN + 1)
    return flat_len.reshape(N_MICRO, DEC_ROWS).astype(jnp.int32), pre_len.astype(jnp.int32)


def setup_inputs(seed: int = 0, part: int = 0) -> dict:
    base_key = jax.random.key(seed)
    shared_keys = jax.random.split(base_key, 11)
    own_keys = jax.random.split(jax.random.fold_in(base_key, part), 10)
    q_width = Q_HEADS * HEAD_DIM
    kv_width = KV_COUNT * HEAD_DIM

    def weight_of(rng_key, arr_shape, fan_in):
        return (jax.random.normal(rng_key, arr_shape, jnp.float32) * fan_in ** -0.5).astype(jnp.bfloat16)

    def gain_of(rng_key, arr_shape):
        return (1.0 + 0.3 * jax.random.normal(rng_key, arr_shape, jnp.float32)).astype(jnp.bfloat16)

    dec_len, pre_len = draw_lengths(own_keys[2])
    cache_shape = (N_LAYERS, N_MICRO, DEC_ROWS, CACHE_LEN, KV_COUNT, HEAD_DIM)
    mean_shape = (N_LAYERS, N_MICRO, DEC_ROWS, 1, KV_COUNT, HEAD_DIM)
    pre_shape = (N_LAYERS, CACHE_LEN, KV_COUNT, HEAD_DIM)
    return {
        'x_dec': jax.random.normal(own_keys[0], (N_MICRO, DEC_ROWS, HIDDEN), jnp.float32).astype(jnp.bfloat16),
        'x_pre': jax.random.normal(own_keys[1], (N_MICRO, SEG_LEN, HIDDEN), jnp.float32).astype(jnp.bfloat16),
        'dec_len': dec_len,
        'pre_len': pre_len,
        'g_attn': gain_of(shared_keys[0], (N_LAYERS, HIDDEN)),
        'w_q': weight_of(shared_keys[1], (N_LAYERS, HIDDEN, q_width), HIDDEN),
        'w_k': weight_of(shared_keys[2], (N_LAYERS, HIDDEN, kv_width), HIDDEN),
        'w_v': weight_of(shared_keys[3], (N_LAYERS, HIDDEN, kv_width), HIDDEN),
        'w_o': weight_of(shared_keys[4], (N_LAYERS, q_width, HIDDEN), q_width),
        'g_mlp': gain_of(shared_keys[5], (N_LAYERS, HIDDEN)),
        'w_gate': weight_of(shared_keys[6], (N_LAYERS, HIDDEN, FFN_DIM), HIDDEN),
        'w_up': weight_of(shared_keys[7], (N_LAYERS, HIDDEN, FFN_DIM), HIDDEN),
        'w_down': weight_of(shared_keys[8], (N_LAYERS, FFN_DIM, HIDDEN), FFN_DIM),
        'g_final': gain_of(shared_keys[9], (HIDDEN,)),
        'w_head': weight_of(shared_keys[10], (HIDDEN, VOCAB_SIZE), HIDDEN),
        'k_dec': jax.random.normal(own_keys[3], cache_shape, jnp.float32).astype(jnp.bfloat16),
        'v_dec': (jax.random.normal(own_keys[4], cache_shape, jnp.float32) + jax.random.normal(own_keys[5], mean_shape, jnp.float32)).astype(jnp.bfloat16),
        'k_pre': jax.random.normal(own_keys[6], pre_shape, jnp.float32).astype(jnp.bfloat16),
        'v_pre': (jax.random.normal(own_keys[7], pre_shape, jnp.float32) + jax.random.normal(own_keys[8], (N_LAYERS, 1, KV_COUNT, HEAD_DIM), jnp.float32)).astype(jnp.bfloat16),
    }


def rms_norm(acts, gain):
    acts_f = acts.astype(jnp.float32)
    inv_rms = lax.rsqrt(jnp.mean(acts_f * acts_f, axis=-1, keepdims=True) + NORM_EPS)
    return (acts_f * inv_rms * gain.astype(jnp.float32)).astype(jnp.bfloat16)


def rotate(proj, positions):
    half_dim = HEAD_DIM // 2
    inv_freq = ROPE_BASE ** (-jnp.arange(half_dim, dtype=jnp.float32) * (2.0 / HEAD_DIM))
    angles = positions.astype(jnp.float32)[:, None, None] * inv_freq
    cosine = jnp.cos(angles)
    sine_v = jnp.sin(angles)
    first_h = proj[..., :half_dim]
    second_h = proj[..., half_dim:]
    return jnp.concatenate([first_h * cosine - second_h * sine_v, second_h * cosine + first_h * sine_v], axis=-1)


def softmax_mix(scores, valid, values, form):
    masked = jnp.where(valid, scores, -1e30)
    probs = jax.nn.softmax(masked, axis=-1).astype(jnp.bfloat16)
    return jnp.einsum(form, probs.astype(jnp.float32), values.astype(jnp.float32)).astype(jnp.bfloat16)


def micro_block(acts, dec_pos, pre_begin, layer_w, kd_m, vd_m, k_cache, v_cache):
    g_att, wq_l, wk_l, wv_l, wo_l, g_ffn, wg_l, wu_l, wd_l = layer_w
    n_rows = DEC_ROWS + SEG_LEN
    pre_pos = pre_begin + jnp.arange(SEG_LEN)
    positions = jnp.concatenate([dec_pos, pre_pos])
    normed = rms_norm(acts, g_att)
    q_all = rotate(jnp.dot(normed, wq_l, preferred_element_type=jnp.float32).reshape(n_rows, Q_HEADS, HEAD_DIM), positions).astype(jnp.bfloat16)
    k_all = rotate(jnp.dot(normed, wk_l, preferred_element_type=jnp.float32).reshape(n_rows, KV_COUNT, HEAD_DIM), positions).astype(jnp.bfloat16)
    v_all = jnp.dot(normed, wv_l, preferred_element_type=jnp.float32).astype(jnp.bfloat16).reshape(n_rows, KV_COUNT, HEAD_DIM)
    row_ids = jnp.arange(DEC_ROWS)
    kd_m = kd_m.at[row_ids, dec_pos].set(k_all[:DEC_ROWS])
    vd_m = vd_m.at[row_ids, dec_pos].set(v_all[:DEC_ROWS])
    k_cache = lax.dynamic_update_slice(k_cache, k_all[DEC_ROWS:], (pre_begin, 0, 0))
    v_cache = lax.dynamic_update_slice(v_cache, v_all[DEC_ROWS:], (pre_begin, 0, 0))
    q_grp = q_all.reshape(n_rows, KV_COUNT, GROUP_SIZE, HEAD_DIM).astype(jnp.float32)
    att_scale = HEAD_DIM ** -0.5
    cache_pos = jnp.arange(CACHE_LEN)
    dec_scores = jnp.einsum('bkgd,bskd->bkgs', q_grp[:DEC_ROWS], kd_m.astype(jnp.float32)) * att_scale
    dec_valid = (cache_pos[None, :] <= dec_pos[:, None])[:, None, None, :]
    dec_out = softmax_mix(dec_scores, dec_valid, vd_m, 'bkgs,bskd->bkgd').reshape(DEC_ROWS, Q_HEADS * HEAD_DIM)
    pre_scores = jnp.einsum('ikgd,skd->ikgs', q_grp[DEC_ROWS:], k_cache.astype(jnp.float32)) * att_scale
    pre_valid = (cache_pos[None, :] <= pre_pos[:, None])[:, None, None, :]
    pre_out = softmax_mix(pre_scores, pre_valid, v_cache, 'ikgs,skd->ikgd').reshape(SEG_LEN, Q_HEADS * HEAD_DIM)
    attn_out = jnp.concatenate([dec_out, pre_out], axis=0)
    acts = (acts.astype(jnp.float32) + jnp.dot(attn_out, wo_l, preferred_element_type=jnp.float32)).astype(jnp.bfloat16)
    normed2 = rms_norm(acts, g_ffn)
    gate_f = jnp.dot(normed2, wg_l, preferred_element_type=jnp.float32)
    up_proj = jnp.dot(normed2, wu_l, preferred_element_type=jnp.float32)
    hidden_act = (jax.nn.silu(gate_f) * up_proj).astype(jnp.bfloat16)
    acts = (acts.astype(jnp.float32) + jnp.dot(hidden_act, wd_l, preferred_element_type=jnp.float32)).astype(jnp.bfloat16)
    return acts, kd_m, vd_m, k_cache, v_cache


def reference(x_dec, x_pre, dec_len, pre_len, g_attn, w_q, w_k, w_v, w_o, g_mlp, w_gate, w_up, w_down, g_final, w_head, k_dec, v_dec, k_pre, v_pre):
    acts_init = jnp.concatenate([x_dec, x_pre], axis=1)
    pre_starts = pre_len[0] + jnp.arange(N_MICRO) * SEG_LEN

    def layer_fn(acts_all, layer_in):
        layer_w = layer_in[:9]
        kd_l, vd_l, kp_l, vp_l = layer_in[9:]

        def micro_fn(pre_cache, micro_in):
            kp_c, vp_c = pre_cache
            acts_m, dec_pos, pre_begin, kd_m, vd_m = micro_in
            acts_m, kd_m, vd_m, kp_c, vp_c = micro_block(acts_m, dec_pos, pre_begin, layer_w, kd_m, vd_m, kp_c, vp_c)
            return (kp_c, vp_c), (acts_m, kd_m, vd_m)

        (kp_l, vp_l), (acts_all, kd_l, vd_l) = lax.scan(micro_fn, (kp_l, vp_l), (acts_all, dec_len, pre_starts, kd_l, vd_l))
        return acts_all, (kd_l, vd_l, kp_l, vp_l)

    acts_last, caches = lax.scan(layer_fn, acts_init, (g_attn, w_q, w_k, w_v, w_o, g_mlp, w_gate, w_up, w_down, k_dec, v_dec, k_pre, v_pre))
    kd_new, vd_new, kp_new, vp_new = caches
    kept = jnp.concatenate([acts_last[:, :DEC_ROWS], acts_last[:, -1:]], axis=1)
    final_h = rms_norm(kept, g_final)
    logits = jnp.dot(final_h.reshape(-1, HIDDEN), w_head, preferred_element_type=jnp.float32).reshape(N_MICRO, DEC_ROWS + 1, VOCAB_SIZE)
    return (logits, kd_new, vd_new, kp_new, vp_new)
```

```python
import functools

import jax
import jax.numpy as jnp
import numpy as np
from jax import lax
from jax.experimental import pallas as pl
from jax.experimental.pallas import tpu as pltpu
from jax.sharding import PartitionSpec as P

NORM_EPS = 1e-6
ROPE_BASE = 10000.0
F32 = jnp.float32
BF16 = jnp.bfloat16
NEG = -1e30
HBM = pl.ANY
VMEM = pltpu.VMEM
SMEM = pltpu.SMEM
MESH = pl.DeviceIdType.MESH


def rms_norm(acts, gain):
    acts_f = acts.astype(F32)
    inv_rms = lax.rsqrt(jnp.mean(acts_f * acts_f, axis=-1, keepdims=True) + NORM_EPS)
    return (acts_f * inv_rms * gain.astype(F32)).astype(BF16)


def dot(lhs, rhs):
    return jnp.dot(lhs, rhs, preferred_element_type=F32)


def dot_t(lhs, rhs):
    return lax.dot_general(lhs, rhs, (((1,), (1,)), ((), ())), preferred_element_type=F32)


def softmax(scores):
    expd = jnp.exp(scores - jnp.max(scores, axis=-1, keepdims=True))
    return expd * (1.0 / jnp.sum(expd, axis=-1, keepdims=True))


def pipeline_kernel(
    n_stages,
    dec_len, pre_len, inv_freq, g_attn, g_mlp, g_final,
    x_dec, x_pre, w_q, w_k, w_v, w_o, w_gate, w_up, w_down, k_dec, v_dec, k_pre, v_pre,
    fin_out, kn_out, vn_out, kp_out, vp_out,
    wqkv, wo, w1, w3, w2, kc, vc, kp, vp, xin, xout, fin, qd, od, kn, vn, cosv, sinv, hid,
    w_sem, kv_sem, p_sem, x_sem, o_sem, send_sem, recv_sem, fsend_sem, frecv_sem,
):
    n_micro, n_rows, hidden = xin.shape
    dec_rows = x_dec.shape[1]
    seg_len = x_pre.shape[1]
    kv_width, cache_len = kp.shape
    q_width = wo.shape[0]
    ffn = w1.shape[1]
    head_dim = 64
    kv_count = kv_width // head_dim
    q_heads = q_width // head_dim
    group = q_heads // kv_count
    stage = lax.axis_index('stage')
    last = n_stages - 1
    half = ffn // 2

    barrier = pltpu.get_barrier_semaphore()

    def x_copies(m):
        return (
            pltpu.make_async_copy(x_dec.at[m], xin.at[m, pl.ds(0, dec_rows)], x_sem.at[m, 0]),
            pltpu.make_async_copy(x_pre.at[m], xin.at[m, pl.ds(dec_rows, seg_len)], x_sem.at[m, 1]),
        )

    def kv_copies(m):
        return (
            pltpu.make_async_copy(k_dec.at[m], kc.at[m], kv_sem.at[m, 0]),
            pltpu.make_async_copy(v_dec.at[m], vc.at[m], kv_sem.at[m, 1]),
        )

    qkv_copies = (
        pltpu.make_async_copy(w_q, wqkv.at[:, pl.ds(0, q_width)], w_sem.at[0]),
        pltpu.make_async_copy(w_k, wqkv.at[:, pl.ds(q_width, kv_width)], w_sem.at[1]),
        pltpu.make_async_copy(w_v, wqkv.at[:, pl.ds(q_width + kv_width, kv_width)], w_sem.at[2]),
    )
    pre_copies = (
        pltpu.make_async_copy(k_pre, kp, p_sem.at[0]),
        pltpu.make_async_copy(v_pre, vp, p_sem.at[1]),
    )
    wo_copies = (pltpu.make_async_copy(w_o, wo, w_sem.at[3]),)
    up_copies = tuple(
        (
            pltpu.make_async_copy(w_gate.at[:, pl.ds(i * half, half)], w1.at[:, pl.ds(i * half, half)], w_sem.at[4 + 2 * i]),
            pltpu.make_async_copy(w_up.at[:, pl.ds(i * half, half)], w3.at[:, pl.ds(i * half, half)], w_sem.at[5 + 2 * i]),
        )
        for i in range(2)
    )
    down_copies = (pltpu.make_async_copy(w_down, w2, w_sem.at[8]),)

    @pl.when(stage == 0)
    def _():
        for copy in x_copies(0):
            copy.start()
    for copy in qkv_copies + pre_copies + kv_copies(0) + wo_copies + up_copies[0] + up_copies[1] + down_copies:
        copy.start()

    @pl.when(stage == 0)
    def _():
        for m in range(1, n_micro):
            for copy in x_copies(m):
                copy.start()
    for m in range(1, n_micro):
        for copy in kv_copies(m):
            copy.start()

    @pl.when(stage > 0)
    def _():
        pl.semaphore_signal(barrier, inc=1, device_id={'stage': stage - 1}, device_id_type=MESH)

    @pl.when(stage < last)
    def _():
        pl.semaphore_signal(barrier, inc=1, device_id={'stage': last}, device_id_type=MESH)

    lane = lax.broadcasted_iota(jnp.int32, (8, 128), 1)
    row8 = lax.broadcasted_iota(jnp.int32, (8, 128), 0)
    freq = inv_freq[...]
    sign = jnp.where((lane % head_dim) < head_dim // 2, -1.0, 1.0)

    def table_body(m, carry):
        for g in range(n_rows // 8):
            if g < dec_rows // 8:
                pos = jnp.zeros((8, 128), jnp.int32)
                for r in range(8):
                    pos = jnp.where(row8 == r, dec_len[m, g * 8 + r], pos)
            else:
                pos = pre_len[0] + m * seg_len + (g * 8 - dec_rows) + row8
            angle = pos.astype(F32) * freq
            cosv[m, pl.ds(g * 8, 8), :] = jnp.cos(angle)
            sinv[m, pl.ds(g * 8, 8), :] = jnp.sin(angle) * sign
        return carry

    lax.fori_loop(0, n_micro, table_body, 0)
    qd[...] = jnp.zeros(qd.shape, F32)

    @pl.when(stage < last)
    def _():
        pl.semaphore_wait(barrier, 1)

    @pl.when(stage == last)
    def _():
        pl.semaphore_wait(barrier, n_stages - 1)

    def x_send(m):
        return pltpu.make_async_remote_copy(
            src_ref=xout.at[m], dst_ref=xin.at[m], send_sem=send_sem.at[m], recv_sem=recv_sem.at[m],
            device_id={'stage': jnp.minimum(stage + 1, last)}, device_id_type=MESH)

    def fin_send(m, target):
        return pltpu.make_async_remote_copy(
            src_ref=fin.at[m], dst_ref=fin.at[m], send_sem=fsend_sem.at[m, target], recv_sem=frecv_sem.at[m],
            device_id={'stage': target}, device_id_type=MESH)

    def tick(m, carry):
        first = m == 0

        @pl.when(stage == 0)
        def _():
            for copy in x_copies(m):
                copy.wait()

        @pl.when(stage > 0)
        def _():
            x_send(m).wait_recv()

        @pl.when(first)
        def _():
            for copy in qkv_copies + pre_copies:
                copy.wait()

        acts = xin[m]
        normed = rms_norm(acts, g_attn[...])
        cosine = cosv[m]
        sine = sinv[m]
        lane_q = lax.broadcasted_iota(jnp.int32, (n_rows, 128), 1)
        low32 = (lane_q % head_dim) < head_dim // 2
        low_half = lax.broadcasted_iota(jnp.int32, (dec_rows, 128), 1) < head_dim

        def rotate(tile):
            swapped = jnp.where(low32, pltpu.roll(tile, 128 - head_dim // 2, 1), pltpu.roll(tile, head_dim // 2, 1))
            return tile * cosine + swapped * sine

        proj = dot(normed, wqkv[...])
        q_tiles = [rotate(proj[:, t * 128:(t + 1) * 128]).astype(BF16).astype(F32) for t in range(q_width // 128)]
        k_new = rotate(proj[:, q_width:q_width + kv_width]).astype(BF16)
        v_new = proj[:, q_width + kv_width:].astype(BF16)
        kn[...] = k_new[:dec_rows].astype(F32)
        vn[...] = v_new[:dec_rows].astype(F32)
        kn_out[m] = k_new[:dec_rows]
        vn_out[m] = v_new[:dec_rows]

        for j in range(q_heads):
            tile = q_tiles[j // 2][:dec_rows]
            if j % 2 != j // group:
                tile = pltpu.roll(tile, head_dim, 1)
            keep = low_half if j // group == 0 else jnp.logical_not(low_half)
            qd[pl.ds(j, dec_rows, stride=16), :] = jnp.where(keep, tile, 0.0)

        pre_begin = pre_len[0] + m * seg_len
        seg_row = lax.broadcasted_iota(jnp.int32, (seg_len, cache_len), 0)
        seg_col = lax.broadcasted_iota(jnp.int32, (seg_len, cache_len), 1)
        spread = (seg_col == seg_row + pre_begin).astype(F32).astype(BF16)
        col = lax.broadcasted_iota(jnp.int32, (kv_width, cache_len), 1)
        written = (col >= pre_begin) & (col < pre_begin + seg_len)
        contract0 = (((0,), (0,)), ((), ()))
        k_put = lax.dot_general(k_new[dec_rows:], spread, contract0, preferred_element_type=F32)
        v_put = lax.dot_general(v_new[dec_rows:], spread, contract0, preferred_element_type=F32)
        kp_f = jnp.where(written, k_put, kp[...].astype(F32)).astype(BF16)
        vp_f = jnp.where(written, v_put, vp[...].astype(F32)).astype(BF16)
        kp[...] = kp_f
        vp[...] = vp_f

        scale = head_dim ** -0.5
        pre_valid = seg_col <= seg_row + pre_begin
        valid_g = jnp.concatenate([pre_valid] * group, axis=0)
        pre_heads = []
        for g in range(kv_count):
            rows = []
            for j in range(g * group, (g + 1) * group):
                keep = low_half if j % 2 == 0 else jnp.logical_not(low_half)
                rows.append(jnp.where(keep, q_tiles[j // 2][dec_rows:], 0.0).astype(BF16))
            q_g = jnp.concatenate(rows, axis=0)
            k_g = kp_f[g * head_dim:(g + 1) * head_dim]
            v_g = vp_f[g * head_dim:(g + 1) * head_dim]
            scores = dot(q_g, jnp.concatenate([k_g, k_g], axis=0)) * scale
            probs = softmax(jnp.where(valid_g, scores, NEG)).astype(BF16)
            mixed = dot_t(probs, jnp.concatenate([v_g, v_g], axis=0))
            pre_heads += [mixed[i * seg_len:(i + 1) * seg_len] for i in range(group)]

        for copy in kv_copies(m):
            copy.wait()
        pos_lane = lax.broadcasted_iota(jnp.int32, (16, cache_len), 1)
        for b in range(dec_rows):
            pos = dec_len[m, b]
            q_b = qd[b * 16:(b + 1) * 16, :]
            s_old = dot(q_b.astype(BF16), kc[m, b]) * scale
            s_new = jnp.sum(q_b * kn[b:b + 1, :], axis=-1, keepdims=True) * scale
            here = pos_lane == pos
            scores = jnp.where(here, s_new, jnp.where(pos_lane < pos, s_old, NEG))
            peak = jnp.max(scores, axis=-1, keepdims=True)
            expd = jnp.exp(scores - peak)
            inv = 1.0 / jnp.sum(expd, axis=-1, keepdims=True)
            p_old = jnp.where(here, 0.0, expd * inv).astype(BF16)
            p_new = (jnp.exp(s_new - peak) * inv).astype(BF16).astype(F32)
            od[b * 16:(b + 1) * 16, :] = dot_t(p_old, vc[m, b]) + p_new * vn[b:b + 1, :]

        att_tiles = []
        for t in range(q_width // 128):
            parts = []
            for j in (2 * t, 2 * t + 1):
                part = od[pl.ds(j, dec_rows, stride=16), :]
                if j % 2 != j // group:
                    part = pltpu.roll(part, head_dim, 1)
                parts.append(part)
            dec_tile = jnp.where(low_half, parts[0], parts[1])
            pre_tile = jnp.where(low_half, pre_heads[2 * t], pre_heads[2 * t + 1])
            att_tiles.append(jnp.concatenate([dec_tile, pre_tile], axis=0).astype(BF16))
        att = jnp.concatenate(att_tiles, axis=1)

        @pl.when(first)
        def _():
            for copy in wo_copies:
                copy.wait()

        acts = (acts.astype(F32) + dot(att, wo[...])).astype(BF16)
        normed = rms_norm(acts, g_mlp[...])

        n_blk = 256
        for i in range(2):
            @pl.when(first)
            def _():
                for copy in up_copies[i]:
                    copy.wait()
            lo = 0 if i == 0 else half // n_blk * n_blk
            hi = half // n_blk * n_blk if i == 0 else ffn
            for n in range(lo, hi, n_blk):
                gate = dot(normed, w1[:, n:n + n_blk])
                up = dot(normed, w3[:, n:n + n_blk])
                hid[:, n:n + n_blk] = (jax.nn.silu(gate) * up).astype(BF16)

        @pl.when(first)
        def _():
            for copy in down_copies:
                copy.wait()
        acts = (acts.astype(F32) + dot(hid[...], w2[...])).astype(BF16)

        @pl.when(stage < last)
        def _():
            xout[m] = acts
            x_send(m).start()

        @pl.when(stage == last)
        def _():
            tail = jnp.concatenate([acts[:dec_rows], acts[n_rows - 8:]], axis=0)
            fin[m] = rms_norm(tail, g_final[...])
            for target in range(n_stages - 1):
                fin_send(m, target).start()
        return carry

    lax.fori_loop(0, n_micro, tick, 0)

    kp_copy = pltpu.make_async_copy(kp, kp_out, o_sem.at[0])
    vp_copy = pltpu.make_async_copy(vp, vp_out, o_sem.at[1])
    kp_copy.start()
    vp_copy.start()

    @pl.when(stage < last)
    def _():
        for m in range(n_micro):
            x_send(m).wait_send()
        for m in range(n_micro):
            fin_send(m, 0).wait_recv()

    @pl.when(stage == last)
    def _():
        for m in range(n_micro):
            for target in range(n_stages - 1):
                fin_send(m, target).wait_send()

    fin_copy = pltpu.make_async_copy(fin, fin_out, o_sem.at[2])
    fin_copy.start()
    kp_copy.wait()
    vp_copy.wait()
    fin_copy.wait()


def head_kernel(fin, w_head, logits, rows):
    n_micro = fin.shape[0]
    n_kept = logits.shape[0]

    @pl.when(pl.program_id(0) == 0)
    def _():
        for m in range(n_micro):
            kept = fin[m].astype(F32)
            for t in range(rows.shape[0]):
                tile = kept[:, t * 128:(t + 1) * 128]
                rows[t, pl.ds(m, n_kept - 1, stride=n_micro), :] = tile[:n_kept - 1]
                rows[t, (n_kept - 1) * n_micro + m:(n_kept - 1) * n_micro + m + 1, :] = tile[fin.shape[1] - 1:]

    lhs = jnp.concatenate([rows[t].astype(BF16) for t in range(rows.shape[0])], axis=1)
    out = dot(lhs, w_head[...])
    for i in range(n_kept):
        logits[i] = out[i * n_micro:(i + 1) * n_micro]


def cache_kernel(dec_len, kn, vn, k_in, v_in, k_out, v_out):
    n_seq, kv_width, cache_len = k_in.shape[1:]
    m = pl.program_id(0)
    first = pl.program_id(1) * n_seq
    col = lax.broadcasted_iota(jnp.int32, (kv_width, cache_len), 1)
    for new, old, out in ((kn, k_in, k_out), (vn, v_in, v_out)):
        cols = jnp.transpose(new[0].astype(F32))
        for b in range(n_seq):
            here = col == dec_len[m, first + b]
            out[0, b] = jnp.where(here, cols[:, b:b + 1], old[0, b].astype(F32)).astype(BF16)


def solution(mesh):
    n_stages = mesh.shape['stage']
    part_spec = P('replica')
    layer_spec = P('stage')
    cache_spec = P('stage', 'replica')
    in_specs = (part_spec,) * 4 + (layer_spec,) * 9 + (P(), P()) + (cache_spec,) * 4
    out_specs = (part_spec,) + (cache_spec,) * 4

    def device_fn(x_dec, x_pre, dec_len, pre_len, g_attn, w_q, w_k, w_v, w_o, g_mlp, w_gate, w_up, w_down, g_final, w_head, k_dec, v_dec, k_pre, v_pre):
        n_micro, dec_rows, hidden = x_dec.shape
        seg_len = x_pre.shape[1]
        n_rows = dec_rows + seg_len
        _, cache_len, kv_count, head_dim = k_pre.shape
        kv_width = kv_count * head_dim
        q_width = w_q.shape[2]
        ffn = w_gate.shape[2]
        vocab = w_head.shape[1]
        fin_rows = dec_rows + 8

        kd = jnp.transpose(k_dec[0], (0, 1, 3, 4, 2)).reshape(n_micro, dec_rows, kv_width, cache_len)
        vd = jnp.transpose(v_dec[0], (0, 1, 3, 4, 2)).reshape(n_micro, dec_rows, kv_width, cache_len)
        kpre = jnp.transpose(k_pre[0], (1, 2, 0)).reshape(kv_width, cache_len)
        vpre = jnp.transpose(v_pre[0], (1, 2, 0)).reshape(kv_width, cache_len)

        lanes = np.arange(128) % (head_dim // 2)
        inv_freq = jnp.asarray((ROPE_BASE ** (-lanes * (2.0 / head_dim))).astype(np.float32)[None, :])

        def spec(space):
            return pl.BlockSpec(memory_space=space)

        fin, kn, vn, kp, vp = pl.pallas_call(
            functools.partial(pipeline_kernel, n_stages),
            out_shape=(
                jax.ShapeDtypeStruct((n_micro, fin_rows, hidden), BF16),
                jax.ShapeDtypeStruct((n_micro, dec_rows, kv_width), BF16),
                jax.ShapeDtypeStruct((n_micro, dec_rows, kv_width), BF16),
                jax.ShapeDtypeStruct((kv_width, cache_len), BF16),
                jax.ShapeDtypeStruct((kv_width, cache_len), BF16),
            ),
            in_specs=[spec(SMEM)] * 2 + [spec(VMEM)] * 4 + [spec(HBM)] * 13,
            out_specs=(spec(HBM), spec(VMEM), spec(VMEM), spec(HBM), spec(HBM)),
            scratch_shapes=[
                VMEM((hidden, q_width + 2 * kv_width), BF16),
                VMEM((q_width, hidden), BF16),
                VMEM((hidden, ffn), BF16),
                VMEM((hidden, ffn), BF16),
                VMEM((ffn, hidden), BF16),
                VMEM((n_micro, dec_rows, kv_width, cache_len), BF16),
                VMEM((n_micro, dec_rows, kv_width, cache_len), BF16),
                VMEM((kv_width, cache_len), BF16),
                VMEM((kv_width, cache_len), BF16),
                VMEM((n_micro, n_rows, hidden), BF16),
                VMEM((n_micro, n_rows, hidden), BF16),
                VMEM((n_micro, fin_rows, hidden), BF16),
                VMEM((dec_rows * 16, 128), F32),
                VMEM((dec_rows * 16, 128), F32),
                VMEM((dec_rows, kv_width), F32),
                VMEM((dec_rows, kv_width), F32),
                VMEM((n_micro, n_rows, 128), F32),
                VMEM((n_micro, n_rows, 128), F32),
                VMEM((n_rows, ffn), BF16),
                pltpu.SemaphoreType.DMA((9,)),
                pltpu.SemaphoreType.DMA((n_micro, 2)),
                pltpu.SemaphoreType.DMA((2,)),
                pltpu.SemaphoreType.DMA((n_micro, 2)),
                pltpu.SemaphoreType.DMA((3,)),
                pltpu.SemaphoreType.DMA((n_micro,)),
                pltpu.SemaphoreType.DMA((n_micro,)),
                pltpu.SemaphoreType.DMA((n_micro, n_stages - 1)),
                pltpu.SemaphoreType.DMA((n_micro,)),
            ],
            compiler_params=pltpu.CompilerParams(collective_id=0, has_side_effects=True, vmem_limit_bytes=62 * 1024 * 1024),
            name='pipeline',
        )(dec_len, pre_len, inv_freq, g_attn, g_mlp, g_final.reshape(1, hidden),
          x_dec, x_pre, w_q[0], w_k[0], w_v[0], w_o[0], w_gate[0], w_up[0], w_down[0], kd, vd, kpre, vpre)

        v_blk = 1024
        logits = pl.pallas_call(
            head_kernel,
            grid=(vocab // v_blk,),
            out_shape=jax.ShapeDtypeStruct((dec_rows + 1, n_micro, vocab), F32),
            in_specs=[
                pl.BlockSpec((n_micro, fin_rows, hidden), lambda n: (0, 0, 0)),
                pl.BlockSpec((hidden, v_blk), lambda n: (0, n)),
            ],
            out_specs=pl.BlockSpec((dec_rows + 1, n_micro, v_blk), lambda n: (0, 0, n)),
            scratch_shapes=[VMEM((hidden // 128, (dec_rows + 1) * n_micro, 128), F32)],
            name='head',
        )(fin, w_head)

        n_seq = 8
        new_spec = pl.BlockSpec((1, n_seq, kv_width), lambda m, b: (m, b, 0))
        cache_blk = pl.BlockSpec((1, n_seq, kv_width, cache_len), lambda m, b: (m, b, 0, 0))
        kd_out, vd_out = pl.pallas_call(
            cache_kernel,
            grid=(n_micro, dec_rows // n_seq),
            out_shape=(jax.ShapeDtypeStruct(kd.shape, BF16),) * 2,
            in_specs=[spec(SMEM), new_spec, new_spec, cache_blk, cache_blk],
            out_specs=(cache_blk, cache_blk),
            name='cache',
        )(dec_len, kn, vn, kd, vd)

        def dec_cache(arr):
            return jnp.transpose(arr.reshape(n_micro, dec_rows, kv_count, head_dim, cache_len), (0, 1, 4, 2, 3))[None]

        def pre_cache(arr):
            return jnp.transpose(arr.reshape(kv_count, head_dim, cache_len), (2, 0, 1))[None]

        return jnp.transpose(logits, (1, 0, 2)), dec_cache(kd_out), dec_cache(vd_out), pre_cache(kp), pre_cache(vp)

    return jax.shard_map(device_fn, mesh=mesh, in_specs=in_specs, out_specs=out_specs, check_vma=False)
```

```python
import functools

import jax
import jax.numpy as jnp
import numpy as np
from jax import lax
from jax.experimental import pallas as pl
from jax.experimental.pallas import tpu as pltpu
from jax.sharding import PartitionSpec as P

NORM_EPS = 1e-6
ROPE_BASE = 10000.0
F32 = jnp.float32
BF16 = jnp.bfloat16
NEG = -1e30
HBM = pl.ANY
VMEM = pltpu.VMEM
SMEM = pltpu.SMEM
MESH = pl.DeviceIdType.MESH
JOIN = 2


def rms_norm(acts, gain):
    acts_f = acts.astype(F32)
    inv_rms = lax.rsqrt(jnp.mean(acts_f * acts_f, axis=-1, keepdims=True) + NORM_EPS)
    return (acts_f * inv_rms * gain.astype(F32)).astype(BF16)


def dot(lhs, rhs):
    return jnp.dot(lhs, rhs, preferred_element_type=F32)


def dot_t(lhs, rhs):
    return lax.dot_general(lhs, rhs, (((1,), (1,)), ((), ())), preferred_element_type=F32)


def softmax(scores):
    expd = jnp.exp(scores - jnp.max(scores, axis=-1, keepdims=True))
    return expd * (1.0 / jnp.sum(expd, axis=-1, keepdims=True))


def pipeline_kernel(
    n_stages,
    dec_len, pre_len, inv_freq, g_attn, g_mlp, g_final,
    x_dec, x_pre, w_q, w_k, w_v, w_o, w_gate, w_up, w_down, k_dec, v_dec, k_pre, v_pre,
    fin_out, kn_out, vn_out, kp_out, vp_out,
    wqkv, wo, w1, w3, w2, kc, vc, kp, vp, xin, xout, fin, qd, od, kn, vn, cosv, sinv, hid, sp, pp, pd,
    w_sem, kv_sem, p_sem, x_sem, o_sem, send_sem, recv_sem, fsend_sem, frecv_sem,
):
    n_micro, n_rows, hidden = xin.shape
    dec_rows = x_dec.shape[1]
    seg_len = x_pre.shape[1]
    per_micro = dec_len.shape[1]
    kv_width, cache_len = kp.shape
    q_width = wo.shape[0]
    ffn = w1.shape[1]
    head_dim = 64
    kv_count = kv_width // head_dim
    q_heads = q_width // head_dim
    group = q_heads // kv_count
    stage = lax.axis_index('stage')
    last = n_stages - 1
    half = ffn // 2
    seg_micro = seg_len * per_micro // dec_rows

    barrier = pltpu.get_barrier_semaphore()

    def x_copies(m):
        return (
            pltpu.make_async_copy(x_dec.at[m], xin.at[m, pl.ds(0, dec_rows)], x_sem.at[m, 0]),
            pltpu.make_async_copy(x_pre.at[m], xin.at[m, pl.ds(dec_rows, seg_len)], x_sem.at[m, 1]),
        )

    def k_copy(m):
        return pltpu.make_async_copy(k_dec.at[m], kc.at[m], kv_sem.at[m, 0])

    def v_copy(m):
        return pltpu.make_async_copy(v_dec.at[m], vc.at[m], kv_sem.at[m, 1])

    qkv_copies = (
        pltpu.make_async_copy(w_q, wqkv.at[:, pl.ds(0, q_width)], w_sem.at[0]),
        pltpu.make_async_copy(w_k, wqkv.at[:, pl.ds(q_width, kv_width)], w_sem.at[1]),
        pltpu.make_async_copy(w_v, wqkv.at[:, pl.ds(q_width + kv_width, kv_width)], w_sem.at[2]),
    )
    pre_copies = (
        pltpu.make_async_copy(k_pre, kp, p_sem.at[0]),
        pltpu.make_async_copy(v_pre, vp, p_sem.at[1]),
    )
    wo_copies = (pltpu.make_async_copy(w_o, wo, w_sem.at[3]),)
    up_copies = tuple(
        (
            pltpu.make_async_copy(w_gate.at[:, pl.ds(i * half, half)], w1.at[:, pl.ds(i * half, half)], w_sem.at[4 + 2 * i]),
            pltpu.make_async_copy(w_up.at[:, pl.ds(i * half, half)], w3.at[:, pl.ds(i * half, half)], w_sem.at[5 + 2 * i]),
        )
        for i in range(2)
    )
    down_copies = (pltpu.make_async_copy(w_down, w2, w_sem.at[8]),)

    @pl.when(stage == 0)
    def _():
        for copy in x_copies(0):
            copy.start()
    for copy in qkv_copies + pre_copies + (k_copy(0), v_copy(0)) + wo_copies + up_copies[0] + up_copies[1] + down_copies:
        copy.start()

    @pl.when(stage == 0)
    def _():
        for m in range(1, n_micro):
            for copy in x_copies(m):
                copy.start()
    for m in range(1, n_micro):
        for copy in (k_copy(m), v_copy(m)):
            copy.start()

    @pl.when(stage > 0)
    def _():
        pl.semaphore_signal(barrier, inc=1, device_id={'stage': stage - 1}, device_id_type=MESH)

    @pl.when(stage < last)
    def _():
        pl.semaphore_signal(barrier, inc=1, device_id={'stage': last}, device_id_type=MESH)

    lane = lax.broadcasted_iota(jnp.int32, (8, 128), 1)
    row8 = lax.broadcasted_iota(jnp.int32, (8, 128), 0)
    freq = inv_freq[...]
    sign = jnp.where((lane % head_dim) < head_dim // 2, -1.0, 1.0)

    def table_body(m, carry):
        for g in range(n_rows // 8):
            if g < dec_rows // 8:
                pos = jnp.zeros((8, 128), jnp.int32)
                for r in range(8):
                    pos = jnp.where(row8 == r, dec_len[m * (dec_rows // per_micro) + (g * 8 + r) // per_micro, (g * 8 + r) % per_micro], pos)
            else:
                pos = pre_len[0] + m * seg_len + (g * 8 - dec_rows) + row8
            angle = pos.astype(F32) * freq
            cosv[m, pl.ds(g * 8, 8), :] = jnp.cos(angle)
            sinv[m, pl.ds(g * 8, 8), :] = jnp.sin(angle) * sign
        return carry

    lax.fori_loop(0, n_micro, table_body, 0)
    qd[...] = jnp.zeros(qd.shape, F32)

    @pl.when(stage < last)
    def _():
        pl.semaphore_wait(barrier, 1)

    @pl.when(stage == last)
    def _():
        pl.semaphore_wait(barrier, n_stages - 1)

    def x_send(m):
        return pltpu.make_async_remote_copy(
            src_ref=xout.at[m], dst_ref=xin.at[m], send_sem=send_sem.at[m], recv_sem=recv_sem.at[m],
            device_id={'stage': jnp.minimum(stage + 1, last)}, device_id_type=MESH)

    def fin_send(m, target):
        return pltpu.make_async_remote_copy(
            src_ref=fin.at[m], dst_ref=fin.at[m], send_sem=fsend_sem.at[m, target], recv_sem=frecv_sem.at[m],
            device_id={'stage': target}, device_id_type=MESH)

    def tick(m, carry):
        first = m == 0

        @pl.when(stage == 0)
        def _():
            for copy in x_copies(m):
                copy.wait()

        @pl.when(stage > 0)
        def _():
            x_send(m).wait_recv()

        @pl.when(first)
        def _():
            for copy in qkv_copies + pre_copies:
                copy.wait()

        acts = xin[m]
        normed = rms_norm(acts, g_attn[...])
        cosine = cosv[m]
        sine = sinv[m]
        lane_q = lax.broadcasted_iota(jnp.int32, (n_rows, 128), 1)
        low32 = (lane_q % head_dim) < head_dim // 2
        low_half = lax.broadcasted_iota(jnp.int32, (dec_rows, 128), 1) < head_dim

        def rotate(tile):
            swapped = jnp.where(low32, pltpu.roll(tile, 128 - head_dim // 2, 1), pltpu.roll(tile, head_dim // 2, 1))
            return tile * cosine + swapped * sine

        proj = dot(normed, wqkv[...])
        q_tiles = [rotate(proj[:, t * 128:(t + 1) * 128]).astype(BF16).astype(F32) for t in range(q_width // 128)]
        k_new = rotate(proj[:, q_width:q_width + kv_width]).astype(BF16)
        v_new = proj[:, q_width + kv_width:].astype(BF16)
        kn[...] = k_new[:dec_rows].astype(F32)
        vn[...] = v_new[:dec_rows].astype(F32)
        kn_out[m] = k_new[:dec_rows]
        vn_out[m] = v_new[:dec_rows]

        for j in range(q_heads):
            tile = q_tiles[j // 2][:dec_rows]
            if j % 2 != j // group:
                tile = pltpu.roll(tile, head_dim, 1)
            keep = low_half if j // group == 0 else jnp.logical_not(low_half)
            qd[pl.ds(j, dec_rows, stride=16), :] = jnp.where(keep, tile, 0.0)

        pre_begin = pre_len[0] + m * seg_len
        seg_row = lax.broadcasted_iota(jnp.int32, (seg_len, cache_len), 0)
        seg_col = lax.broadcasted_iota(jnp.int32, (seg_len, cache_len), 1)
        spread = (seg_col == seg_row + pre_begin).astype(F32).astype(BF16)
        col = lax.broadcasted_iota(jnp.int32, (kv_width, cache_len), 1)
        written = (col >= pre_begin) & (col < pre_begin + seg_len)
        contract0 = (((0,), (0,)), ((), ()))
        k_put = lax.dot_general(k_new[dec_rows:], spread, contract0, preferred_element_type=F32)
        v_put = lax.dot_general(v_new[dec_rows:], spread, contract0, preferred_element_type=F32)
        kp_f = jnp.where(written, k_put, kp[...].astype(F32)).astype(BF16)
        vp_f = jnp.where(written, v_put, vp[...].astype(F32)).astype(BF16)
        kp[...] = kp_f
        vp[...] = vp_f

        scale = head_dim ** -0.5
        pre_valid = seg_col <= seg_row + pre_begin
        span = group * seg_len
        for g in range(kv_count):
            rows = []
            for j in range(g * group, (g + 1) * group):
                keep = low_half if j % 2 == 0 else jnp.logical_not(low_half)
                rows.append(jnp.where(keep, q_tiles[j // 2][dec_rows:], 0.0).astype(BF16))
            k_g = kp_f[g * head_dim:(g + 1) * head_dim]
            sp[g * span:(g + 1) * span, :] = dot(jnp.concatenate(rows, axis=0), jnp.concatenate([k_g, k_g], axis=0))
        for j in range(q_heads):
            scores = sp[j * seg_len:(j + 1) * seg_len, :] * scale
            pp[j * seg_len:(j + 1) * seg_len, :] = softmax(jnp.where(pre_valid, scores, NEG)).astype(BF16)

        k_copy(m).wait()
        pos_lane = lax.broadcasted_iota(jnp.int32, (16, cache_len), 1)
        for b in range(dec_rows):
            pos = dec_len[m * (dec_rows // per_micro) + b // per_micro, b % per_micro]
            q_b = qd[b * 16:(b + 1) * 16, :]
            s_old = dot(q_b.astype(BF16), kc[m, b]) * scale
            s_new = jnp.sum(q_b * kn[b:b + 1, :], axis=-1, keepdims=True) * scale
            here = pos_lane == pos
            scores = jnp.where(here, s_new, jnp.where(pos_lane < pos, s_old, NEG))
            peak = jnp.max(scores, axis=-1, keepdims=True)
            expd = jnp.exp(scores - peak)
            inv = 1.0 / jnp.sum(expd, axis=-1, keepdims=True)
            pd[b * 16:(b + 1) * 16, :] = jnp.where(here, 0.0, expd * inv).astype(BF16)
            p_new = (jnp.exp(s_new - peak) * inv).astype(BF16).astype(F32)
            od[b * 16:(b + 1) * 16, :] = p_new * vn[b:b + 1, :]

        pre_heads = []
        for g in range(kv_count):
            v_g = vp_f[g * head_dim:(g + 1) * head_dim]
            mixed = dot_t(pp[g * span:(g + 1) * span, :], jnp.concatenate([v_g, v_g], axis=0))
            pre_heads += [mixed[i * seg_len:(i + 1) * seg_len] for i in range(group)]
        v_copy(m).wait()
        for b in range(dec_rows):
            od[b * 16:(b + 1) * 16, :] += dot_t(pd[b * 16:(b + 1) * 16, :], vc[m, b])

        att_tiles = []
        for t in range(q_width // 128):
            parts = []
            for j in (2 * t, 2 * t + 1):
                part = od[pl.ds(j, dec_rows, stride=16), :]
                if j % 2 != j // group:
                    part = pltpu.roll(part, head_dim, 1)
                parts.append(part)
            dec_tile = jnp.where(low_half, parts[0], parts[1])
            pre_tile = jnp.where(low_half, pre_heads[2 * t], pre_heads[2 * t + 1])
            att_tiles.append(jnp.concatenate([dec_tile, pre_tile], axis=0).astype(BF16))
        att = jnp.concatenate(att_tiles, axis=1)

        @pl.when(first)
        def _():
            for copy in wo_copies:
                copy.wait()

        acts = (acts.astype(F32) + dot(att, wo[...])).astype(BF16)
        normed = rms_norm(acts, g_mlp[...])

        n_blk = 256
        for i in range(2):
            @pl.when(first)
            def _():
                for copy in up_copies[i]:
                    copy.wait()
            lo = 0 if i == 0 else half // n_blk * n_blk
            hi = half // n_blk * n_blk if i == 0 else ffn
            for n in range(lo, hi, n_blk):
                gate = dot(normed, w1[:, n:n + n_blk])
                up = dot(normed, w3[:, n:n + n_blk])
                hid[:, n:n + n_blk] = (jax.nn.silu(gate) * up).astype(BF16)

        @pl.when(first)
        def _():
            for copy in down_copies:
                copy.wait()
        acts = (acts.astype(F32) + dot(hid[...], w2[...])).astype(BF16)

        @pl.when(stage < last)
        def _():
            xout[m] = acts
            x_send(m).start()

        @pl.when(stage == last)
        def _():
            ends = [acts[dec_rows + e - 8:dec_rows + e] for e in range(seg_micro, seg_len + 1, seg_micro)]
            tail = jnp.concatenate([acts[:dec_rows]] + ends, axis=0)
            fin[m] = rms_norm(tail, g_final[...].astype(F32)[None, :])
            for target in range(n_stages - 1):
                fin_send(m, target).start()
        return carry

    lax.fori_loop(0, n_micro, tick, 0)

    kp_copy = pltpu.make_async_copy(kp, kp_out, o_sem.at[0])
    vp_copy = pltpu.make_async_copy(vp, vp_out, o_sem.at[1])
    kp_copy.start()
    vp_copy.start()

    @pl.when(stage < last)
    def _():
        for m in range(n_micro):
            x_send(m).wait_send()
        for m in range(n_micro):
            fin_send(m, 0).wait_recv()

    @pl.when(stage == last)
    def _():
        for m in range(n_micro):
            for target in range(n_stages - 1):
                fin_send(m, target).wait_send()

    fin_copy = pltpu.make_async_copy(fin, fin_out, o_sem.at[2])
    fin_copy.start()
    kp_copy.wait()
    vp_copy.wait()
    fin_copy.wait()


def head_kernel(micros, fin, w_head, logits, rows):
    n_chunk, fin_rows, _ = fin.shape
    n_kept = logits.shape[0]
    join = micros // n_chunk

    @pl.when(pl.program_id(0) == 0)
    def _():
        for m in range(micros):
            kept = fin[m // join].astype(F32)
            first = (m % join) * (n_kept - 1)
            last = (n_kept - 1) * join + 8 * (m % join) + 7
            for t in range(rows.shape[0]):
                tile = kept[:, t * 128:(t + 1) * 128]
                rows[t, pl.ds(m, n_kept - 1, stride=micros), :] = tile[first:first + n_kept - 1]
                rows[t, (n_kept - 1) * micros + m:(n_kept - 1) * micros + m + 1, :] = tile[last:last + 1]

    lhs = jnp.concatenate([rows[t].astype(BF16) for t in range(rows.shape[0])], axis=1)
    out = dot(lhs, w_head[...])
    for i in range(n_kept):
        logits[i] = out[i * micros:(i + 1) * micros]


def cache_kernel(dec_len, kn, vn, k_in, v_in, k_out, v_out, buf, in_sem, out_sem):
    n_slot, n_seq, kv_width, cache_len = buf.shape
    n_chunk, dec_rows = k_in.shape[:2]
    per_micro = dec_len.shape[1]
    blocks = [(t, m, b) for m in range(n_chunk) for b in range(0, dec_rows, n_seq) for t in range(2)]
    arrays = ((kn, k_in, k_out), (vn, v_in, v_out))

    def load(i):
        t, m, b = blocks[i]
        return pltpu.make_async_copy(arrays[t][1].at[m, pl.ds(b, n_seq)], buf.at[i % n_slot], in_sem.at[i % n_slot])

    def store(i):
        t, m, b = blocks[i]
        return pltpu.make_async_copy(buf.at[i % n_slot], arrays[t][2].at[m, pl.ds(b, n_seq)], out_sem.at[i % n_slot])

    ahead = n_slot // 2
    for i in range(ahead):
        load(i).start()
    lane = lax.broadcasted_iota(jnp.int32, (kv_width, 128), 1)
    for i, (t, m, b) in enumerate(blocks):
        if i + ahead < len(blocks):
            if i + ahead >= n_slot:
                store(i + ahead - n_slot).wait()
            load(i + ahead).start()
        load(i).wait()
        cols = jnp.transpose(arrays[t][0][m, b:b + n_seq, :].astype(F32))
        for r in range(n_seq):
            pos = dec_len[m * (dec_rows // per_micro) + (b + r) // per_micro, (b + r) % per_micro]
            at = pl.ds(pl.multiple_of(pos // 128 * 128, 128), 128)
            old = buf[i % n_slot, r, :, at]
            buf[i % n_slot, r, :, at] = jnp.where(lane == pos % 128, cols[:, r:r + 1], old.astype(F32)).astype(BF16)
        store(i).start()
    for i in range(len(blocks) - n_slot, len(blocks)):
        store(i).wait()


def solution(mesh):
    n_stages = mesh.shape['stage']
    part_spec = P('replica')
    layer_spec = P('stage')
    cache_spec = P('stage', 'replica')
    in_specs = (part_spec,) * 4 + (layer_spec,) * 9 + (P(), P()) + (cache_spec,) * 4
    out_specs = (part_spec,) + (cache_spec,) * 4

    def device_fn(x_dec, x_pre, dec_len, pre_len, g_attn, w_q, w_k, w_v, w_o, g_mlp, w_gate, w_up, w_down, g_final, w_head, k_dec, v_dec, k_pre, v_pre):
        micros, micro_rows, hidden = x_dec.shape
        n_micro = micros // JOIN
        dec_rows = micro_rows * JOIN
        seg_len = x_pre.shape[1] * JOIN
        x_dec = x_dec.reshape(n_micro, dec_rows, hidden)
        x_pre = x_pre.reshape(n_micro, seg_len, hidden)
        n_rows = dec_rows + seg_len
        _, cache_len, kv_count, head_dim = k_pre.shape
        kv_width = kv_count * head_dim
        q_width = w_q.shape[2]
        ffn = w_gate.shape[2]
        vocab = w_head.shape[1]
        fin_rows = dec_rows + 8 * JOIN

        kd = jnp.transpose(k_dec[0], (0, 1, 3, 4, 2)).reshape(n_micro, dec_rows, kv_width, cache_len)
        vd = jnp.transpose(v_dec[0], (0, 1, 3, 4, 2)).reshape(n_micro, dec_rows, kv_width, cache_len)
        kpre = jnp.transpose(k_pre[0], (1, 2, 0)).reshape(kv_width, cache_len)
        vpre = jnp.transpose(v_pre[0], (1, 2, 0)).reshape(kv_width, cache_len)

        lanes = np.arange(128) % (head_dim // 2)
        inv_freq = jnp.asarray((ROPE_BASE ** (-lanes * (2.0 / head_dim))).astype(np.float32)[None, :])

        def spec(space):
            return pl.BlockSpec(memory_space=space)

        fin, kn, vn, kp, vp = pl.pallas_call(
            functools.partial(pipeline_kernel, n_stages),
            out_shape=(
                jax.ShapeDtypeStruct((n_micro, fin_rows, hidden), BF16),
                jax.ShapeDtypeStruct((n_micro, dec_rows, kv_width), BF16),
                jax.ShapeDtypeStruct((n_micro, dec_rows, kv_width), BF16),
                jax.ShapeDtypeStruct((kv_width, cache_len), BF16),
                jax.ShapeDtypeStruct((kv_width, cache_len), BF16),
            ),
            in_specs=[spec(SMEM)] * 2 + [spec(VMEM)] * 4 + [spec(HBM)] * 13,
            out_specs=(spec(HBM), spec(VMEM), spec(VMEM), spec(HBM), spec(HBM)),
            scratch_shapes=[
                VMEM((hidden, q_width + 2 * kv_width), BF16),
                VMEM((q_width, hidden), BF16),
                VMEM((hidden, ffn), BF16),
                VMEM((hidden, ffn), BF16),
                VMEM((ffn, hidden), BF16),
                VMEM((n_micro, dec_rows, kv_width, cache_len), BF16),
                VMEM((n_micro, dec_rows, kv_width, cache_len), BF16),
                VMEM((kv_width, cache_len), BF16),
                VMEM((kv_width, cache_len), BF16),
                VMEM((n_micro, n_rows, hidden), BF16),
                VMEM((n_micro, n_rows, hidden), BF16),
                VMEM((n_micro, fin_rows, hidden), BF16),
                VMEM((dec_rows * 16, 128), F32),
                VMEM((dec_rows * 16, 128), F32),
                VMEM((dec_rows, kv_width), F32),
                VMEM((dec_rows, kv_width), F32),
                VMEM((n_micro, n_rows, 128), F32),
                VMEM((n_micro, n_rows, 128), F32),
                VMEM((n_rows, ffn), BF16),
                VMEM((q_width // head_dim * seg_len, cache_len), F32),
                VMEM((q_width // head_dim * seg_len, cache_len), BF16),
                VMEM((dec_rows * 16, cache_len), BF16),
                pltpu.SemaphoreType.DMA((9,)),
                pltpu.SemaphoreType.DMA((n_micro, 2)),
                pltpu.SemaphoreType.DMA((2,)),
                pltpu.SemaphoreType.DMA((n_micro, 2)),
                pltpu.SemaphoreType.DMA((3,)),
                pltpu.SemaphoreType.DMA((n_micro,)),
                pltpu.SemaphoreType.DMA((n_micro,)),
                pltpu.SemaphoreType.DMA((n_micro, n_stages - 1)),
                pltpu.SemaphoreType.DMA((n_micro,)),
            ],
            compiler_params=pltpu.CompilerParams(collective_id=0, has_side_effects=True, vmem_limit_bytes=62 * 1024 * 1024),
            name='pipeline',
        )(dec_len, pre_len, inv_freq, g_attn, g_mlp, g_final,
          x_dec, x_pre, w_q[0], w_k[0], w_v[0], w_o[0], w_gate[0], w_up[0], w_down[0], kd, vd, kpre, vpre)

        v_blk = 1024
        logits = pl.pallas_call(
            functools.partial(head_kernel, micros),
            grid=(vocab // v_blk,),
            out_shape=jax.ShapeDtypeStruct((micro_rows + 1, micros, vocab), F32),
            in_specs=[
                pl.BlockSpec((n_micro, fin_rows, hidden), lambda n: (0, 0, 0)),
                pl.BlockSpec((hidden, v_blk), lambda n: (0, n)),
            ],
            out_specs=pl.BlockSpec((micro_rows + 1, micros, v_blk), lambda n: (0, 0, n)),
            scratch_shapes=[VMEM((hidden // 128, (micro_rows + 1) * micros, 128), F32)],
            name='head',
        )(fin, w_head)

        kd_out, vd_out = pl.pallas_call(
            cache_kernel,
            out_shape=(jax.ShapeDtypeStruct(kd.shape, BF16),) * 2,
            in_specs=[spec(SMEM), spec(VMEM), spec(VMEM), spec(HBM), spec(HBM)],
            out_specs=(spec(HBM), spec(HBM)),
            scratch_shapes=[
                VMEM((16, 16, kv_width, cache_len), BF16),
                pltpu.SemaphoreType.DMA((16,)),
                pltpu.SemaphoreType.DMA((16,)),
            ],
            compiler_params=pltpu.CompilerParams(vmem_limit_bytes=62 * 1024 * 1024),
            name='cache',
        )(dec_len, kn, vn, kd, vd)

        def dec_cache(arr):
            return jnp.transpose(arr.reshape(micros, micro_rows, kv_count, head_dim, cache_len), (0, 1, 4, 2, 3))[None]

        def pre_cache(arr):
            return jnp.transpose(arr.reshape(kv_count, head_dim, cache_len), (2, 0, 1))[None]

        return jnp.transpose(logits, (1, 0, 2)), dec_cache(kd_out), dec_cache(vd_out), pre_cache(kp), pre_cache(vp)

    return jax.shard_map(device_fn, mesh=mesh, in_specs=in_specs, out_specs=out_specs, check_vma=False)
```

```python
import functools

import jax
import jax.numpy as jnp
import numpy as np
from jax import lax
from jax.experimental import pallas as pl
from jax.experimental.pallas import tpu as pltpu
from jax.sharding import PartitionSpec as P

NORM_EPS = 1e-6
ROPE_BASE = 10000.0
F32 = jnp.float32
BF16 = jnp.bfloat16
NEG = -1e30
HBM = pl.ANY
VMEM = pltpu.VMEM
SMEM = pltpu.SMEM
MESH = pl.DeviceIdType.MESH
R1_MB = 25
JOIN = 2


def rms_norm(acts, gain):
    acts_f = acts.astype(F32)
    inv_rms = lax.rsqrt(jnp.mean(acts_f * acts_f, axis=-1, keepdims=True) + NORM_EPS)
    return (acts_f * inv_rms * gain.astype(F32)).astype(BF16)


def dot(lhs, rhs):
    return jnp.dot(lhs, rhs, preferred_element_type=F32)


def dot_t(lhs, rhs):
    return lax.dot_general(lhs, rhs, (((1,), (1,)), ((), ())), preferred_element_type=F32)


def softmax(scores):
    expd = jnp.exp(scores - jnp.max(scores, axis=-1, keepdims=True))
    return expd * (1.0 / jnp.sum(expd, axis=-1, keepdims=True))


def pipeline_kernel(
    n_stages,
    dec_len, pre_len, inv_freq_in, g_attn_in, g_mlp_in, g_final_in,
    x_dec, x_pre, w_q, w_k, w_v, w_o, w_gate, w_up, w_down, k_dec, v_dec, k_pre, v_pre, w_head,
    kc, vc, w1, fin_out, kp_out, vp_out,
    inv_freq, g_attn, g_mlp, g_final, wqkv, wo, w3, w2, kp, vp, xin, fin, qd, kn, vn, cosv, sinv, hid, sp,
    w_sem, kv_sem, p_sem, x_sem, o_sem, g_sem, send_sem, recv_sem, fsend_sem, frecv_sem,
):
    n_micro, n_rows, hidden = xin.shape
    dec_rows = x_dec.shape[1]
    seg_len = x_pre.shape[1]
    per_micro = dec_len.shape[1]
    kv_width, cache_len = kp.shape
    q_width = wo.shape[0]
    ffn = w2.shape[0]
    head_dim = 64
    kv_count = kv_width // head_dim
    q_heads = q_width // head_dim
    group = q_heads // kv_count
    stage = lax.axis_index('stage')
    last = n_stages - 1
    half = ffn // 2
    seg_micro = seg_len * per_micro // dec_rows

    barrier = pltpu.get_barrier_semaphore()

    def x_copies(m):
        return (
            pltpu.make_async_copy(x_dec.at[m], xin.at[m, pl.ds(0, dec_rows)], x_sem.at[m, 0]),
            pltpu.make_async_copy(x_pre.at[m], xin.at[m, pl.ds(dec_rows, seg_len)], x_sem.at[m, 1]),
        )

    def k_copy(m):
        return pltpu.make_async_copy(k_dec.at[m], kc.at[m], kv_sem.at[m, 0])

    def v_copy(m):
        return pltpu.make_async_copy(v_dec.at[m], vc.at[m], kv_sem.at[m, 1])

    qkv_copies = (
        pltpu.make_async_copy(w_q, wqkv.at[:, pl.ds(0, q_width)], w_sem.at[0]),
        pltpu.make_async_copy(w_k, wqkv.at[:, pl.ds(q_width, kv_width)], w_sem.at[1]),
        pltpu.make_async_copy(w_v, wqkv.at[:, pl.ds(q_width + kv_width, kv_width)], w_sem.at[2]),
    )
    pre_copies = (
        pltpu.make_async_copy(k_pre, kp, p_sem.at[0]),
        pltpu.make_async_copy(v_pre, vp, p_sem.at[1]),
    )
    wo_copies = (pltpu.make_async_copy(w_o, wo, w_sem.at[3]),)
    up_copies = tuple(
        (
            pltpu.make_async_copy(w_gate.at[:, pl.ds(i * half, half)], w1.at[:, pl.ds(i * half, half)], w_sem.at[4 + 2 * i]),
            pltpu.make_async_copy(w_up.at[:, pl.ds(i * half, half)], w3.at[:, pl.ds(i * half, half)], w_sem.at[5 + 2 * i]),
        )
        for i in range(2)
    )
    head_copies = (pltpu.make_async_copy(w_head.at[:, pl.ds(0, ffn)], w1, w_sem.at[9]),)
    down_copies = (pltpu.make_async_copy(w_down, w2, w_sem.at[8]),)

    gain_copies = [pltpu.make_async_copy(src, dst, g_sem.at[i]) for i, (src, dst) in enumerate((
        (inv_freq_in, inv_freq), (g_attn_in, g_attn), (g_mlp_in, g_mlp), (g_final_in, g_final)))]
    for copy in gain_copies:
        copy.start()

    @pl.when(stage == 0)
    def _():
        for copy in x_copies(0):
            copy.start()
    for copy in qkv_copies + pre_copies + (k_copy(0), v_copy(0)) + wo_copies + up_copies[0] + up_copies[1] + down_copies:
        copy.start()

    @pl.when(stage == 0)
    def _():
        for m in range(1, n_micro):
            for copy in x_copies(m):
                copy.start()
    for m in range(1, n_micro):
        for copy in (k_copy(m), v_copy(m)):
            copy.start()

    @pl.when(stage > 0)
    def _():
        pl.semaphore_signal(barrier, inc=1, device_id={'stage': stage - 1}, device_id_type=MESH)

    @pl.when(stage < last)
    def _():
        pl.semaphore_signal(barrier, inc=1, device_id={'stage': last}, device_id_type=MESH)

    for copy in gain_copies:
        copy.wait()

    lane = lax.broadcasted_iota(jnp.int32, (8, 128), 1)
    row8 = lax.broadcasted_iota(jnp.int32, (8, 128), 0)
    freq = inv_freq[...]
    sign = jnp.where((lane % head_dim) < head_dim // 2, -1.0, 1.0)

    def table_body(m, carry):
        for g in range(n_rows // 8):
            if g < dec_rows // 8:
                pos = jnp.zeros((8, 128), jnp.int32)
                for r in range(8):
                    pos = jnp.where(row8 == r, dec_len[m * (dec_rows // per_micro) + (g * 8 + r) // per_micro, (g * 8 + r) % per_micro], pos)
            else:
                pos = pre_len[0] + m * seg_len + (g * 8 - dec_rows) + row8
            angle = pos.astype(F32) * freq
            cosv[m, pl.ds(g * 8, 8), :] = jnp.cos(angle)
            sinv[m, pl.ds(g * 8, 8), :] = jnp.sin(angle) * sign
        return carry

    lax.fori_loop(0, n_micro, table_body, 0)
    qd[...] = jnp.zeros(qd.shape, F32)

    @pl.when(stage < last)
    def _():
        pl.semaphore_wait(barrier, 1)

    @pl.when(stage == last)
    def _():
        pl.semaphore_wait(barrier, n_stages - 1)

    def x_send(m):
        return pltpu.make_async_remote_copy(
            src_ref=xin.at[m], dst_ref=xin.at[m], send_sem=send_sem.at[m], recv_sem=recv_sem.at[m],
            device_id={'stage': jnp.minimum(stage + 1, last)}, device_id_type=MESH)

    def fin_send(m, target):
        return pltpu.make_async_remote_copy(
            src_ref=fin.at[m], dst_ref=fin.at[m], send_sem=fsend_sem.at[m, target], recv_sem=frecv_sem.at[m],
            device_id={'stage': target}, device_id_type=MESH)

    def tick(m, carry):
        first = m == 0

        @pl.when(stage == 0)
        def _():
            for copy in x_copies(m):
                copy.wait()

        @pl.when(stage > 0)
        def _():
            x_send(m).wait_recv()

        @pl.when(first)
        def _():
            for copy in qkv_copies + pre_copies:
                copy.wait()

        acts = xin[m]
        normed = rms_norm(acts, g_attn[...])
        cosine = cosv[m]
        sine = sinv[m]
        lane_q = lax.broadcasted_iota(jnp.int32, (n_rows, 128), 1)
        low32 = (lane_q % head_dim) < head_dim // 2
        low_half = lax.broadcasted_iota(jnp.int32, (dec_rows, 128), 1) < head_dim

        def rotate(tile):
            swapped = jnp.where(low32, pltpu.roll(tile, 128 - head_dim // 2, 1), pltpu.roll(tile, head_dim // 2, 1))
            return tile * cosine + swapped * sine

        proj = dot(normed, wqkv[...])
        q_tiles = [rotate(proj[:, t * 128:(t + 1) * 128]).astype(BF16).astype(F32) for t in range(q_width // 128)]
        k_new = rotate(proj[:, q_width:q_width + kv_width]).astype(BF16)
        v_new = proj[:, q_width + kv_width:].astype(BF16)
        kn[m] = k_new[:dec_rows].astype(F32)
        vn[m] = v_new[:dec_rows].astype(F32)

        for j in range(q_heads):
            tile = q_tiles[j // 2][:dec_rows]
            if j % 2 != j // group:
                tile = pltpu.roll(tile, head_dim, 1)
            keep = low_half if j // group == 0 else jnp.logical_not(low_half)
            qd[pl.ds(j, dec_rows, stride=16), :] = jnp.where(keep, tile, 0.0)

        pre_begin = pre_len[0] + m * seg_len
        seg_row = lax.broadcasted_iota(jnp.int32, (seg_len, cache_len), 0)
        seg_col = lax.broadcasted_iota(jnp.int32, (seg_len, cache_len), 1)
        spread = (seg_col == seg_row + pre_begin).astype(F32).astype(BF16)
        col = lax.broadcasted_iota(jnp.int32, (kv_width, cache_len), 1)
        written = (col >= pre_begin) & (col < pre_begin + seg_len)
        contract0 = (((0,), (0,)), ((), ()))
        k_put = lax.dot_general(k_new[dec_rows:], spread, contract0, preferred_element_type=F32)
        v_put = lax.dot_general(v_new[dec_rows:], spread, contract0, preferred_element_type=F32)
        kp_f = jnp.where(written, k_put, kp[...].astype(F32)).astype(BF16)
        vp_f = jnp.where(written, v_put, vp[...].astype(F32)).astype(BF16)
        kp[...] = kp_f
        vp[...] = vp_f

        scale = head_dim ** -0.5
        pre_valid = seg_col <= seg_row + pre_begin
        span = group * seg_len
        pd_base = q_heads * seg_len
        for g in range(kv_count):
            rows = []
            for j in range(g * group, (g + 1) * group):
                keep = low_half if j % 2 == 0 else jnp.logical_not(low_half)
                rows.append(jnp.where(keep, q_tiles[j // 2][dec_rows:], 0.0).astype(BF16))
            k_g = kp_f[g * head_dim:(g + 1) * head_dim]
            sp[...] = dot(jnp.concatenate(rows, axis=0), jnp.concatenate([k_g, k_g], axis=0))
            for j in range(group):
                scores = sp[j * seg_len:(j + 1) * seg_len, :] * scale
                base = (g * group + j) * seg_len
                hid[base:base + seg_len, :] = softmax(jnp.where(pre_valid, scores, NEG)).astype(BF16)

        k_copy(m).wait()
        pos_lane = lax.broadcasted_iota(jnp.int32, (16, cache_len), 1)
        for b in range(dec_rows):
            pos = dec_len[m * (dec_rows // per_micro) + b // per_micro, b % per_micro]
            q_b = qd[b * 16:(b + 1) * 16, :]
            s_old = dot(q_b.astype(BF16), kc[m, b]) * scale
            s_new = jnp.sum(q_b * kn[m, b:b + 1, :], axis=-1, keepdims=True) * scale
            here = pos_lane == pos
            scores = jnp.where(here, s_new, jnp.where(pos_lane < pos, s_old, NEG))
            peak = jnp.max(scores, axis=-1, keepdims=True)
            expd = jnp.exp(scores - peak)
            inv = 1.0 / jnp.sum(expd, axis=-1, keepdims=True)
            hid[pd_base + b * 16:pd_base + (b + 1) * 16, :] = jnp.where(here, 0.0, expd * inv).astype(BF16)
            p_new = (jnp.exp(s_new - peak) * inv).astype(BF16).astype(F32)
            qd[b * 16:(b + 1) * 16, :] = p_new * vn[m, b:b + 1, :]

        pre_heads = []
        for g in range(kv_count):
            v_g = vp_f[g * head_dim:(g + 1) * head_dim]
            mixed = dot_t(hid[g * span:(g + 1) * span, :], jnp.concatenate([v_g, v_g], axis=0))
            pre_heads += [mixed[i * seg_len:(i + 1) * seg_len] for i in range(group)]
        v_copy(m).wait()
        for b in range(dec_rows):
            qd[b * 16:(b + 1) * 16, :] += dot_t(hid[pd_base + b * 16:pd_base + (b + 1) * 16, :], vc[m, b])

        att_tiles = []
        for t in range(q_width // 128):
            parts = []
            for j in (2 * t, 2 * t + 1):
                part = qd[pl.ds(j, dec_rows, stride=16), :]
                if j % 2 != j // group:
                    part = pltpu.roll(part, head_dim, 1)
                parts.append(part)
            dec_tile = jnp.where(low_half, parts[0], parts[1])
            pre_tile = jnp.where(low_half, pre_heads[2 * t], pre_heads[2 * t + 1])
            att_tiles.append(jnp.concatenate([dec_tile, pre_tile], axis=0).astype(BF16))
        att = jnp.concatenate(att_tiles, axis=1)

        @pl.when(first)
        def _():
            for copy in wo_copies:
                copy.wait()

        acts = (acts.astype(F32) + dot(att, wo[...])).astype(BF16)
        normed = rms_norm(acts, g_mlp[...])

        n_blk = 256
        for i in range(2):
            @pl.when(first)
            def _():
                for copy in up_copies[i]:
                    copy.wait()
            lo = 0 if i == 0 else half // n_blk * n_blk
            hi = half // n_blk * n_blk if i == 0 else ffn
            for n in range(lo, hi, n_blk):
                gate = dot(normed, w1[:, n:n + n_blk])
                up = dot(normed, w3[:, n:n + n_blk])
                k = n // n_blk
                hid[k * n_rows:(k + 1) * n_rows, :] = (jax.nn.silu(gate) * up).astype(BF16)

        @pl.when(first)
        def _():
            for copy in down_copies:
                copy.wait()

        @pl.when(m == n_micro - 1)
        def _():
            for copy in head_copies:
                copy.start()

        hidden_act = jnp.concatenate([hid[k * n_rows:(k + 1) * n_rows, :] for k in range(ffn // n_blk)], axis=1)
        acts = (acts.astype(F32) + dot(hidden_act, w2[...])).astype(BF16)

        @pl.when(stage < last)
        def _():
            xin[m] = acts
            x_send(m).start()

        @pl.when(stage == last)
        def _():
            ends = [acts[dec_rows + e - 8:dec_rows + e] for e in range(seg_micro, seg_len + 1, seg_micro)]
            tail = jnp.concatenate([acts[:dec_rows]] + ends, axis=0)
            fin[m] = rms_norm(tail, g_final[...].astype(F32)[None, :])
            for target in range(n_stages - 1):
                fin_send(m, target).start()
        return carry

    lax.fori_loop(0, n_micro, tick, 0)

    pre_out = (pltpu.make_async_copy(kp, kp_out, o_sem.at[0]), pltpu.make_async_copy(vp, vp_out, o_sem.at[1]))
    for copy in pre_out:
        copy.start()

    col_full = lax.broadcasted_iota(jnp.int32, (kv_width, cache_len), 1)

    def patch(m, carry):
        for new, cache in ((kn, kc), (vn, vc)):
            cols = jnp.transpose(new[m])
            for b in range(dec_rows):
                pos = dec_len[m * (dec_rows // per_micro) + b // per_micro, b % per_micro]
                column = jnp.broadcast_to(cols[:, b:b + 1], (kv_width, cache_len)).astype(BF16)
                cache[m, b] = jnp.where(col_full == pos, column, cache[m, b])
        return carry

    lax.fori_loop(0, n_micro, patch, 0)

    @pl.when(stage < last)
    def _():
        for m in range(n_micro):
            x_send(m).wait_send()
        for m in range(n_micro):
            fin_send(m, 0).wait_recv()

    @pl.when(stage == last)
    def _():
        for m in range(n_micro):
            for target in range(n_stages - 1):
                fin_send(m, target).wait_send()

    fin_copy = pltpu.make_async_copy(fin, fin_out, o_sem.at[2])
    fin_copy.start()
    for copy in pre_out:
        copy.wait()
    fin_copy.wait()
    for copy in head_copies:
        copy.wait()


def output_kernel(micros, vocab, kc, vc, w_low, w_all, fin_in, kp_in, vp_in, logits, kc_out, vc_out, kp_out, vp_out, w_high, fin, kp, vp, rows, stage_buf, i_sem, c_sem, l_sem):
    n_chunk = fin.shape[0]
    n_kept = logits.shape[0]
    join = micros // n_chunk
    n_slot, _, _, v_blk = stage_buf.shape
    copies = [pltpu.make_async_copy(src, dst, c_sem.at[i]) for i, (src, dst) in enumerate(((kc, kc_out), (vc, vc_out), (kp, kp_out), (vp, vp_out)))]
    loads = [pltpu.make_async_copy(src, dst, i_sem.at[i]) for i, (src, dst) in enumerate(((fin_in, fin), (kp_in, kp), (vp_in, vp)))]
    low = w_low.shape[1]
    w_load = pltpu.make_async_copy(w_all.at[:, pl.ds(low, vocab - low)], w_high, i_sem.at[3])
    for copy in loads + [w_load] + copies[:2]:
        copy.start()
    for copy in loads:
        copy.wait()
    for copy in copies[2:]:
        copy.start()

    for m in range(micros):
        kept = fin[m // join].astype(F32)
        first = (m % join) * (n_kept - 1)
        last = (n_kept - 1) * join + 8 * (m % join) + 7
        for t in range(rows.shape[0]):
            tile = kept[:, t * 128:(t + 1) * 128]
            rows[t, pl.ds(m, n_kept - 1, stride=micros), :] = tile[first:first + n_kept - 1]
            rows[t, (n_kept - 1) * micros + m:(n_kept - 1) * micros + m + 1, :] = tile[last:last + 1]
    lhs = jnp.concatenate([rows[t].astype(BF16) for t in range(rows.shape[0])], axis=1)

    blocks = [(w_low, 0, n, min(v_blk, low - n)) for n in range(0, low, v_blk)]
    blocks += [(w_high, low, n, min(v_blk, vocab - low - n)) for n in range(0, vocab - low, v_blk)]

    def store(i):
        _, base, n, width = blocks[i]
        return pltpu.make_async_copy(
            stage_buf.at[i % n_slot, :, :, pl.ds(0, width)], logits.at[:, :, pl.ds(base + n, width)], l_sem.at[i % n_slot])

    for i, (w_ref, base, n, width) in enumerate(blocks):
        if i >= n_slot:
            store(i - n_slot).wait()
        if base and n == 0:
            w_load.wait()
        out = dot(lhs, w_ref[:, n:n + width])
        for r in range(n_kept):
            stage_buf[i % n_slot, r, :, :width] = out[r * micros:(r + 1) * micros]
        store(i).start()
    for i in range(len(blocks) - n_slot, len(blocks)):
        store(i).wait()
    for copy in copies:
        copy.wait()


def solution(mesh):
    n_stages = mesh.shape['stage']
    part_spec = P('replica')
    layer_spec = P('stage')
    cache_spec = P('stage', 'replica')
    in_specs = (part_spec,) * 4 + (layer_spec,) * 9 + (P(), P()) + (cache_spec,) * 4
    out_specs = (part_spec,) + (cache_spec,) * 4

    def device_fn(x_dec, x_pre, dec_len, pre_len, g_attn, w_q, w_k, w_v, w_o, g_mlp, w_gate, w_up, w_down, g_final, w_head, k_dec, v_dec, k_pre, v_pre):
        micros, micro_rows, hidden = x_dec.shape
        n_micro = micros // JOIN
        dec_rows = micro_rows * JOIN
        seg_len = x_pre.shape[1] * JOIN
        x_dec = x_dec.reshape(n_micro, dec_rows, hidden)
        x_pre = x_pre.reshape(n_micro, seg_len, hidden)
        n_rows = dec_rows + seg_len
        _, cache_len, kv_count, head_dim = k_pre.shape
        kv_width = kv_count * head_dim
        q_width = w_q.shape[2]
        ffn = w_gate.shape[2]
        vocab = w_head.shape[1]
        fin_rows = dec_rows + 8 * JOIN

        kd = jnp.transpose(k_dec[0], (0, 1, 3, 4, 2)).reshape(n_micro, dec_rows, kv_width, cache_len)
        vd = jnp.transpose(v_dec[0], (0, 1, 3, 4, 2)).reshape(n_micro, dec_rows, kv_width, cache_len)
        kpre = jnp.transpose(k_pre[0], (1, 2, 0)).reshape(kv_width, cache_len)
        vpre = jnp.transpose(v_pre[0], (1, 2, 0)).reshape(kv_width, cache_len)

        lanes = np.arange(128) % (head_dim // 2)
        inv_freq = jnp.asarray((ROPE_BASE ** (-lanes * (2.0 / head_dim))).astype(np.float32)[None, :])

        def spec(space):
            return pl.BlockSpec(memory_space=space)

        kc, vc, w1, fin, kp, vp = pl.pallas_call(
            functools.partial(pipeline_kernel, n_stages),
            out_shape=(
                VMEM((n_micro, dec_rows, kv_width, cache_len), BF16),
                VMEM((n_micro, dec_rows, kv_width, cache_len), BF16),
                VMEM((hidden, ffn), BF16),
                jax.ShapeDtypeStruct((n_micro, fin_rows, hidden), BF16),
                jax.ShapeDtypeStruct((kv_width, cache_len), BF16),
                jax.ShapeDtypeStruct((kv_width, cache_len), BF16),
            ),
            in_specs=[spec(SMEM)] * 2 + [spec(HBM)] * 18,
            out_specs=(spec(VMEM),) * 3 + (spec(HBM),) * 3,
            scratch_shapes=[
                VMEM((1, 128), F32),
                VMEM((1, hidden), BF16),
                VMEM((1, hidden), BF16),
                VMEM((hidden,), BF16),
                VMEM((hidden, q_width + 2 * kv_width), BF16),
                VMEM((q_width, hidden), BF16),
                VMEM((hidden, ffn), BF16),
                VMEM((ffn, hidden), BF16),
                VMEM((kv_width, cache_len), BF16),
                VMEM((kv_width, cache_len), BF16),
                VMEM((n_micro, n_rows, hidden), BF16),
                VMEM((n_micro, fin_rows, hidden), BF16),
                VMEM((dec_rows * 16, 128), F32),
                VMEM((n_micro, dec_rows, kv_width), F32),
                VMEM((n_micro, dec_rows, kv_width), F32),
                VMEM((n_micro, n_rows, 128), F32),
                VMEM((n_micro, n_rows, 128), F32),
                VMEM((ffn // 256 * n_rows, 256), BF16),
                VMEM((q_width // head_dim // kv_count * seg_len, cache_len), F32),
                pltpu.SemaphoreType.DMA((10,)),
                pltpu.SemaphoreType.DMA((n_micro, 2)),
                pltpu.SemaphoreType.DMA((2,)),
                pltpu.SemaphoreType.DMA((n_micro, 2)),
                pltpu.SemaphoreType.DMA((3,)),
                pltpu.SemaphoreType.DMA((4,)),
                pltpu.SemaphoreType.DMA((n_micro,)),
                pltpu.SemaphoreType.DMA((n_micro,)),
                pltpu.SemaphoreType.DMA((n_micro, n_stages - 1)),
                pltpu.SemaphoreType.DMA((n_micro,)),
            ],
            compiler_params=pltpu.CompilerParams(collective_id=0, has_side_effects=True, vmem_limit_bytes=int(R1_MB * 1024 * 1024)),
            name='pipeline',
        )(dec_len, pre_len, *(pltpu.with_memory_space_constraint(arr, pltpu.HBM) for arr in (
              inv_freq, g_attn, g_mlp, g_final, x_dec, x_pre, w_q[0], w_k[0], w_v[0], w_o[0], w_gate[0], w_up[0], w_down[0], kd, vd, kpre, vpre, w_head)))

        v_blk = 512
        n_slot = 4
        logits, kd_out, vd_out, kp_out, vp_out = pl.pallas_call(
            functools.partial(output_kernel, micros, vocab),
            out_shape=(
                jax.ShapeDtypeStruct((micro_rows + 1, micros, vocab), F32),
                jax.ShapeDtypeStruct(kd.shape, BF16),
                jax.ShapeDtypeStruct(vd.shape, BF16),
                jax.ShapeDtypeStruct(kpre.shape, BF16),
                jax.ShapeDtypeStruct(vpre.shape, BF16),
            ),
            in_specs=[spec(VMEM)] * 3 + [spec(HBM)] * 4,
            out_specs=(spec(HBM),) * 5,
            scratch_shapes=[
                VMEM((hidden, vocab - ffn), BF16),
                VMEM((n_micro, fin_rows, hidden), BF16),
                VMEM((kv_width, cache_len), BF16),
                VMEM((kv_width, cache_len), BF16),
                VMEM((hidden // 128, (micro_rows + 1) * micros, 128), F32),
                VMEM((n_slot, micro_rows + 1, micros, v_blk), F32),
                pltpu.SemaphoreType.DMA((4,)),
                pltpu.SemaphoreType.DMA((4,)),
                pltpu.SemaphoreType.DMA((n_slot,)),
            ],
            compiler_params=pltpu.CompilerParams(vmem_limit_bytes=13 * 1024 * 1024),
            name='output',
        )(kc, vc, w1, pltpu.with_memory_space_constraint(w_head, pltpu.HBM), fin, kp, vp)

        def dec_cache(arr):
            return jnp.transpose(arr.reshape(micros, micro_rows, kv_count, head_dim, cache_len), (0, 1, 4, 2, 3))[None]

        def pre_cache(arr):
            return jnp.transpose(arr.reshape(kv_count, head_dim, cache_len), (2, 0, 1))[None]

        return jnp.transpose(logits, (1, 0, 2)), dec_cache(kd_out), dec_cache(vd_out), pre_cache(kp_out), pre_cache(vp_out)

    return jax.shard_map(device_fn, mesh=mesh, in_specs=in_specs, out_specs=out_specs, check_vma=False)
```

```python
import functools

import jax
import jax.numpy as jnp
import numpy as np
from jax import lax
from jax.experimental import pallas as pl
from jax.experimental.pallas import tpu as pltpu
from jax.sharding import PartitionSpec as P

NORM_EPS = 1e-6
ROPE_BASE = 10000.0
F32 = jnp.float32
BF16 = jnp.bfloat16
NEG = -1e30
HBM = pl.ANY
VMEM = pltpu.VMEM
SMEM = pltpu.SMEM
MESH = pl.DeviceIdType.MESH
R1_MB = 26
JOIN = 2


def rms_norm(acts, gain):
    acts_f = acts.astype(F32)
    inv_rms = lax.rsqrt(jnp.mean(acts_f * acts_f, axis=-1, keepdims=True) + NORM_EPS)
    return (acts_f * inv_rms * gain.astype(F32)).astype(BF16)


def dot(lhs, rhs):
    return jnp.dot(lhs, rhs, preferred_element_type=F32)


def dot_t(lhs, rhs):
    return lax.dot_general(lhs, rhs, (((1,), (1,)), ((), ())), preferred_element_type=F32)


def softmax(scores):
    expd = jnp.exp(scores - jnp.max(scores, axis=-1, keepdims=True))
    return expd * (1.0 / jnp.sum(expd, axis=-1, keepdims=True))


def pipeline_kernel(
    n_stages,
    dec_len, pre_len, inv_freq_in, g_attn_in, g_mlp_in, g_final_in,
    x_dec, x_pre, w_q, w_k, w_v, w_o, w_gate, w_up, w_down, k_dec, v_dec, k_pre, v_pre, w_head,
    kc, vc, w1, fin_out, kp_out, vp_out,
    inv_freq, g_attn, g_mlp, g_final, wqkv, wo, w3, w2, kp, vp, xin, fin, qd, kn, vn, cosv, sinv, hid, sp,
    w_sem, kv_sem, p_sem, x_sem, o_sem, g_sem, send_sem, recv_sem, fsend_sem, frecv_sem, fnext_sem,
):
    n_micro, n_rows, hidden = xin.shape
    dec_rows = x_dec.shape[1]
    seg_len = x_pre.shape[1]
    per_micro = dec_len.shape[1]
    kv_width, cache_len = kp.shape
    q_width = wo.shape[0]
    ffn = w2.shape[0]
    head_dim = 64
    kv_count = kv_width // head_dim
    q_heads = q_width // head_dim
    group = q_heads // kv_count
    stage = lax.axis_index('stage')
    last = n_stages - 1
    half = ffn // 2
    seg_micro = seg_len * per_micro // dec_rows

    barrier = pltpu.get_barrier_semaphore()

    def x_copies(m):
        return (
            pltpu.make_async_copy(x_dec.at[m], xin.at[m, pl.ds(0, dec_rows)], x_sem.at[m, 0]),
            pltpu.make_async_copy(x_pre.at[m], xin.at[m, pl.ds(dec_rows, seg_len)], x_sem.at[m, 1]),
        )

    def k_copy(m):
        return pltpu.make_async_copy(k_dec.at[m], kc.at[m], kv_sem.at[m, 0])

    def v_copy(m):
        return pltpu.make_async_copy(v_dec.at[m], vc.at[m], kv_sem.at[m, 1])

    qkv_copies = (
        pltpu.make_async_copy(w_q, wqkv.at[:, pl.ds(0, q_width)], w_sem.at[0]),
        pltpu.make_async_copy(w_k, wqkv.at[:, pl.ds(q_width, kv_width)], w_sem.at[1]),
        pltpu.make_async_copy(w_v, wqkv.at[:, pl.ds(q_width + kv_width, kv_width)], w_sem.at[2]),
    )
    pre_copies = (
        pltpu.make_async_copy(k_pre, kp, p_sem.at[0]),
        pltpu.make_async_copy(v_pre, vp, p_sem.at[1]),
    )
    wo_copies = (pltpu.make_async_copy(w_o, wo, w_sem.at[3]),)
    up_copies = tuple(
        (
            pltpu.make_async_copy(w_gate.at[:, pl.ds(i * half, half)], w1.at[:, pl.ds(i * half, half)], w_sem.at[4 + 2 * i]),
            pltpu.make_async_copy(w_up.at[:, pl.ds(i * half, half)], w3.at[:, pl.ds(i * half, half)], w_sem.at[5 + 2 * i]),
        )
        for i in range(2)
    )
    head_copies = (pltpu.make_async_copy(w_head.at[:, pl.ds(0, ffn)], w1, w_sem.at[9]),)
    down_copies = (pltpu.make_async_copy(w_down, w2, w_sem.at[8]),)

    gain_copies = [pltpu.make_async_copy(src, dst, g_sem.at[i]) for i, (src, dst) in enumerate((
        (inv_freq_in, inv_freq), (g_attn_in, g_attn), (g_mlp_in, g_mlp), (g_final_in, g_final)))]
    for copy in gain_copies:
        copy.start()

    @pl.when(stage == 0)
    def _():
        for copy in x_copies(0):
            copy.start()
    for copy in qkv_copies + pre_copies + (k_copy(0), v_copy(0)) + wo_copies + up_copies[0] + up_copies[1] + down_copies:
        copy.start()

    @pl.when(stage == 0)
    def _():
        for m in range(1, n_micro):
            for copy in x_copies(m):
                copy.start()
    for m in range(1, n_micro):
        for copy in (k_copy(m), v_copy(m)):
            copy.start()

    @pl.when(stage > 0)
    def _():
        pl.semaphore_signal(barrier, inc=1, device_id={'stage': stage - 1}, device_id_type=MESH)

    fin_first = [last - 1] + list(range(last - 2, 0, -2))
    passes_on = (stage % 2 == 1) & (stage < last)
    ends_chain = (stage % 2 == 0) & (stage < last - 1)

    @pl.when(ends_chain)
    def _():
        pl.semaphore_signal(barrier, inc=1, device_id={'stage': stage + 1}, device_id_type=MESH)

    @pl.when((stage < last) & jnp.logical_not(ends_chain))
    def _():
        pl.semaphore_signal(barrier, inc=1, device_id={'stage': last}, device_id_type=MESH)

    for copy in gain_copies:
        copy.wait()

    lane = lax.broadcasted_iota(jnp.int32, (8, 128), 1)
    row8 = lax.broadcasted_iota(jnp.int32, (8, 128), 0)
    freq = inv_freq[...]
    sign = jnp.where((lane % head_dim) < head_dim // 2, -1.0, 1.0)

    def table_body(m, carry):
        for g in range(n_rows // 8):
            if g < dec_rows // 8:
                pos = jnp.zeros((8, 128), jnp.int32)
                for r in range(8):
                    pos = jnp.where(row8 == r, dec_len[m * (dec_rows // per_micro) + (g * 8 + r) // per_micro, (g * 8 + r) % per_micro], pos)
            else:
                pos = pre_len[0] + m * seg_len + (g * 8 - dec_rows) + row8
            angle = pos.astype(F32) * freq
            cosv[m, pl.ds(g * 8, 8), :] = jnp.cos(angle)
            sinv[m, pl.ds(g * 8, 8), :] = jnp.sin(angle) * sign
        return carry

    lax.fori_loop(0, n_micro, table_body, 0)
    qd[...] = jnp.zeros(qd.shape, F32)

    @pl.when((stage < last) & jnp.logical_not(passes_on))
    def _():
        pl.semaphore_wait(barrier, 1)

    @pl.when(passes_on)
    def _():
        pl.semaphore_wait(barrier, 2)

    @pl.when(stage == last)
    def _():
        pl.semaphore_wait(barrier, len(fin_first))

    def x_send(m):
        return pltpu.make_async_remote_copy(
            src_ref=xin.at[m], dst_ref=xin.at[m], send_sem=send_sem.at[m], recv_sem=recv_sem.at[m],
            device_id={'stage': jnp.minimum(stage + 1, last)}, device_id_type=MESH)

    def fin_send(m, target):
        return pltpu.make_async_remote_copy(
            src_ref=fin.at[m], dst_ref=fin.at[m], send_sem=fsend_sem.at[m, target], recv_sem=frecv_sem.at[m],
            device_id={'stage': target}, device_id_type=MESH)

    def tick(loading, m, carry):
        def wait_first(copies):
            if loading:
                @pl.when(m == 0)
                def _():
                    for copy in copies:
                        copy.wait()

        if loading:
            for copy in x_copies(m):
                copy.wait()
        else:
            x_send(m).wait_recv()
        wait_first(qkv_copies + pre_copies)

        acts = xin[m]
        normed = rms_norm(acts, g_attn[...])
        cosine = cosv[m]
        sine = sinv[m]
        lane_q = lax.broadcasted_iota(jnp.int32, (n_rows, 128), 1)
        low32 = (lane_q % head_dim) < head_dim // 2
        low_half = lax.broadcasted_iota(jnp.int32, (dec_rows, 128), 1) < head_dim

        def rotate(tile):
            swapped = jnp.where(low32, pltpu.roll(tile, 128 - head_dim // 2, 1), pltpu.roll(tile, head_dim // 2, 1))
            return tile * cosine + swapped * sine

        proj = dot(normed, wqkv[...])
        q_tiles = [rotate(proj[:, t * 128:(t + 1) * 128]).astype(BF16).astype(F32) for t in range(q_width // 128)]
        k_new = rotate(proj[:, q_width:q_width + kv_width]).astype(BF16)
        v_new = proj[:, q_width + kv_width:].astype(BF16)
        kn[m] = k_new[:dec_rows].astype(F32)
        vn[m] = v_new[:dec_rows].astype(F32)

        for j in range(q_heads):
            tile = q_tiles[j // 2][:dec_rows]
            if j % 2 != j // group:
                tile = pltpu.roll(tile, head_dim, 1)
            keep = low_half if j // group == 0 else jnp.logical_not(low_half)
            qd[pl.ds(j, dec_rows, stride=16), :] = jnp.where(keep, tile, 0.0)

        pre_begin = pre_len[0] + m * seg_len
        seg_row = lax.broadcasted_iota(jnp.int32, (seg_len, cache_len), 0)
        seg_col = lax.broadcasted_iota(jnp.int32, (seg_len, cache_len), 1)
        spread = (seg_col == seg_row + pre_begin).astype(F32).astype(BF16)
        col = lax.broadcasted_iota(jnp.int32, (kv_width, cache_len), 1)
        written = (col >= pre_begin) & (col < pre_begin + seg_len)
        contract0 = (((0,), (0,)), ((), ()))
        k_put = lax.dot_general(k_new[dec_rows:], spread, contract0, preferred_element_type=F32)
        v_put = lax.dot_general(v_new[dec_rows:], spread, contract0, preferred_element_type=F32)
        kp_f = jnp.where(written, k_put, kp[...].astype(F32)).astype(BF16)
        vp_f = jnp.where(written, v_put, vp[...].astype(F32)).astype(BF16)
        kp[...] = kp_f
        vp[...] = vp_f

        scale = head_dim ** -0.5
        pre_valid = seg_col <= seg_row + pre_begin
        span = group * seg_len
        pd_base = q_heads * seg_len
        for g in range(kv_count):
            rows = []
            for j in range(g * group, (g + 1) * group):
                keep = low_half if j % 2 == 0 else jnp.logical_not(low_half)
                rows.append(jnp.where(keep, q_tiles[j // 2][dec_rows:], 0.0).astype(BF16))
            k_g = kp_f[g * head_dim:(g + 1) * head_dim]
            sp[...] = dot(jnp.concatenate(rows, axis=0), jnp.concatenate([k_g, k_g], axis=0))
            for j in range(group):
                scores = sp[j * seg_len:(j + 1) * seg_len, :] * scale
                base = (g * group + j) * seg_len
                hid[base:base + seg_len, :] = softmax(jnp.where(pre_valid, scores, NEG)).astype(BF16)

        if loading:
            k_copy(m).wait()
        pos_lane = lax.broadcasted_iota(jnp.int32, (16, cache_len), 1)
        for b in range(dec_rows):
            pos = dec_len[m * (dec_rows // per_micro) + b // per_micro, b % per_micro]
            q_b = qd[b * 16:(b + 1) * 16, :]
            s_old = dot(q_b.astype(BF16), kc[m, b]) * scale
            s_new = jnp.sum(q_b * kn[m, b:b + 1, :], axis=-1, keepdims=True) * scale
            here = pos_lane == pos
            scores = jnp.where(here, s_new, jnp.where(pos_lane < pos, s_old, NEG))
            peak = jnp.max(scores, axis=-1, keepdims=True)
            expd = jnp.exp(scores - peak)
            inv = 1.0 / jnp.sum(expd, axis=-1, keepdims=True)
            hid[pd_base + b * 16:pd_base + (b + 1) * 16, :] = jnp.where(here, 0.0, expd * inv).astype(BF16)
            p_new = (jnp.exp(s_new - peak) * inv).astype(BF16).astype(F32)
            qd[b * 16:(b + 1) * 16, :] = p_new * vn[m, b:b + 1, :]

        pre_heads = []
        for g in range(kv_count):
            v_g = vp_f[g * head_dim:(g + 1) * head_dim]
            mixed = dot_t(hid[g * span:(g + 1) * span, :], jnp.concatenate([v_g, v_g], axis=0))
            pre_heads += [mixed[i * seg_len:(i + 1) * seg_len] for i in range(group)]
        if loading:
            v_copy(m).wait()
        for b in range(dec_rows):
            qd[b * 16:(b + 1) * 16, :] += dot_t(hid[pd_base + b * 16:pd_base + (b + 1) * 16, :], vc[m, b])

        att_tiles = []
        for t in range(q_width // 128):
            parts = []
            for j in (2 * t, 2 * t + 1):
                part = qd[pl.ds(j, dec_rows, stride=16), :]
                if j % 2 != j // group:
                    part = pltpu.roll(part, head_dim, 1)
                parts.append(part)
            dec_tile = jnp.where(low_half, parts[0], parts[1])
            pre_tile = jnp.where(low_half, pre_heads[2 * t], pre_heads[2 * t + 1])
            att_tiles.append(jnp.concatenate([dec_tile, pre_tile], axis=0).astype(BF16))
        att = jnp.concatenate(att_tiles, axis=1)

        wait_first(wo_copies)

        acts = (acts.astype(F32) + dot(att, wo[...])).astype(BF16)
        normed = rms_norm(acts, g_mlp[...])

        n_blk = 256
        for i in range(2):
            wait_first(up_copies[i])
            lo = 0 if i == 0 else half // n_blk * n_blk
            hi = half // n_blk * n_blk if i == 0 else ffn
            for n in range(lo, hi, n_blk):
                gate = dot(normed, w1[:, n:n + n_blk])
                up = dot(normed, w3[:, n:n + n_blk])
                k = n // n_blk
                hid[k * n_rows:(k + 1) * n_rows, :] = (jax.nn.silu(gate) * up).astype(BF16)

        wait_first(down_copies)
        hidden_act = jnp.concatenate([hid[k * n_rows:(k + 1) * n_rows, :] for k in range(ffn // n_blk)], axis=1)
        acts = (acts.astype(F32) + dot(hidden_act, w2[...])).astype(BF16)

        def send_rows():
            xin[m] = acts
            x_send(m).start()

        def send_final():
            ends = [acts[dec_rows + e - 8:dec_rows + e].astype(F32) for e in range(seg_micro, seg_len + 1, seg_micro)]
            row = lax.broadcasted_iota(jnp.int32, (8, hidden), 0)
            kept = ends[-1]
            for i, rows in enumerate(ends[:-1]):
                shift = len(ends) - 1 - i
                kept = jnp.where(row == 7 - shift, pltpu.roll(rows, 8 - shift, 0), kept)
            tail = jnp.concatenate([acts[:dec_rows], kept.astype(BF16)], axis=0)
            fin[m] = rms_norm(tail, g_final[...].astype(F32)[None, :])
            for target in fin_first:
                fin_send(m, target).start()

        if loading:
            send_rows()
        else:
            pl.when(stage < last)(send_rows)
            pl.when(stage == last)(send_final)
        return carry

    @pl.when(stage == 0)
    def _():
        lax.fori_loop(0, n_micro, functools.partial(tick, True), 0)

    @pl.when(stage > 0)
    def _():
        for copy in qkv_copies + pre_copies + wo_copies + up_copies[0] + up_copies[1] + down_copies:
            copy.wait()
        for m in range(n_micro):
            k_copy(m).wait()
            v_copy(m).wait()
        lax.fori_loop(0, n_micro, functools.partial(tick, False), 0)

    for copy in head_copies:
        copy.start()

    pre_out = (pltpu.make_async_copy(kp, kp_out, o_sem.at[0]), pltpu.make_async_copy(vp, vp_out, o_sem.at[1]))
    for copy in pre_out:
        copy.start()

    col_full = lax.broadcasted_iota(jnp.int32, (kv_width, cache_len), 1)

    def patch(m, carry):
        for new, cache in ((kn, kc), (vn, vc)):
            cols = jnp.transpose(new[m])
            for b in range(dec_rows):
                pos = dec_len[m * (dec_rows // per_micro) + b // per_micro, b % per_micro]
                column = jnp.broadcast_to(cols[:, b:b + 1], (kv_width, cache_len)).astype(BF16)
                cache[m, b] = jnp.where(col_full == pos, column, cache[m, b])
        return carry

    lax.fori_loop(0, n_micro, patch, 0)

    @pl.when(stage < last)
    def _():
        for m in range(n_micro):
            x_send(m).wait_send()

    def fin_next(m):
        return pltpu.make_async_remote_copy(
            src_ref=fin.at[m], dst_ref=fin.at[m], send_sem=fnext_sem.at[m], recv_sem=frecv_sem.at[m],
            device_id={'stage': jnp.maximum(stage - 1, 0)}, device_id_type=MESH)

    @pl.when(passes_on)
    def _():
        for m in range(n_micro):
            fin_next(m).wait_recv()
            fin_next(m).start()
        for m in range(n_micro):
            fin_next(m).wait_send()

    @pl.when((stage < last) & jnp.logical_not(passes_on))
    def _():
        for m in range(n_micro):
            fin_next(m).wait_recv()

    @pl.when(stage == last)
    def _():
        for m in range(n_micro):
            for target in fin_first:
                fin_send(m, target).wait_send()

    fin_copy = pltpu.make_async_copy(fin, fin_out, o_sem.at[2])
    fin_copy.start()
    for copy in pre_out:
        copy.wait()
    fin_copy.wait()
    for copy in head_copies:
        copy.wait()


def output_kernel(micros, vocab, kc, vc, w_low, w_all, fin_in, kp_in, vp_in, logits, kc_out, vc_out, kp_out, vp_out, w_high, fin, kp, vp, rows, stage_buf, i_sem, c_sem, l_sem):
    n_chunk = fin.shape[0]
    n_kept = logits.shape[0]
    join = micros // n_chunk
    n_slot, _, _, v_blk = stage_buf.shape
    copies = [pltpu.make_async_copy(src, dst, c_sem.at[i]) for i, (src, dst) in enumerate(((kc, kc_out), (vc, vc_out), (kp, kp_out), (vp, vp_out)))]
    loads = [pltpu.make_async_copy(src, dst, i_sem.at[i]) for i, (src, dst) in enumerate(((fin_in, fin), (kp_in, kp), (vp_in, vp)))]
    low = w_low.shape[1]
    w_load = pltpu.make_async_copy(w_all.at[:, pl.ds(low, vocab - low)], w_high, i_sem.at[3])
    for copy in loads + [w_load] + copies[:2]:
        copy.start()
    for copy in loads:
        copy.wait()
    for copy in copies[2:]:
        copy.start()

    for m in range(micros):
        kept = fin[m // join].astype(F32)
        first = (m % join) * (n_kept - 1)
        last = fin.shape[1] - join + m % join
        for t in range(rows.shape[0]):
            tile = kept[:, t * 128:(t + 1) * 128]
            rows[t, pl.ds(m, n_kept - 1, stride=micros), :] = tile[first:first + n_kept - 1]
            rows[t, (n_kept - 1) * micros + m:(n_kept - 1) * micros + m + 1, :] = tile[last:last + 1]
    lhs = jnp.concatenate([rows[t].astype(BF16) for t in range(rows.shape[0])], axis=1)

    blocks = [(w_low, 0, n, min(v_blk, low - n)) for n in range(0, low, v_blk)]
    blocks += [(w_high, low, n, min(v_blk, vocab - low - n)) for n in range(0, vocab - low, v_blk)]

    def store(i):
        _, base, n, width = blocks[i]
        return pltpu.make_async_copy(
            stage_buf.at[i % n_slot, :, :, pl.ds(0, width)], logits.at[:, :, pl.ds(base + n, width)], l_sem.at[i % n_slot])

    for i, (w_ref, base, n, width) in enumerate(blocks):
        if i >= n_slot:
            store(i - n_slot).wait()
        if base and n == 0:
            w_load.wait()
        out = dot(lhs, w_ref[:, n:n + width])
        for r in range(n_kept):
            stage_buf[i % n_slot, r, :, :width] = out[r * micros:(r + 1) * micros]
        store(i).start()
    for i in range(len(blocks) - n_slot, len(blocks)):
        store(i).wait()
    for copy in copies:
        copy.wait()


def solution(mesh):
    n_stages = mesh.shape['stage']
    part_spec = P('replica')
    layer_spec = P('stage')
    cache_spec = P('stage', 'replica')
    in_specs = (part_spec,) * 4 + (layer_spec,) * 9 + (P(), P()) + (cache_spec,) * 4
    out_specs = (part_spec,) + (cache_spec,) * 4

    def device_fn(x_dec, x_pre, dec_len, pre_len, g_attn, w_q, w_k, w_v, w_o, g_mlp, w_gate, w_up, w_down, g_final, w_head, k_dec, v_dec, k_pre, v_pre):
        micros, micro_rows, hidden = x_dec.shape
        n_micro = micros // JOIN
        dec_rows = micro_rows * JOIN
        seg_len = x_pre.shape[1] * JOIN
        x_dec = x_dec.reshape(n_micro, dec_rows, hidden)
        x_pre = x_pre.reshape(n_micro, seg_len, hidden)
        n_rows = dec_rows + seg_len
        _, cache_len, kv_count, head_dim = k_pre.shape
        kv_width = kv_count * head_dim
        q_width = w_q.shape[2]
        ffn = w_gate.shape[2]
        vocab = w_head.shape[1]
        fin_rows = dec_rows + 8

        kd = jnp.transpose(k_dec[0], (0, 1, 3, 4, 2)).reshape(n_micro, dec_rows, kv_width, cache_len)
        vd = jnp.transpose(v_dec[0], (0, 1, 3, 4, 2)).reshape(n_micro, dec_rows, kv_width, cache_len)
        kpre = jnp.transpose(k_pre[0], (1, 2, 0)).reshape(kv_width, cache_len)
        vpre = jnp.transpose(v_pre[0], (1, 2, 0)).reshape(kv_width, cache_len)

        lanes = np.arange(128) % (head_dim // 2)
        inv_freq = jnp.asarray((ROPE_BASE ** (-lanes * (2.0 / head_dim))).astype(np.float32)[None, :])

        def spec(space):
            return pl.BlockSpec(memory_space=space)

        kc, vc, w1, fin, kp, vp = pl.pallas_call(
            functools.partial(pipeline_kernel, n_stages),
            out_shape=(
                VMEM((n_micro, dec_rows, kv_width, cache_len), BF16),
                VMEM((n_micro, dec_rows, kv_width, cache_len), BF16),
                VMEM((hidden, ffn), BF16),
                jax.ShapeDtypeStruct((n_micro, fin_rows, hidden), BF16),
                jax.ShapeDtypeStruct((kv_width, cache_len), BF16),
                jax.ShapeDtypeStruct((kv_width, cache_len), BF16),
            ),
            in_specs=[spec(SMEM)] * 2 + [spec(HBM)] * 18,
            out_specs=(spec(VMEM),) * 3 + (spec(HBM),) * 3,
            scratch_shapes=[
                VMEM((1, 128), F32),
                VMEM((1, hidden), BF16),
                VMEM((1, hidden), BF16),
                VMEM((hidden,), BF16),
                VMEM((hidden, q_width + 2 * kv_width), BF16),
                VMEM((q_width, hidden), BF16),
                VMEM((hidden, ffn), BF16),
                VMEM((ffn, hidden), BF16),
                VMEM((kv_width, cache_len), BF16),
                VMEM((kv_width, cache_len), BF16),
                VMEM((n_micro, n_rows, hidden), BF16),
                VMEM((n_micro, fin_rows, hidden), BF16),
                VMEM((dec_rows * 16, 128), F32),
                VMEM((n_micro, dec_rows, kv_width), F32),
                VMEM((n_micro, dec_rows, kv_width), F32),
                VMEM((n_micro, n_rows, 128), F32),
                VMEM((n_micro, n_rows, 128), F32),
                VMEM((ffn // 256 * n_rows, 256), BF16),
                VMEM((q_width // head_dim // kv_count * seg_len, cache_len), F32),
                pltpu.SemaphoreType.DMA((10,)),
                pltpu.SemaphoreType.DMA((n_micro, 2)),
                pltpu.SemaphoreType.DMA((2,)),
                pltpu.SemaphoreType.DMA((n_micro, 2)),
                pltpu.SemaphoreType.DMA((3,)),
                pltpu.SemaphoreType.DMA((4,)),
                pltpu.SemaphoreType.DMA((n_micro,)),
                pltpu.SemaphoreType.DMA((n_micro,)),
                pltpu.SemaphoreType.DMA((n_micro, n_stages - 1)),
                pltpu.SemaphoreType.DMA((n_micro,)),
                pltpu.SemaphoreType.DMA((n_micro,)),
            ],
            compiler_params=pltpu.CompilerParams(collective_id=0, has_side_effects=True, vmem_limit_bytes=int(R1_MB * 1024 * 1024)),
            name='pipeline',
        )(dec_len, pre_len, *(pltpu.with_memory_space_constraint(arr, pltpu.HBM) for arr in (
              inv_freq, g_attn, g_mlp, g_final, x_dec, x_pre, w_q[0], w_k[0], w_v[0], w_o[0], w_gate[0], w_up[0], w_down[0], kd, vd, kpre, vpre, w_head)))

        v_blk = 512
        n_slot = -(-ffn // v_blk) - (ffn - vocab) // v_blk
        logits, kd_out, vd_out, kp_out, vp_out = pl.pallas_call(
            functools.partial(output_kernel, micros, vocab),
            out_shape=(
                jax.ShapeDtypeStruct((micro_rows + 1, micros, vocab), F32),
                jax.ShapeDtypeStruct(kd.shape, BF16),
                jax.ShapeDtypeStruct(vd.shape, BF16),
                jax.ShapeDtypeStruct(kpre.shape, BF16),
                jax.ShapeDtypeStruct(vpre.shape, BF16),
            ),
            in_specs=[spec(VMEM)] * 3 + [spec(HBM)] * 4,
            out_specs=(spec(HBM),) * 5,
            scratch_shapes=[
                VMEM((hidden, vocab - ffn), BF16),
                VMEM((n_micro, fin_rows, hidden), BF16),
                VMEM((kv_width, cache_len), BF16),
                VMEM((kv_width, cache_len), BF16),
                VMEM((hidden // 128, (micro_rows + 1) * micros, 128), F32),
                VMEM((n_slot, micro_rows + 1, micros, v_blk), F32),
                pltpu.SemaphoreType.DMA((4,)),
                pltpu.SemaphoreType.DMA((4,)),
                pltpu.SemaphoreType.DMA((n_slot,)),
            ],
            compiler_params=pltpu.CompilerParams(vmem_limit_bytes=14 * 1024 * 1024),
            name='output',
        )(kc, vc, w1, pltpu.with_memory_space_constraint(w_head, pltpu.HBM), fin, kp, vp)

        def dec_cache(arr):
            return jnp.transpose(arr.reshape(micros, micro_rows, kv_count, head_dim, cache_len), (0, 1, 4, 2, 3))[None]

        def pre_cache(arr):
            return jnp.transpose(arr.reshape(kv_count, head_dim, cache_len), (2, 0, 1))[None]

        return jnp.transpose(logits, (1, 0, 2)), dec_cache(kd_out), dec_cache(vd_out), pre_cache(kp_out), pre_cache(vp_out)

    return jax.shard_map(device_fn, mesh=mesh, in_specs=in_specs, out_specs=out_specs, check_vma=False)
```

```python
import functools

import jax
import jax.numpy as jnp
import numpy as np
from jax import lax
from jax.experimental import pallas as pl
from jax.experimental.pallas import tpu as pltpu
from jax.sharding import PartitionSpec as P

NORM_EPS = 1e-6
ROPE_BASE = 10000.0
F32 = jnp.float32
BF16 = jnp.bfloat16
NEG = -1e30
HBM = pl.ANY
VMEM = pltpu.VMEM
SMEM = pltpu.SMEM
MESH = pl.DeviceIdType.MESH
R1_MB = 21.5
JOIN = 2


def rms_norm(acts, gain):
    acts_f = acts.astype(F32)
    inv_rms = lax.rsqrt(jnp.mean(acts_f * acts_f, axis=-1, keepdims=True) + NORM_EPS)
    return (acts_f * inv_rms * gain.astype(F32)).astype(BF16)


def dot(lhs, rhs):
    return jnp.dot(lhs, rhs, preferred_element_type=F32)


def dot_t(lhs, rhs):
    return lax.dot_general(lhs, rhs, (((1,), (1,)), ((), ())), preferred_element_type=F32)


def softmax(scores):
    expd = jnp.exp(scores - jnp.max(scores, axis=-1, keepdims=True))
    return expd * (1.0 / jnp.sum(expd, axis=-1, keepdims=True))


def pipeline_kernel(
    n_stages,
    dec_len, pre_len, inv_freq_in, g_attn_in, g_mlp_in, g_final_in,
    x_dec, x_pre, w_q, w_k, w_v, w_o, w_gate, w_up, w_down, k_dec, v_dec, k_pre, v_pre, w_head,
    kc, vc, w1, w3, fin_out, kp_out, vp_out,
    inv_freq, g_attn, g_mlp, g_final, wqkv, wo, w2, kp, vp, xin, fin, qd, kn, vn, cosv, sinv, hid, sp,
    w_sem, kv_sem, p_sem, x_sem, o_sem, g_sem, send_sem, recv_sem, fsend_sem, frecv_sem, fnext_sem,
):
    n_micro, n_rows, hidden = xin.shape
    dec_rows = x_dec.shape[1]
    seg_len = x_pre.shape[1]
    per_micro = dec_len.shape[1]
    kv_width, cache_len = kp.shape
    q_width = wo.shape[0]
    ffn = w2.shape[0]
    head_dim = 64
    kv_count = kv_width // head_dim
    q_heads = q_width // head_dim
    group = q_heads // kv_count
    stage = lax.axis_index('stage')
    last = n_stages - 1
    half = ffn // 2
    seg_micro = seg_len * per_micro // dec_rows

    barrier = pltpu.get_barrier_semaphore()

    def x_copies(m):
        return (
            pltpu.make_async_copy(x_dec.at[m], xin.at[m, pl.ds(0, dec_rows)], x_sem.at[m, 0]),
            pltpu.make_async_copy(x_pre.at[m], xin.at[m, pl.ds(dec_rows, seg_len)], x_sem.at[m, 1]),
        )

    def k_copy(m):
        return pltpu.make_async_copy(k_dec.at[m], kc.at[m], kv_sem.at[m, 0])

    def v_copy(m):
        return pltpu.make_async_copy(v_dec.at[m], vc.at[m], kv_sem.at[m, 1])

    qkv_copies = (
        pltpu.make_async_copy(w_q, wqkv.at[:, pl.ds(0, q_width)], w_sem.at[0]),
        pltpu.make_async_copy(w_k, wqkv.at[:, pl.ds(q_width, kv_width)], w_sem.at[1]),
        pltpu.make_async_copy(w_v, wqkv.at[:, pl.ds(q_width + kv_width, kv_width)], w_sem.at[2]),
    )
    pre_copies = (
        pltpu.make_async_copy(k_pre, kp, p_sem.at[0]),
        pltpu.make_async_copy(v_pre, vp, p_sem.at[1]),
    )
    wo_copies = (pltpu.make_async_copy(w_o, wo, w_sem.at[3]),)
    up_copies = tuple(
        (
            pltpu.make_async_copy(w_gate.at[:, pl.ds(i * half, half)], w1.at[:, pl.ds(i * half, half)], w_sem.at[4 + 2 * i]),
            pltpu.make_async_copy(w_up.at[:, pl.ds(i * half, half)], w3.at[:, pl.ds(i * half, half)], w_sem.at[5 + 2 * i]),
        )
        for i in range(2)
    )
    rest = w_head.shape[1] - ffn
    head_copies = (
        pltpu.make_async_copy(w_head.at[:, pl.ds(0, ffn)], w1, w_sem.at[9]),
        pltpu.make_async_copy(w_head.at[:, pl.ds(ffn, rest)], w3.at[:, pl.ds(0, rest)], w_sem.at[10]),
    )
    cut = ffn // 512 * 256 + 256
    down_copies = tuple(
        pltpu.make_async_copy(w_down.at[pl.ds(lo, size)], w2.at[pl.ds(lo, size)], w_sem.at[sem])
        for lo, size, sem in ((0, cut, 8), (cut, ffn - cut, 11)))

    gain_copies = [pltpu.make_async_copy(src, dst, g_sem.at[i]) for i, (src, dst) in enumerate((
        (inv_freq_in, inv_freq), (g_attn_in, g_attn), (g_mlp_in, g_mlp), (g_final_in, g_final)))]
    for copy in gain_copies:
        copy.start()

    @pl.when(stage == 0)
    def _():
        for copy in x_copies(0):
            copy.start()
    for copy in qkv_copies + pre_copies + (k_copy(0), v_copy(0)) + wo_copies + up_copies[0] + up_copies[1] + down_copies:
        copy.start()

    @pl.when(stage == 0)
    def _():
        for m in range(1, n_micro):
            for copy in x_copies(m):
                copy.start()
    for m in range(1, n_micro):
        for copy in (k_copy(m), v_copy(m)):
            copy.start()

    @pl.when(stage > 0)
    def _():
        pl.semaphore_signal(barrier, inc=1, device_id={'stage': stage - 1}, device_id_type=MESH)

    fin_first = [last - 1] + list(range(last - 2, 0, -2))
    passes_on = (stage % 2 == 1) & (stage < last)
    ends_chain = (stage % 2 == 0) & (stage < last - 1)

    @pl.when(ends_chain)
    def _():
        pl.semaphore_signal(barrier, inc=1, device_id={'stage': stage + 1}, device_id_type=MESH)

    @pl.when((stage < last) & jnp.logical_not(ends_chain))
    def _():
        pl.semaphore_signal(barrier, inc=1, device_id={'stage': last}, device_id_type=MESH)

    for copy in gain_copies:
        copy.wait()

    lane = lax.broadcasted_iota(jnp.int32, (8, 128), 1)
    row8 = lax.broadcasted_iota(jnp.int32, (8, 128), 0)
    freq = inv_freq[...]
    sign = jnp.where((lane % head_dim) < head_dim // 2, -1.0, 1.0)

    def table_body(m, carry):
        for g in range(n_rows // 8):
            if g < dec_rows // 8:
                pos = jnp.zeros((8, 128), jnp.int32)
                for r in range(8):
                    pos = jnp.where(row8 == r, dec_len[m * (dec_rows // per_micro) + (g * 8 + r) // per_micro, (g * 8 + r) % per_micro], pos)
            else:
                pos = pre_len[0] + m * seg_len + (g * 8 - dec_rows) + row8
            angle = pos.astype(F32) * freq
            cosv[m, pl.ds(g * 8, 8), :] = jnp.cos(angle)
            sinv[m, pl.ds(g * 8, 8), :] = jnp.sin(angle) * sign
        return carry

    lax.fori_loop(0, n_micro, table_body, 0)
    qd[...] = jnp.zeros(qd.shape, F32)

    @pl.when((stage < last) & jnp.logical_not(passes_on))
    def _():
        pl.semaphore_wait(barrier, 1)

    @pl.when(passes_on)
    def _():
        pl.semaphore_wait(barrier, 2)

    @pl.when(stage == last)
    def _():
        pl.semaphore_wait(barrier, len(fin_first))

    def x_send(m):
        return pltpu.make_async_remote_copy(
            src_ref=xin.at[m], dst_ref=xin.at[m], send_sem=send_sem.at[m], recv_sem=recv_sem.at[m],
            device_id={'stage': jnp.minimum(stage + 1, last)}, device_id_type=MESH)

    def fin_send(m, target):
        return pltpu.make_async_remote_copy(
            src_ref=fin.at[m], dst_ref=fin.at[m], send_sem=fsend_sem.at[m, target], recv_sem=frecv_sem.at[m],
            device_id={'stage': target}, device_id_type=MESH)

    def tick(loading, m, carry):
        def wait_first(copies):
            if loading:
                @pl.when(m == 0)
                def _():
                    for copy in copies:
                        copy.wait()

        if loading:
            for copy in x_copies(m):
                copy.wait()
        else:
            x_send(m).wait_recv()
        wait_first(qkv_copies + pre_copies)

        acts = xin[m]
        normed = rms_norm(acts, g_attn[...])
        cosine = cosv[m]
        sine = sinv[m]
        lane_q = lax.broadcasted_iota(jnp.int32, (n_rows, 128), 1)
        low32 = (lane_q % head_dim) < head_dim // 2
        low_half = lax.broadcasted_iota(jnp.int32, (dec_rows, 128), 1) < head_dim

        def rotate(tile):
            swapped = jnp.where(low32, pltpu.roll(tile, 128 - head_dim // 2, 1), pltpu.roll(tile, head_dim // 2, 1))
            return tile * cosine + swapped * sine

        proj = dot(normed, wqkv[...])
        q_tiles = [rotate(proj[:, t * 128:(t + 1) * 128]).astype(BF16).astype(F32) for t in range(q_width // 128)]
        k_new = rotate(proj[:, q_width:q_width + kv_width]).astype(BF16)
        v_new = proj[:, q_width + kv_width:].astype(BF16)
        kn[m] = k_new[:dec_rows].astype(F32)
        vn[m] = v_new[:dec_rows].astype(F32)

        for j in range(q_heads):
            tile = q_tiles[j // 2][:dec_rows]
            if j % 2 != j // group:
                tile = pltpu.roll(tile, head_dim, 1)
            keep = low_half if j // group == 0 else jnp.logical_not(low_half)
            qd[pl.ds(j, dec_rows, stride=16), :] = jnp.where(keep, tile, 0.0)

        pre_begin = pre_len[0] + m * seg_len
        seg_row = lax.broadcasted_iota(jnp.int32, (seg_len, cache_len), 0)
        seg_col = lax.broadcasted_iota(jnp.int32, (seg_len, cache_len), 1)
        spread = (seg_col == seg_row + pre_begin).astype(F32).astype(BF16)
        col = lax.broadcasted_iota(jnp.int32, (kv_width, cache_len), 1)
        written = (col >= pre_begin) & (col < pre_begin + seg_len)
        contract0 = (((0,), (0,)), ((), ()))
        k_put = lax.dot_general(k_new[dec_rows:], spread, contract0, preferred_element_type=F32)
        v_put = lax.dot_general(v_new[dec_rows:], spread, contract0, preferred_element_type=F32)
        kp_f = jnp.where(written, k_put, kp[...].astype(F32)).astype(BF16)
        vp_f = jnp.where(written, v_put, vp[...].astype(F32)).astype(BF16)
        kp[...] = kp_f
        vp[...] = vp_f

        scale = head_dim ** -0.5
        pre_valid = seg_col <= seg_row + pre_begin
        span = group * seg_len
        pd_base = q_heads * seg_len
        for g in range(kv_count):
            rows = []
            for j in range(g * group, (g + 1) * group):
                keep = low_half if j % 2 == 0 else jnp.logical_not(low_half)
                rows.append(jnp.where(keep, q_tiles[j // 2][dec_rows:], 0.0).astype(BF16))
            k_g = kp_f[g * head_dim:(g + 1) * head_dim]
            sp[g * span:(g + 1) * span, :] = dot(jnp.concatenate(rows, axis=0), jnp.concatenate([k_g, k_g], axis=0))

        if loading:
            k_copy(m).wait()
        pos_lane = lax.broadcasted_iota(jnp.int32, (16, cache_len), 1)
        for b in range(dec_rows):
            pos = dec_len[m * (dec_rows // per_micro) + b // per_micro, b % per_micro]
            q_b = qd[b * 16:(b + 1) * 16, :]
            s_old = jnp.where(pos_lane < pos, dot(q_b.astype(BF16), kc[m, b]) * scale, NEG)
            s_new = jnp.sum(q_b * kn[m, b:b + 1, :], axis=-1, keepdims=True) * scale
            peak = jnp.maximum(jnp.max(s_old, axis=-1, keepdims=True), s_new)
            expd = jnp.exp(s_old - peak)
            e_new = jnp.exp(s_new - peak)
            inv = 1.0 / (jnp.sum(expd, axis=-1, keepdims=True) + e_new)
            hid[pd_base + b * 16:pd_base + (b + 1) * 16, :] = (expd * inv).astype(BF16)
            p_new = (e_new * inv).astype(BF16).astype(F32)
            qd[b * 16:(b + 1) * 16, :] = p_new * vn[m, b:b + 1, :]

        if loading:
            v_copy(m).wait()
        for j in range(q_heads):
            scores = sp[j * seg_len:(j + 1) * seg_len, :] * scale
            hid[j * seg_len:(j + 1) * seg_len, :] = softmax(jnp.where(pre_valid, scores, NEG)).astype(BF16)
        for b in range(dec_rows):
            qd[b * 16:(b + 1) * 16, :] += dot_t(hid[pd_base + b * 16:pd_base + (b + 1) * 16, :], vc[m, b])
        pre_heads = []
        for g in range(kv_count):
            v_g = vp_f[g * head_dim:(g + 1) * head_dim]
            mixed = dot_t(hid[g * span:(g + 1) * span, :], jnp.concatenate([v_g, v_g], axis=0))
            pre_heads += [mixed[i * seg_len:(i + 1) * seg_len] for i in range(group)]


        att_tiles = []
        for t in range(q_width // 128):
            parts = []
            for j in (2 * t, 2 * t + 1):
                part = qd[pl.ds(j, dec_rows, stride=16), :]
                if j % 2 != j // group:
                    part = pltpu.roll(part, head_dim, 1)
                parts.append(part)
            dec_tile = jnp.where(low_half, parts[0], parts[1])
            pre_tile = jnp.where(low_half, pre_heads[2 * t], pre_heads[2 * t + 1])
            att_tiles.append(jnp.concatenate([dec_tile, pre_tile], axis=0).astype(BF16))
        att = jnp.concatenate(att_tiles, axis=1)

        wait_first(wo_copies)

        acts = (acts.astype(F32) + dot(att, wo[...])).astype(BF16)
        normed = rms_norm(acts, g_mlp[...])

        n_blk = 256
        for i in range(2):
            wait_first(up_copies[i])
            lo = 0 if i == 0 else half // n_blk * n_blk
            hi = half // n_blk * n_blk if i == 0 else ffn
            for n in range(lo, hi, n_blk):
                gate = dot(normed, w1[:, n:n + n_blk])
                up = dot(normed, w3[:, n:n + n_blk])
                k = n // n_blk
                hid[k * n_rows:(k + 1) * n_rows, :] = (jax.nn.silu(gate) * up).astype(BF16)

        def act_blocks(lo, hi):
            return jnp.concatenate([hid[k * n_rows:(k + 1) * n_rows, :] for k in range(lo // n_blk, hi // n_blk)], axis=1)

        if loading:
            wait_first(down_copies[:1])
            down = dot(act_blocks(0, cut), w2[:cut, :])
            wait_first(down_copies[1:])
            down = down + dot(act_blocks(cut, ffn), w2[cut:, :])
        else:
            down = dot(act_blocks(0, ffn), w2[...])
        acts = (acts.astype(F32) + down).astype(BF16)

        def send_rows():
            xin[m] = acts
            x_send(m).start()

        def send_final():
            ends = [acts[dec_rows + e - 8:dec_rows + e].astype(F32) for e in range(seg_micro, seg_len + 1, seg_micro)]
            row = lax.broadcasted_iota(jnp.int32, (8, hidden), 0)
            kept = ends[-1]
            for i, rows in enumerate(ends[:-1]):
                shift = len(ends) - 1 - i
                kept = jnp.where(row == 7 - shift, pltpu.roll(rows, 8 - shift, 0), kept)
            tail = jnp.concatenate([acts[:dec_rows], kept.astype(BF16)], axis=0)
            fin[m] = rms_norm(tail, g_final[...].astype(F32)[None, :])
            for target in fin_first:
                fin_send(m, target).start()

        if loading:
            send_rows()
        else:
            pl.when(stage < last)(send_rows)
            pl.when(stage == last)(send_final)
        return carry

    @pl.when(stage == 0)
    def _():
        lax.fori_loop(0, n_micro, functools.partial(tick, True), 0)

    @pl.when(stage > 0)
    def _():
        for copy in qkv_copies + pre_copies + wo_copies + up_copies[0] + up_copies[1] + down_copies:
            copy.wait()
        for m in range(n_micro):
            k_copy(m).wait()
            v_copy(m).wait()
        lax.fori_loop(0, n_micro, functools.partial(tick, False), 0)

    for copy in head_copies:
        copy.start()

    pre_out = (pltpu.make_async_copy(kp, kp_out, o_sem.at[0]), pltpu.make_async_copy(vp, vp_out, o_sem.at[1]))
    for copy in pre_out:
        copy.start()

    col_full = lax.broadcasted_iota(jnp.int32, (kv_width, cache_len), 1)

    def patch(m, carry):
        for new, cache in ((kn, kc), (vn, vc)):
            cols = jnp.transpose(new[m])
            for b in range(dec_rows):
                pos = dec_len[m * (dec_rows // per_micro) + b // per_micro, b % per_micro]
                column = jnp.broadcast_to(cols[:, b:b + 1], (kv_width, cache_len)).astype(BF16)
                cache[m, b] = jnp.where(col_full == pos, column, cache[m, b])
        return carry

    lax.fori_loop(0, n_micro, patch, 0)

    @pl.when(stage < last)
    def _():
        for m in range(n_micro):
            x_send(m).wait_send()

    def fin_next(m):
        return pltpu.make_async_remote_copy(
            src_ref=fin.at[m], dst_ref=fin.at[m], send_sem=fnext_sem.at[m], recv_sem=frecv_sem.at[m],
            device_id={'stage': jnp.maximum(stage - 1, 0)}, device_id_type=MESH)

    @pl.when(passes_on)
    def _():
        for m in range(n_micro):
            fin_next(m).wait_recv()
            fin_next(m).start()
        for m in range(n_micro):
            fin_next(m).wait_send()

    @pl.when((stage < last) & jnp.logical_not(passes_on))
    def _():
        for m in range(n_micro):
            fin_next(m).wait_recv()

    @pl.when(stage == last)
    def _():
        for m in range(n_micro):
            for target in fin_first:
                fin_send(m, target).wait_send()

    fin_copy = pltpu.make_async_copy(fin, fin_out, o_sem.at[2])
    fin_copy.start()
    for copy in pre_out:
        copy.wait()
    fin_copy.wait()
    for copy in head_copies:
        copy.wait()


def output_kernel(micros, vocab, kc, vc, w_low, w_high, fin_in, kp_in, vp_in, logits, kc_out, vc_out, kp_out, vp_out, fin, kp, vp, rows, stage_buf, i_sem, c_sem, l_sem):
    n_chunk = fin.shape[0]
    n_kept = logits.shape[0]
    join = micros // n_chunk
    n_slot, _, _, v_blk = stage_buf.shape
    copies = [pltpu.make_async_copy(src, dst, c_sem.at[i]) for i, (src, dst) in enumerate(((kc, kc_out), (vc, vc_out), (kp, kp_out), (vp, vp_out)))]
    loads = [pltpu.make_async_copy(src, dst, i_sem.at[i]) for i, (src, dst) in enumerate(((fin_in, fin), (kp_in, kp), (vp_in, vp)))]
    low = w_low.shape[1]
    for copy in loads + copies[:2]:
        copy.start()
    for copy in loads:
        copy.wait()
    for copy in copies[2:]:
        copy.start()

    for m in range(micros):
        kept = fin[m // join].astype(F32)
        first = (m % join) * (n_kept - 1)
        last = fin.shape[1] - join + m % join
        for t in range(rows.shape[0]):
            tile = kept[:, t * 128:(t + 1) * 128]
            rows[t, pl.ds(m, n_kept - 1, stride=micros), :] = tile[first:first + n_kept - 1]
            rows[t, (n_kept - 1) * micros + m:(n_kept - 1) * micros + m + 1, :] = tile[last:last + 1]
    lhs = jnp.concatenate([rows[t].astype(BF16) for t in range(rows.shape[0])], axis=1)

    blocks = [(w_low, 0, n, min(v_blk, low - n)) for n in range(0, low, v_blk)]
    blocks += [(w_high, low, n, min(v_blk, vocab - low - n)) for n in range(0, vocab - low, v_blk)]

    def store(i):
        _, base, n, width = blocks[i]
        return pltpu.make_async_copy(
            stage_buf.at[i % n_slot, :, :, pl.ds(0, width)], logits.at[:, :, pl.ds(base + n, width)], l_sem.at[i % n_slot])

    for i, (w_ref, base, n, width) in enumerate(blocks):
        if i >= n_slot:
            store(i - n_slot).wait()
        out = dot(lhs, w_ref[:, n:n + width])
        for r in range(n_kept):
            stage_buf[i % n_slot, r, :, :width] = out[r * micros:(r + 1) * micros]
        store(i).start()
    for i in range(len(blocks) - n_slot, len(blocks)):
        store(i).wait()
    for copy in copies:
        copy.wait()


def solution(mesh):
    n_stages = mesh.shape['stage']
    part_spec = P('replica')
    layer_spec = P('stage')
    cache_spec = P('stage', 'replica')
    in_specs = (part_spec,) * 4 + (layer_spec,) * 9 + (P(), P()) + (cache_spec,) * 4
    out_specs = (part_spec,) + (cache_spec,) * 4

    def device_fn(x_dec, x_pre, dec_len, pre_len, g_attn, w_q, w_k, w_v, w_o, g_mlp, w_gate, w_up, w_down, g_final, w_head, k_dec, v_dec, k_pre, v_pre):
        micros, micro_rows, hidden = x_dec.shape
        n_micro = micros // JOIN
        dec_rows = micro_rows * JOIN
        seg_len = x_pre.shape[1] * JOIN
        x_dec = x_dec.reshape(n_micro, dec_rows, hidden)
        x_pre = x_pre.reshape(n_micro, seg_len, hidden)
        n_rows = dec_rows + seg_len
        _, cache_len, kv_count, head_dim = k_pre.shape
        kv_width = kv_count * head_dim
        q_width = w_q.shape[2]
        ffn = w_gate.shape[2]
        vocab = w_head.shape[1]
        fin_rows = dec_rows + 8

        kd = jnp.transpose(k_dec[0], (0, 1, 3, 4, 2)).reshape(n_micro, dec_rows, kv_width, cache_len)
        vd = jnp.transpose(v_dec[0], (0, 1, 3, 4, 2)).reshape(n_micro, dec_rows, kv_width, cache_len)
        kpre = jnp.transpose(k_pre[0], (1, 2, 0)).reshape(kv_width, cache_len)
        vpre = jnp.transpose(v_pre[0], (1, 2, 0)).reshape(kv_width, cache_len)

        lanes = np.arange(128) % (head_dim // 2)
        inv_freq = jnp.asarray((ROPE_BASE ** (-lanes * (2.0 / head_dim))).astype(np.float32)[None, :])

        def spec(space):
            return pl.BlockSpec(memory_space=space)

        kc, vc, w1, w3, fin, kp, vp = pl.pallas_call(
            functools.partial(pipeline_kernel, n_stages),
            out_shape=(
                VMEM((n_micro, dec_rows, kv_width, cache_len), BF16),
                VMEM((n_micro, dec_rows, kv_width, cache_len), BF16),
                VMEM((hidden, ffn), BF16),
                VMEM((hidden, ffn), BF16),
                pltpu.HBM((n_micro, fin_rows, hidden), BF16),
                pltpu.HBM((kv_width, cache_len), BF16),
                pltpu.HBM((kv_width, cache_len), BF16),
            ),
            in_specs=[spec(SMEM)] * 2 + [spec(HBM)] * 18,
            out_specs=(spec(VMEM),) * 4 + (spec(pltpu.HBM),) * 3,
            scratch_shapes=[
                VMEM((1, 128), F32),
                VMEM((1, hidden), BF16),
                VMEM((1, hidden), BF16),
                VMEM((hidden,), BF16),
                VMEM((hidden, q_width + 2 * kv_width), BF16),
                VMEM((q_width, hidden), BF16),
                VMEM((ffn, hidden), BF16),
                VMEM((kv_width, cache_len), BF16),
                VMEM((kv_width, cache_len), BF16),
                VMEM((n_micro, n_rows, hidden), BF16),
                VMEM((n_micro, fin_rows, hidden), BF16),
                VMEM((dec_rows * 16, 128), F32),
                VMEM((n_micro, dec_rows, kv_width), F32),
                VMEM((n_micro, dec_rows, kv_width), F32),
                VMEM((n_micro, n_rows, 128), F32),
                VMEM((n_micro, n_rows, 128), F32),
                VMEM((ffn // 256 * n_rows, 256), BF16),
                VMEM((q_width // head_dim * seg_len, cache_len), F32),
                pltpu.SemaphoreType.DMA((12,)),
                pltpu.SemaphoreType.DMA((n_micro, 2)),
                pltpu.SemaphoreType.DMA((2,)),
                pltpu.SemaphoreType.DMA((n_micro, 2)),
                pltpu.SemaphoreType.DMA((3,)),
                pltpu.SemaphoreType.DMA((4,)),
                pltpu.SemaphoreType.DMA((n_micro,)),
                pltpu.SemaphoreType.DMA((n_micro,)),
                pltpu.SemaphoreType.DMA((n_micro, n_stages - 1)),
                pltpu.SemaphoreType.DMA((n_micro,)),
                pltpu.SemaphoreType.DMA((n_micro,)),
            ],
            compiler_params=pltpu.CompilerParams(collective_id=0, has_side_effects=True, vmem_limit_bytes=int(R1_MB * 1024 * 1024)),
            name='pipeline',
        )(dec_len, pre_len, *(pltpu.with_memory_space_constraint(arr, pltpu.HBM) for arr in (
              inv_freq, g_attn, g_mlp, g_final, x_dec, x_pre, w_q[0], w_k[0], w_v[0], w_o[0], w_gate[0], w_up[0], w_down[0], kd, vd, kpre, vpre, w_head)))

        v_blk = 512
        n_slot = -(-ffn // v_blk) - (ffn - vocab) // v_blk
        logits, kd_out, vd_out, kp_out, vp_out = pl.pallas_call(
            functools.partial(output_kernel, micros, vocab),
            out_shape=(
                jax.ShapeDtypeStruct((micro_rows + 1, micros, vocab), F32),
                jax.ShapeDtypeStruct(kd.shape, BF16),
                jax.ShapeDtypeStruct(vd.shape, BF16),
                jax.ShapeDtypeStruct(kpre.shape, BF16),
                jax.ShapeDtypeStruct(vpre.shape, BF16),
            ),
            in_specs=[spec(VMEM)] * 4 + [spec(HBM)] * 3,
            out_specs=(spec(HBM),) * 5,
            scratch_shapes=[
                VMEM((n_micro, fin_rows, hidden), BF16),
                VMEM((kv_width, cache_len), BF16),
                VMEM((kv_width, cache_len), BF16),
                VMEM((hidden // 128, (micro_rows + 1) * micros, 128), F32),
                VMEM((n_slot, micro_rows + 1, micros, v_blk), F32),
                pltpu.SemaphoreType.DMA((4,)),
                pltpu.SemaphoreType.DMA((4,)),
                pltpu.SemaphoreType.DMA((n_slot,)),
            ],
            compiler_params=pltpu.CompilerParams(vmem_limit_bytes=7 * 1024 * 1024),
            name='output',
        )(kc, vc, w1, w3, *(pltpu.with_memory_space_constraint(arr, pltpu.HBM) for arr in (fin, kp, vp)))

        def dec_cache(arr):
            return jnp.transpose(arr.reshape(micros, micro_rows, kv_count, head_dim, cache_len), (0, 1, 4, 2, 3))[None]

        def pre_cache(arr):
            return jnp.transpose(arr.reshape(kv_count, head_dim, cache_len), (2, 0, 1))[None]

        return jnp.transpose(logits, (1, 0, 2)), dec_cache(kd_out), dec_cache(vd_out), pre_cache(kp_out), pre_cache(vp_out)

    return jax.shard_map(device_fn, mesh=mesh, in_specs=in_specs, out_specs=out_specs, check_vma=False)
```

```python
import functools

import jax
import jax.numpy as jnp
import numpy as np
from jax import lax
from jax.experimental import pallas as pl
from jax.experimental.pallas import tpu as pltpu
from jax.sharding import PartitionSpec as P

NORM_EPS = 1e-6
ROPE_BASE = 10000.0
F32 = jnp.float32
BF16 = jnp.bfloat16
NEG = -1e30
HBM = pl.ANY
VMEM = pltpu.VMEM
SMEM = pltpu.SMEM
MESH = pl.DeviceIdType.MESH
R1_MB = 21.5
JOIN = 2


def rms_norm(acts, gain):
    acts_f = acts.astype(F32)
    inv_rms = lax.rsqrt(jnp.mean(acts_f * acts_f, axis=-1, keepdims=True) + NORM_EPS)
    return (acts_f * inv_rms * gain.astype(F32)).astype(BF16)


def dot(lhs, rhs):
    return jnp.dot(lhs, rhs, preferred_element_type=F32)


def dot_t(lhs, rhs):
    return lax.dot_general(lhs, rhs, (((1,), (1,)), ((), ())), preferred_element_type=F32)


def softmax(scores):
    expd = jnp.exp(scores - jnp.max(scores, axis=-1, keepdims=True))
    return expd * (1.0 / jnp.sum(expd, axis=-1, keepdims=True))


def pipeline_kernel(
    n_stages,
    dec_len, pre_len, inv_freq_in, g_attn_in, g_mlp_in, g_final_in,
    x_dec, x_pre, w_q, w_k, w_v, w_o, w_gate, w_up, w_down, k_dec, v_dec, k_pre, v_pre, w_head,
    kc, vc, w1, w3, fin_out, kp_out, vp_out,
    inv_freq, g_attn, g_mlp, g_final, wqkv, wo, w2, kp, vp, xin, fin, qd, kn, vn, cosv, sinv, hid, sp,
    w_sem, kv_sem, p_sem, x_sem, o_sem, g_sem, send_sem, recv_sem, fsend_sem, frecv_sem, fnext_sem,
):
    n_micro, n_rows, hidden = xin.shape
    dec_rows = x_dec.shape[1]
    seg_len = x_pre.shape[1]
    per_micro = dec_len.shape[1]
    kv_width, cache_len = kp.shape
    q_width = wo.shape[0]
    ffn = w2.shape[0]
    head_dim = 64
    kv_count = kv_width // head_dim
    q_heads = q_width // head_dim
    group = q_heads // kv_count
    stage = lax.axis_index('stage')
    last = n_stages - 1
    half = ffn // 2
    seg_micro = seg_len * per_micro // dec_rows

    barrier = pltpu.get_barrier_semaphore()

    def x_copies(m):
        return (
            pltpu.make_async_copy(x_dec.at[m], xin.at[m, pl.ds(0, dec_rows)], x_sem.at[m, 0]),
            pltpu.make_async_copy(x_pre.at[m], xin.at[m, pl.ds(dec_rows, seg_len)], x_sem.at[m, 1]),
        )

    def k_copy(m):
        return pltpu.make_async_copy(k_dec.at[m], kc.at[m], kv_sem.at[m, 0])

    def v_copy(m):
        return pltpu.make_async_copy(v_dec.at[m], vc.at[m], kv_sem.at[m, 1])

    qkv_copies = (
        pltpu.make_async_copy(w_q, wqkv.at[:, pl.ds(0, q_width)], w_sem.at[0]),
        pltpu.make_async_copy(w_k, wqkv.at[:, pl.ds(q_width, kv_width)], w_sem.at[1]),
        pltpu.make_async_copy(w_v, wqkv.at[:, pl.ds(q_width + kv_width, kv_width)], w_sem.at[2]),
    )
    pre_copies = (
        pltpu.make_async_copy(k_pre, kp, p_sem.at[0]),
        pltpu.make_async_copy(v_pre, vp, p_sem.at[1]),
    )
    wo_copies = (pltpu.make_async_copy(w_o, wo, w_sem.at[3]),)
    up_copies = tuple(
        (
            pltpu.make_async_copy(w_gate.at[:, pl.ds(i * half, half)], w1.at[:, pl.ds(i * half, half)], w_sem.at[4 + 2 * i]),
            pltpu.make_async_copy(w_up.at[:, pl.ds(i * half, half)], w3.at[:, pl.ds(i * half, half)], w_sem.at[5 + 2 * i]),
        )
        for i in range(2)
    )
    rest = w_head.shape[1] - ffn
    head_copies = (
        pltpu.make_async_copy(w_head.at[:, pl.ds(0, ffn)], w1, w_sem.at[9]),
        pltpu.make_async_copy(w_head.at[:, pl.ds(ffn, rest)], w3.at[:, pl.ds(0, rest)], w_sem.at[10]),
    )
    cut = ffn // 512 * 256 + 256
    down_copies = tuple(
        pltpu.make_async_copy(w_down.at[pl.ds(lo, size)], w2.at[pl.ds(lo, size)], w_sem.at[sem])
        for lo, size, sem in ((0, cut, 8), (cut, ffn - cut, 11)))

    gain_copies = [pltpu.make_async_copy(src, dst, g_sem.at[i]) for i, (src, dst) in enumerate((
        (inv_freq_in, inv_freq), (g_attn_in, g_attn), (g_mlp_in, g_mlp), (g_final_in, g_final)))]
    for copy in gain_copies:
        copy.start()

    @pl.when(stage == 0)
    def _():
        for copy in x_copies(0):
            copy.start()
    for copy in qkv_copies + pre_copies + (k_copy(0), v_copy(0)) + wo_copies + up_copies[0] + up_copies[1] + down_copies:
        copy.start()

    @pl.when(stage == 0)
    def _():
        for m in range(1, n_micro):
            for copy in x_copies(m):
                copy.start()
    for m in range(1, n_micro):
        for copy in (k_copy(m), v_copy(m)):
            copy.start()

    @pl.when(stage > 0)
    def _():
        pl.semaphore_signal(barrier, inc=1, device_id={'stage': stage - 1}, device_id_type=MESH)

    n_chips = n_stages // 2
    hops = {t: min((last - t) // 2, n_chips - (last - t) // 2) for t in range(1, last, 2)}
    fin_first = sorted(hops, key=lambda t: -hops[t]) + [last - 1]
    passes_on = (stage % 2 == 1) & (stage < last)
    ends_chain = (stage % 2 == 0) & (stage < last - 1)

    @pl.when(ends_chain)
    def _():
        pl.semaphore_signal(barrier, inc=1, device_id={'stage': stage + 1}, device_id_type=MESH)

    @pl.when((stage < last) & jnp.logical_not(ends_chain))
    def _():
        pl.semaphore_signal(barrier, inc=1, device_id={'stage': last}, device_id_type=MESH)

    for copy in gain_copies:
        copy.wait()

    lane = lax.broadcasted_iota(jnp.int32, (8, 128), 1)
    row8 = lax.broadcasted_iota(jnp.int32, (8, 128), 0)
    freq = inv_freq[...]
    sign = jnp.where((lane % head_dim) < head_dim // 2, -1.0, 1.0)

    def table_body(m, carry):
        for g in range(n_rows // 8):
            if g < dec_rows // 8:
                pos = jnp.zeros((8, 128), jnp.int32)
                for r in range(8):
                    pos = jnp.where(row8 == r, dec_len[m * (dec_rows // per_micro) + (g * 8 + r) // per_micro, (g * 8 + r) % per_micro], pos)
            else:
                pos = pre_len[0] + m * seg_len + (g * 8 - dec_rows) + row8
            angle = pos.astype(F32) * freq
            cosv[m, pl.ds(g * 8, 8), :] = jnp.cos(angle)
            sinv[m, pl.ds(g * 8, 8), :] = jnp.sin(angle) * sign
        return carry

    lax.fori_loop(0, n_micro, table_body, 0)
    qd[...] = jnp.zeros(qd.shape, F32)

    @pl.when((stage < last) & jnp.logical_not(passes_on))
    def _():
        pl.semaphore_wait(barrier, 1)

    @pl.when(passes_on)
    def _():
        pl.semaphore_wait(barrier, 2)

    @pl.when(stage == last)
    def _():
        pl.semaphore_wait(barrier, len(fin_first))

    def x_send(m):
        return pltpu.make_async_remote_copy(
            src_ref=xin.at[m], dst_ref=xin.at[m], send_sem=send_sem.at[m], recv_sem=recv_sem.at[m],
            device_id={'stage': jnp.minimum(stage + 1, last)}, device_id_type=MESH)

    def fin_send(m, target):
        return pltpu.make_async_remote_copy(
            src_ref=fin.at[m], dst_ref=fin.at[m], send_sem=fsend_sem.at[m, target], recv_sem=frecv_sem.at[m],
            device_id={'stage': target}, device_id_type=MESH)

    def tick(loading, m, carry):
        def wait_first(copies):
            if loading:
                for copy in copies:
                    copy.wait()

        if loading:
            for copy in x_copies(m):
                copy.wait()
        else:
            @pl.when(stage > 0)
            def _():
                x_send(m).wait_recv()
        wait_first(qkv_copies + pre_copies)

        acts = xin[m]
        normed = rms_norm(acts, g_attn[...])
        cosine = cosv[m]
        sine = sinv[m]
        lane_q = lax.broadcasted_iota(jnp.int32, (n_rows, 128), 1)
        low32 = (lane_q % head_dim) < head_dim // 2
        low_half = lax.broadcasted_iota(jnp.int32, (dec_rows, 128), 1) < head_dim

        def rotate(tile):
            swapped = jnp.where(low32, pltpu.roll(tile, 128 - head_dim // 2, 1), pltpu.roll(tile, head_dim // 2, 1))
            return tile * cosine + swapped * sine

        proj = dot(normed, wqkv[...])
        q_tiles = [rotate(proj[:, t * 128:(t + 1) * 128]).astype(BF16).astype(F32) for t in range(q_width // 128)]
        k_new = rotate(proj[:, q_width:q_width + kv_width]).astype(BF16)
        v_new = proj[:, q_width + kv_width:].astype(BF16)
        kn[m] = k_new[:dec_rows].astype(F32)
        vn[m] = v_new[:dec_rows].astype(F32)

        for j in range(q_heads):
            tile = q_tiles[j // 2][:dec_rows]
            if j % 2 != j // group:
                tile = pltpu.roll(tile, head_dim, 1)
            keep = low_half if j // group == 0 else jnp.logical_not(low_half)
            qd[pl.ds(j, dec_rows, stride=16), :] = jnp.where(keep, tile, 0.0)

        pre_begin = pre_len[0] + m * seg_len
        seg_row = lax.broadcasted_iota(jnp.int32, (seg_len, cache_len), 0)
        seg_col = lax.broadcasted_iota(jnp.int32, (seg_len, cache_len), 1)
        spread = (seg_col == seg_row + pre_begin).astype(F32).astype(BF16)
        col = lax.broadcasted_iota(jnp.int32, (kv_width, cache_len), 1)
        written = (col >= pre_begin) & (col < pre_begin + seg_len)
        contract0 = (((0,), (0,)), ((), ()))
        k_put = lax.dot_general(k_new[dec_rows:], spread, contract0, preferred_element_type=F32)
        v_put = lax.dot_general(v_new[dec_rows:], spread, contract0, preferred_element_type=F32)
        kp_f = jnp.where(written, k_put, kp[...].astype(F32)).astype(BF16)
        vp_f = jnp.where(written, v_put, vp[...].astype(F32)).astype(BF16)
        kp[...] = kp_f
        vp[...] = vp_f

        scale = head_dim ** -0.5
        pre_valid = seg_col <= seg_row + pre_begin
        span = group * seg_len
        pd_base = q_heads * seg_len
        for g in range(kv_count):
            rows = []
            for j in range(g * group, (g + 1) * group):
                keep = low_half if j % 2 == 0 else jnp.logical_not(low_half)
                rows.append(jnp.where(keep, q_tiles[j // 2][dec_rows:], 0.0).astype(BF16))
            k_g = kp_f[g * head_dim:(g + 1) * head_dim]
            sp[g * span:(g + 1) * span, :] = dot(jnp.concatenate(rows, axis=0), jnp.concatenate([k_g, k_g], axis=0))

        if loading:
            k_copy(m).wait()
        pos_lane = lax.broadcasted_iota(jnp.int32, (16, cache_len), 1)
        for b in range(dec_rows):
            pos = dec_len[m * (dec_rows // per_micro) + b // per_micro, b % per_micro]
            q_b = qd[b * 16:(b + 1) * 16, :]
            s_old = jnp.where(pos_lane < pos, dot(q_b.astype(BF16), kc[m, b]) * scale, NEG)
            s_new = jnp.sum(q_b * kn[m, b:b + 1, :], axis=-1, keepdims=True) * scale
            peak = jnp.maximum(jnp.max(s_old, axis=-1, keepdims=True), s_new)
            expd = jnp.exp(s_old - peak)
            e_new = jnp.exp(s_new - peak)
            inv = 1.0 / (jnp.sum(expd, axis=-1, keepdims=True) + e_new)
            hid[pd_base + b * 16:pd_base + (b + 1) * 16, :] = (expd * inv).astype(BF16)
            p_new = (e_new * inv).astype(BF16).astype(F32)
            qd[b * 16:(b + 1) * 16, :] = p_new * vn[m, b:b + 1, :]

        if loading:
            v_copy(m).wait()
        for j in range(q_heads):
            scores = sp[j * seg_len:(j + 1) * seg_len, :] * scale
            hid[j * seg_len:(j + 1) * seg_len, :] = softmax(jnp.where(pre_valid, scores, NEG)).astype(BF16)
        for b in range(dec_rows):
            qd[b * 16:(b + 1) * 16, :] += dot_t(hid[pd_base + b * 16:pd_base + (b + 1) * 16, :], vc[m, b])
        pre_heads = []
        for g in range(kv_count):
            v_g = vp_f[g * head_dim:(g + 1) * head_dim]
            mixed = dot_t(hid[g * span:(g + 1) * span, :], jnp.concatenate([v_g, v_g], axis=0))
            pre_heads += [mixed[i * seg_len:(i + 1) * seg_len] for i in range(group)]


        att_tiles = []
        for t in range(q_width // 128):
            parts = []
            for j in (2 * t, 2 * t + 1):
                part = qd[pl.ds(j, dec_rows, stride=16), :]
                if j % 2 != j // group:
                    part = pltpu.roll(part, head_dim, 1)
                parts.append(part)
            dec_tile = jnp.where(low_half, parts[0], parts[1])
            pre_tile = jnp.where(low_half, pre_heads[2 * t], pre_heads[2 * t + 1])
            att_tiles.append(jnp.concatenate([dec_tile, pre_tile], axis=0).astype(BF16))
        att = jnp.concatenate(att_tiles, axis=1)

        wait_first(wo_copies)

        acts = (acts.astype(F32) + dot(att, wo[...])).astype(BF16)
        normed = rms_norm(acts, g_mlp[...])

        n_blk = 256
        for i in range(2):
            wait_first(up_copies[i])
            lo = 0 if i == 0 else half // n_blk * n_blk
            hi = half // n_blk * n_blk if i == 0 else ffn
            for n in range(lo, hi, n_blk):
                gate = dot(normed, w1[:, n:n + n_blk])
                up = dot(normed, w3[:, n:n + n_blk])
                k = n // n_blk
                hid[k * n_rows:(k + 1) * n_rows, :] = (jax.nn.silu(gate) * up).astype(BF16)

        def act_blocks(lo, hi):
            return jnp.concatenate([hid[k * n_rows:(k + 1) * n_rows, :] for k in range(lo // n_blk, hi // n_blk)], axis=1)

        if loading:
            wait_first(down_copies[:1])
            down = dot(act_blocks(0, cut), w2[:cut, :])
            wait_first(down_copies[1:])
            down = down + dot(act_blocks(cut, ffn), w2[cut:, :])
        else:
            down = dot(act_blocks(0, ffn), w2[...])
        acts = (acts.astype(F32) + down).astype(BF16)

        def send_rows():
            xin[m] = acts
            x_send(m).start()

        def send_final():
            ends = [acts[dec_rows + e - 8:dec_rows + e].astype(F32) for e in range(seg_micro, seg_len + 1, seg_micro)]
            row = lax.broadcasted_iota(jnp.int32, (8, hidden), 0)
            kept = ends[-1]
            for i, rows in enumerate(ends[:-1]):
                shift = len(ends) - 1 - i
                kept = jnp.where(row == 7 - shift, pltpu.roll(rows, 8 - shift, 0), kept)
            tail = jnp.concatenate([acts[:dec_rows], kept.astype(BF16)], axis=0)
            fin[m] = rms_norm(tail, g_final[...].astype(F32)[None, :])
            for target in fin_first:
                fin_send(m, target).start()

        if loading:
            send_rows()
        else:
            pl.when(stage < last)(send_rows)
            pl.when(stage == last)(send_final)
        return carry

    @pl.when(stage == 0)
    def _():
        tick(True, 0, 0)
        for m in range(1, n_micro):
            for copy in x_copies(m) + (k_copy(m), v_copy(m)):
                copy.wait()

    @pl.when(stage > 0)
    def _():
        for copy in qkv_copies + pre_copies + wo_copies + up_copies[0] + up_copies[1] + down_copies:
            copy.wait()
        for m in range(n_micro):
            k_copy(m).wait()
            v_copy(m).wait()

    lax.fori_loop(jnp.maximum(1 - stage, 0), n_micro, functools.partial(tick, False), 0)

    for copy in head_copies:
        copy.start()

    pre_out = (pltpu.make_async_copy(kp, kp_out, o_sem.at[0]), pltpu.make_async_copy(vp, vp_out, o_sem.at[1]))
    for copy in pre_out:
        copy.start()

    col_full = lax.broadcasted_iota(jnp.int32, (kv_width, cache_len), 1)

    def patch(m, carry):
        for new, cache in ((kn, kc), (vn, vc)):
            cols = jnp.transpose(new[m])
            for b in range(dec_rows):
                pos = dec_len[m * (dec_rows // per_micro) + b // per_micro, b % per_micro]
                column = jnp.broadcast_to(cols[:, b:b + 1], (kv_width, cache_len)).astype(BF16)
                cache[m, b] = jnp.where(col_full == pos, column, cache[m, b])
        return carry

    lax.fori_loop(0, n_micro, patch, 0)

    @pl.when(stage < last)
    def _():
        for m in range(n_micro):
            x_send(m).wait_send()

    def fin_next(m):
        return pltpu.make_async_remote_copy(
            src_ref=fin.at[m], dst_ref=fin.at[m], send_sem=fnext_sem.at[m], recv_sem=frecv_sem.at[m],
            device_id={'stage': jnp.maximum(stage - 1, 0)}, device_id_type=MESH)

    @pl.when(passes_on)
    def _():
        for m in range(n_micro):
            fin_next(m).wait_recv()
            fin_next(m).start()
        for m in range(n_micro):
            fin_next(m).wait_send()

    @pl.when((stage < last) & jnp.logical_not(passes_on))
    def _():
        for m in range(n_micro):
            fin_next(m).wait_recv()

    @pl.when(stage == last)
    def _():
        for m in range(n_micro):
            for target in fin_first:
                fin_send(m, target).wait_send()

    fin_copy = pltpu.make_async_copy(fin, fin_out, o_sem.at[2])
    fin_copy.start()
    for copy in pre_out:
        copy.wait()
    fin_copy.wait()
    for copy in head_copies:
        copy.wait()


def output_kernel(micros, vocab, kc, vc, w_low, w_high, fin_in, kp_in, vp_in, logits, kc_out, vc_out, kp_out, vp_out, fin, kp, vp, rows, stage_buf, i_sem, c_sem, l_sem):
    n_chunk = fin.shape[0]
    n_kept = logits.shape[0]
    join = micros // n_chunk
    n_slot, _, _, v_blk = stage_buf.shape
    copies = [pltpu.make_async_copy(src, dst, c_sem.at[i]) for i, (src, dst) in enumerate(((kc, kc_out), (vc, vc_out), (kp, kp_out), (vp, vp_out)))]
    loads = [pltpu.make_async_copy(src, dst, i_sem.at[i]) for i, (src, dst) in enumerate(((fin_in, fin), (kp_in, kp), (vp_in, vp)))]
    low = w_low.shape[1]
    for copy in loads + copies[:2]:
        copy.start()
    for copy in loads:
        copy.wait()
    for copy in copies[2:]:
        copy.start()

    for m in range(micros):
        kept = fin[m // join].astype(F32)
        first = (m % join) * (n_kept - 1)
        last = fin.shape[1] - join + m % join
        for t in range(rows.shape[0]):
            tile = kept[:, t * 128:(t + 1) * 128]
            rows[t, pl.ds(m, n_kept - 1, stride=micros), :] = tile[first:first + n_kept - 1]
            rows[t, (n_kept - 1) * micros + m:(n_kept - 1) * micros + m + 1, :] = tile[last:last + 1]
    lhs = jnp.concatenate([rows[t].astype(BF16) for t in range(rows.shape[0])], axis=1)

    blocks = [(w_low, 0, n, min(v_blk, low - n)) for n in range(0, low, v_blk)]
    blocks += [(w_high, low, n, min(v_blk, vocab - low - n)) for n in range(0, vocab - low, v_blk)]

    def store(i):
        _, base, n, width = blocks[i]
        return pltpu.make_async_copy(
            stage_buf.at[i % n_slot, :, :, pl.ds(0, width)], logits.at[:, :, pl.ds(base + n, width)], l_sem.at[i % n_slot])

    for i, (w_ref, base, n, width) in enumerate(blocks):
        if i >= n_slot:
            store(i - n_slot).wait()
        out = dot(lhs, w_ref[:, n:n + width])
        for r in range(n_kept):
            stage_buf[i % n_slot, r, :, :width] = out[r * micros:(r + 1) * micros]
        store(i).start()
    for i in range(len(blocks) - n_slot, len(blocks)):
        store(i).wait()
    for copy in copies:
        copy.wait()


def solution(mesh):
    n_stages = mesh.shape['stage']
    part_spec = P('replica')
    layer_spec = P('stage')
    cache_spec = P('stage', 'replica')
    in_specs = (part_spec,) * 4 + (layer_spec,) * 9 + (P(), P()) + (cache_spec,) * 4
    out_specs = (part_spec,) + (cache_spec,) * 4

    def device_fn(x_dec, x_pre, dec_len, pre_len, g_attn, w_q, w_k, w_v, w_o, g_mlp, w_gate, w_up, w_down, g_final, w_head, k_dec, v_dec, k_pre, v_pre):
        micros, micro_rows, hidden = x_dec.shape
        n_micro = micros // JOIN
        dec_rows = micro_rows * JOIN
        seg_len = x_pre.shape[1] * JOIN
        x_dec = x_dec.reshape(n_micro, dec_rows, hidden)
        x_pre = x_pre.reshape(n_micro, seg_len, hidden)
        n_rows = dec_rows + seg_len
        _, cache_len, kv_count, head_dim = k_pre.shape
        kv_width = kv_count * head_dim
        q_width = w_q.shape[2]
        ffn = w_gate.shape[2]
        vocab = w_head.shape[1]
        fin_rows = dec_rows + 8

        kd = jnp.transpose(k_dec[0], (0, 1, 3, 4, 2)).reshape(n_micro, dec_rows, kv_width, cache_len)
        vd = jnp.transpose(v_dec[0], (0, 1, 3, 4, 2)).reshape(n_micro, dec_rows, kv_width, cache_len)
        kpre = jnp.transpose(k_pre[0], (1, 2, 0)).reshape(kv_width, cache_len)
        vpre = jnp.transpose(v_pre[0], (1, 2, 0)).reshape(kv_width, cache_len)

        lanes = np.arange(128) % (head_dim // 2)
        inv_freq = jnp.asarray((ROPE_BASE ** (-lanes * (2.0 / head_dim))).astype(np.float32)[None, :])

        def spec(space):
            return pl.BlockSpec(memory_space=space)

        kc, vc, w1, w3, fin, kp, vp = pl.pallas_call(
            functools.partial(pipeline_kernel, n_stages),
            out_shape=(
                VMEM((n_micro, dec_rows, kv_width, cache_len), BF16),
                VMEM((n_micro, dec_rows, kv_width, cache_len), BF16),
                VMEM((hidden, ffn), BF16),
                VMEM((hidden, ffn), BF16),
                pltpu.HBM((n_micro, fin_rows, hidden), BF16),
                pltpu.HBM((kv_width, cache_len), BF16),
                pltpu.HBM((kv_width, cache_len), BF16),
            ),
            in_specs=[spec(SMEM)] * 2 + [spec(HBM)] * 18,
            out_specs=(spec(VMEM),) * 4 + (spec(pltpu.HBM),) * 3,
            scratch_shapes=[
                VMEM((1, 128), F32),
                VMEM((1, hidden), BF16),
                VMEM((1, hidden), BF16),
                VMEM((hidden,), BF16),
                VMEM((hidden, q_width + 2 * kv_width), BF16),
                VMEM((q_width, hidden), BF16),
                VMEM((ffn, hidden), BF16),
                VMEM((kv_width, cache_len), BF16),
                VMEM((kv_width, cache_len), BF16),
                VMEM((n_micro, n_rows, hidden), BF16),
                VMEM((n_micro, fin_rows, hidden), BF16),
                VMEM((dec_rows * 16, 128), F32),
                VMEM((n_micro, dec_rows, kv_width), F32),
                VMEM((n_micro, dec_rows, kv_width), F32),
                VMEM((n_micro, n_rows, 128), F32),
                VMEM((n_micro, n_rows, 128), F32),
                VMEM((ffn // 256 * n_rows, 256), BF16),
                VMEM((q_width // head_dim * seg_len, cache_len), F32),
                pltpu.SemaphoreType.DMA((12,)),
                pltpu.SemaphoreType.DMA((n_micro, 2)),
                pltpu.SemaphoreType.DMA((2,)),
                pltpu.SemaphoreType.DMA((n_micro, 2)),
                pltpu.SemaphoreType.DMA((3,)),
                pltpu.SemaphoreType.DMA((4,)),
                pltpu.SemaphoreType.DMA((n_micro,)),
                pltpu.SemaphoreType.DMA((n_micro,)),
                pltpu.SemaphoreType.DMA((n_micro, n_stages - 1)),
                pltpu.SemaphoreType.DMA((n_micro,)),
                pltpu.SemaphoreType.DMA((n_micro,)),
            ],
            compiler_params=pltpu.CompilerParams(collective_id=0, has_side_effects=True, vmem_limit_bytes=int(R1_MB * 1024 * 1024)),
            name='pipeline',
        )(dec_len, pre_len, *(pltpu.with_memory_space_constraint(arr, pltpu.HBM) for arr in (
              inv_freq, g_attn, g_mlp, g_final, x_dec, x_pre, w_q[0], w_k[0], w_v[0], w_o[0], w_gate[0], w_up[0], w_down[0], kd, vd, kpre, vpre, w_head)))

        v_blk = 512
        n_slot = -(-ffn // v_blk) - (ffn - vocab) // v_blk
        logits, kd_out, vd_out, kp_out, vp_out = pl.pallas_call(
            functools.partial(output_kernel, micros, vocab),
            out_shape=(
                jax.ShapeDtypeStruct((micro_rows + 1, micros, vocab), F32),
                jax.ShapeDtypeStruct(kd.shape, BF16),
                jax.ShapeDtypeStruct(vd.shape, BF16),
                jax.ShapeDtypeStruct(kpre.shape, BF16),
                jax.ShapeDtypeStruct(vpre.shape, BF16),
            ),
            in_specs=[spec(VMEM)] * 4 + [spec(HBM)] * 3,
            out_specs=(spec(HBM),) * 5,
            scratch_shapes=[
                VMEM((n_micro, fin_rows, hidden), BF16),
                VMEM((kv_width, cache_len), BF16),
                VMEM((kv_width, cache_len), BF16),
                VMEM((hidden // 128, (micro_rows + 1) * micros, 128), F32),
                VMEM((n_slot, micro_rows + 1, micros, v_blk), F32),
                pltpu.SemaphoreType.DMA((4,)),
                pltpu.SemaphoreType.DMA((4,)),
                pltpu.SemaphoreType.DMA((n_slot,)),
            ],
            compiler_params=pltpu.CompilerParams(vmem_limit_bytes=7 * 1024 * 1024),
            name='output',
        )(kc, vc, w1, w3, *(pltpu.with_memory_space_constraint(arr, pltpu.HBM) for arr in (fin, kp, vp)))

        def dec_cache(arr):
            return jnp.transpose(arr.reshape(micros, micro_rows, kv_count, head_dim, cache_len), (0, 1, 4, 2, 3))[None]

        def pre_cache(arr):
            return jnp.transpose(arr.reshape(kv_count, head_dim, cache_len), (2, 0, 1))[None]

        return jnp.transpose(logits, (1, 0, 2)), dec_cache(kd_out), dec_cache(vd_out), pre_cache(kp_out), pre_cache(vp_out)

    return jax.shard_map(device_fn, mesh=mesh, in_specs=in_specs, out_specs=out_specs, check_vma=False)
```

```python
import functools

import jax
import jax.numpy as jnp
import numpy as np
from jax import lax
from jax.experimental import pallas as pl
from jax.experimental.pallas import tpu as pltpu
from jax.sharding import PartitionSpec as P

NORM_EPS = 1e-6
ROPE_BASE = 10000.0
F32 = jnp.float32
BF16 = jnp.bfloat16
NEG = -1e30
HBM = pl.ANY
VMEM = pltpu.VMEM
SMEM = pltpu.SMEM
MESH = pl.DeviceIdType.MESH
R1_MB = 21.5
JOIN = 2


def rms_norm(acts, gain):
    acts_f = acts.astype(F32)
    inv_rms = lax.rsqrt(jnp.mean(acts_f * acts_f, axis=-1, keepdims=True) + NORM_EPS)
    return (acts_f * inv_rms * gain.astype(F32)).astype(BF16)


def dot(lhs, rhs):
    return jnp.dot(lhs, rhs, preferred_element_type=F32)


def dot_t(lhs, rhs):
    return lax.dot_general(lhs, rhs, (((1,), (1,)), ((), ())), preferred_element_type=F32)


def softmax(scores):
    expd = jnp.exp(scores - jnp.max(scores, axis=-1, keepdims=True))
    return expd * (1.0 / jnp.sum(expd, axis=-1, keepdims=True))


def pipeline_kernel(
    n_stages,
    dec_len, pre_len, inv_freq_in, g_attn_in, g_mlp_in, g_final_in,
    x_dec, x_pre, w_q, w_k, w_v, w_o, w_gate, w_up, w_down, k_dec, v_dec, k_pre, v_pre, w_head,
    kc, vc, w1, w3, fin_out, kp_out, vp_out,
    inv_freq, g_attn, g_mlp, g_final, wqkv, wo, w2, kp, vp, xin, fin, qd, kn, vn, cosv, sinv, hid, sp,
    w_sem, kv_sem, p_sem, x_sem, o_sem, g_sem, send_sem, recv_sem, fsend_sem, frecv_sem, fnext_sem,
):
    n_micro, n_rows, hidden = xin.shape
    dec_rows = x_dec.shape[1]
    seg_len = x_pre.shape[1]
    per_micro = dec_len.shape[1]
    kv_width, cache_len = kp.shape
    q_width = wo.shape[0]
    ffn = w2.shape[0]
    head_dim = 64
    kv_count = kv_width // head_dim
    q_heads = q_width // head_dim
    group = q_heads // kv_count
    stage = lax.axis_index('stage')
    last = n_stages - 1
    half = ffn // 2
    seg_micro = seg_len * per_micro // dec_rows

    barrier = pltpu.get_barrier_semaphore()

    def x_copies(m):
        return (
            pltpu.make_async_copy(x_dec.at[m], xin.at[m, pl.ds(0, dec_rows)], x_sem.at[m, 0]),
            pltpu.make_async_copy(x_pre.at[m], xin.at[m, pl.ds(dec_rows, seg_len)], x_sem.at[m, 1]),
        )

    def k_copy(m):
        return pltpu.make_async_copy(k_dec.at[m], kc.at[m], kv_sem.at[m, 0])

    def v_copy(m):
        return pltpu.make_async_copy(v_dec.at[m], vc.at[m], kv_sem.at[m, 1])

    qkv_copies = (
        pltpu.make_async_copy(w_q, wqkv.at[:, pl.ds(0, q_width)], w_sem.at[0]),
        pltpu.make_async_copy(w_k, wqkv.at[:, pl.ds(q_width, kv_width)], w_sem.at[1]),
        pltpu.make_async_copy(w_v, wqkv.at[:, pl.ds(q_width + kv_width, kv_width)], w_sem.at[2]),
    )
    pre_copies = (
        pltpu.make_async_copy(k_pre, kp, p_sem.at[0]),
        pltpu.make_async_copy(v_pre, vp, p_sem.at[1]),
    )
    wo_copies = (pltpu.make_async_copy(w_o, wo, w_sem.at[3]),)
    up_copies = tuple(
        (
            pltpu.make_async_copy(w_gate.at[:, pl.ds(i * half, half)], w1.at[:, pl.ds(i * half, half)], w_sem.at[4 + 2 * i]),
            pltpu.make_async_copy(w_up.at[:, pl.ds(i * half, half)], w3.at[:, pl.ds(i * half, half)], w_sem.at[5 + 2 * i]),
        )
        for i in range(2)
    )
    rest = w_head.shape[1] - ffn
    head_copies = (
        pltpu.make_async_copy(w_head.at[:, pl.ds(0, ffn)], w1, w_sem.at[9]),
        pltpu.make_async_copy(w_head.at[:, pl.ds(ffn, rest)], w3.at[:, pl.ds(0, rest)], w_sem.at[10]),
    )
    cut = ffn // 512 * 256 + 256
    down_copies = tuple(
        pltpu.make_async_copy(w_down.at[pl.ds(lo, size)], w2.at[pl.ds(lo, size)], w_sem.at[sem])
        for lo, size, sem in ((0, cut, 8), (cut, ffn - cut, 11)))

    gain_copies = [pltpu.make_async_copy(src, dst, g_sem.at[i]) for i, (src, dst) in enumerate((
        (inv_freq_in, inv_freq), (g_attn_in, g_attn), (g_mlp_in, g_mlp), (g_final_in, g_final)))]
    for copy in gain_copies:
        copy.start()

    @pl.when(stage == 0)
    def _():
        for copy in x_copies(0):
            copy.start()
    for copy in qkv_copies + pre_copies + (k_copy(0), v_copy(0)) + wo_copies:
        copy.start()
    later = [up_copies[0], up_copies[1], down_copies, (k_copy(1), v_copy(1)) if n_micro > 1 else ()]
    later[-1] += tuple(copy for m in range(2, n_micro) for copy in (k_copy(m), v_copy(m)))

    def start_later(i):
        for copy in later[i]:
            copy.start()

    @pl.when(stage == 0)
    def _():
        for m in range(1, n_micro):
            for copy in x_copies(m):
                copy.start()

    @pl.when(stage > 0)
    def _():
        for i in range(len(later)):
            start_later(i)

    @pl.when(stage > 0)
    def _():
        pl.semaphore_signal(barrier, inc=1, device_id={'stage': stage - 1}, device_id_type=MESH)

    n_chips = n_stages // 2
    hops = {t: min((last - t) // 2, n_chips - (last - t) // 2) for t in range(1, last, 2)}
    fin_first = sorted(hops, key=lambda t: -hops[t]) + [last - 1]
    passes_on = (stage % 2 == 1) & (stage < last)
    ends_chain = (stage % 2 == 0) & (stage < last - 1)

    @pl.when(ends_chain)
    def _():
        pl.semaphore_signal(barrier, inc=1, device_id={'stage': stage + 1}, device_id_type=MESH)

    @pl.when((stage < last) & jnp.logical_not(ends_chain))
    def _():
        pl.semaphore_signal(barrier, inc=1, device_id={'stage': last}, device_id_type=MESH)

    for copy in gain_copies:
        copy.wait()

    lane = lax.broadcasted_iota(jnp.int32, (8, 128), 1)
    row8 = lax.broadcasted_iota(jnp.int32, (8, 128), 0)
    freq = inv_freq[...]
    sign = jnp.where((lane % head_dim) < head_dim // 2, -1.0, 1.0)

    def table_body(m, carry):
        for g in range(n_rows // 8):
            if g < dec_rows // 8:
                pos = jnp.zeros((8, 128), jnp.int32)
                for r in range(8):
                    pos = jnp.where(row8 == r, dec_len[m * (dec_rows // per_micro) + (g * 8 + r) // per_micro, (g * 8 + r) % per_micro], pos)
            else:
                pos = pre_len[0] + m * seg_len + (g * 8 - dec_rows) + row8
            angle = pos.astype(F32) * freq
            cosv[m, pl.ds(g * 8, 8), :] = jnp.cos(angle)
            sinv[m, pl.ds(g * 8, 8), :] = jnp.sin(angle) * sign
        return carry

    lax.fori_loop(0, n_micro, table_body, 0)
    qd[...] = jnp.zeros(qd.shape, F32)

    @pl.when((stage < last) & jnp.logical_not(passes_on))
    def _():
        pl.semaphore_wait(barrier, 1)

    @pl.when(passes_on)
    def _():
        pl.semaphore_wait(barrier, 2)

    @pl.when(stage == last)
    def _():
        pl.semaphore_wait(barrier, len(fin_first))

    def x_send(m):
        return pltpu.make_async_remote_copy(
            src_ref=xin.at[m], dst_ref=xin.at[m], send_sem=send_sem.at[m], recv_sem=recv_sem.at[m],
            device_id={'stage': jnp.minimum(stage + 1, last)}, device_id_type=MESH)

    def fin_send(m, target):
        return pltpu.make_async_remote_copy(
            src_ref=fin.at[m], dst_ref=fin.at[m], send_sem=fsend_sem.at[m, target], recv_sem=frecv_sem.at[m],
            device_id={'stage': target}, device_id_type=MESH)

    def tick(loading, m, carry):
        def wait_first(copies):
            if loading:
                for copy in copies:
                    copy.wait()

        if loading:
            for copy in x_copies(m):
                copy.wait()
        else:
            @pl.when(stage > 0)
            def _():
                x_send(m).wait_recv()
        wait_first(qkv_copies + pre_copies)
        if loading:
            start_later(0)

        acts = xin[m]
        normed = rms_norm(acts, g_attn[...])
        cosine = cosv[m]
        sine = sinv[m]
        lane_q = lax.broadcasted_iota(jnp.int32, (n_rows, 128), 1)
        low32 = (lane_q % head_dim) < head_dim // 2
        low_half = lax.broadcasted_iota(jnp.int32, (dec_rows, 128), 1) < head_dim

        def rotate(tile):
            swapped = jnp.where(low32, pltpu.roll(tile, 128 - head_dim // 2, 1), pltpu.roll(tile, head_dim // 2, 1))
            return tile * cosine + swapped * sine

        proj = dot(normed, wqkv[...])
        q_tiles = [rotate(proj[:, t * 128:(t + 1) * 128]).astype(BF16).astype(F32) for t in range(q_width // 128)]
        k_new = rotate(proj[:, q_width:q_width + kv_width]).astype(BF16)
        v_new = proj[:, q_width + kv_width:].astype(BF16)
        kn[m] = k_new[:dec_rows].astype(F32)
        vn[m] = v_new[:dec_rows].astype(F32)

        for j in range(q_heads):
            tile = q_tiles[j // 2][:dec_rows]
            if j % 2 != j // group:
                tile = pltpu.roll(tile, head_dim, 1)
            keep = low_half if j // group == 0 else jnp.logical_not(low_half)
            qd[pl.ds(j, dec_rows, stride=16), :] = jnp.where(keep, tile, 0.0)

        pre_begin = pre_len[0] + m * seg_len
        seg_row = lax.broadcasted_iota(jnp.int32, (seg_len, cache_len), 0)
        seg_col = lax.broadcasted_iota(jnp.int32, (seg_len, cache_len), 1)
        spread = (seg_col == seg_row + pre_begin).astype(F32).astype(BF16)
        col = lax.broadcasted_iota(jnp.int32, (kv_width, cache_len), 1)
        written = (col >= pre_begin) & (col < pre_begin + seg_len)
        contract0 = (((0,), (0,)), ((), ()))
        k_put = lax.dot_general(k_new[dec_rows:], spread, contract0, preferred_element_type=F32)
        v_put = lax.dot_general(v_new[dec_rows:], spread, contract0, preferred_element_type=F32)
        kp_f = jnp.where(written, k_put, kp[...].astype(F32)).astype(BF16)
        vp_f = jnp.where(written, v_put, vp[...].astype(F32)).astype(BF16)
        kp[...] = kp_f
        vp[...] = vp_f

        scale = head_dim ** -0.5
        pre_valid = seg_col <= seg_row + pre_begin
        span = group * seg_len
        pd_base = q_heads * seg_len
        for g in range(kv_count):
            rows = []
            for j in range(g * group, (g + 1) * group):
                keep = low_half if j % 2 == 0 else jnp.logical_not(low_half)
                rows.append(jnp.where(keep, q_tiles[j // 2][dec_rows:], 0.0).astype(BF16))
            k_g = kp_f[g * head_dim:(g + 1) * head_dim]
            sp[g * span:(g + 1) * span, :] = dot(jnp.concatenate(rows, axis=0), jnp.concatenate([k_g, k_g], axis=0))

        if loading:
            k_copy(m).wait()
            start_later(1)
        pos_lane = lax.broadcasted_iota(jnp.int32, (16, cache_len), 1)
        for b in range(dec_rows):
            pos = dec_len[m * (dec_rows // per_micro) + b // per_micro, b % per_micro]
            q_b = qd[b * 16:(b + 1) * 16, :]
            s_old = jnp.where(pos_lane < pos, dot(q_b.astype(BF16), kc[m, b]) * scale, NEG)
            s_new = jnp.sum(q_b * kn[m, b:b + 1, :], axis=-1, keepdims=True) * scale
            peak = jnp.maximum(jnp.max(s_old, axis=-1, keepdims=True), s_new)
            expd = jnp.exp(s_old - peak)
            e_new = jnp.exp(s_new - peak)
            inv = 1.0 / (jnp.sum(expd, axis=-1, keepdims=True) + e_new)
            hid[pd_base + b * 16:pd_base + (b + 1) * 16, :] = (expd * inv).astype(BF16)
            p_new = (e_new * inv).astype(BF16).astype(F32)
            qd[b * 16:(b + 1) * 16, :] = p_new * vn[m, b:b + 1, :]

        if loading:
            v_copy(m).wait()
            start_later(2)
        for j in range(q_heads):
            scores = sp[j * seg_len:(j + 1) * seg_len, :] * scale
            hid[j * seg_len:(j + 1) * seg_len, :] = softmax(jnp.where(pre_valid, scores, NEG)).astype(BF16)
        for b in range(dec_rows):
            qd[b * 16:(b + 1) * 16, :] += dot_t(hid[pd_base + b * 16:pd_base + (b + 1) * 16, :], vc[m, b])
        pre_heads = []
        for g in range(kv_count):
            v_g = vp_f[g * head_dim:(g + 1) * head_dim]
            mixed = dot_t(hid[g * span:(g + 1) * span, :], jnp.concatenate([v_g, v_g], axis=0))
            pre_heads += [mixed[i * seg_len:(i + 1) * seg_len] for i in range(group)]


        att_tiles = []
        for t in range(q_width // 128):
            parts = []
            for j in (2 * t, 2 * t + 1):
                part = qd[pl.ds(j, dec_rows, stride=16), :]
                if j % 2 != j // group:
                    part = pltpu.roll(part, head_dim, 1)
                parts.append(part)
            dec_tile = jnp.where(low_half, parts[0], parts[1])
            pre_tile = jnp.where(low_half, pre_heads[2 * t], pre_heads[2 * t + 1])
            att_tiles.append(jnp.concatenate([dec_tile, pre_tile], axis=0).astype(BF16))
        att = jnp.concatenate(att_tiles, axis=1)

        wait_first(wo_copies)

        acts = (acts.astype(F32) + dot(att, wo[...])).astype(BF16)
        normed = rms_norm(acts, g_mlp[...])

        n_blk = 256
        for i in range(2):
            wait_first(up_copies[i])
            if loading and i == 1:
                start_later(3)
            lo = 0 if i == 0 else half // n_blk * n_blk
            hi = half // n_blk * n_blk if i == 0 else ffn
            for n in range(lo, hi, n_blk):
                gate = dot(normed, w1[:, n:n + n_blk])
                up = dot(normed, w3[:, n:n + n_blk])
                k = n // n_blk
                hid[k * n_rows:(k + 1) * n_rows, :] = (jax.nn.silu(gate) * up).astype(BF16)

        def act_blocks(lo, hi):
            return jnp.concatenate([hid[k * n_rows:(k + 1) * n_rows, :] for k in range(lo // n_blk, hi // n_blk)], axis=1)

        if loading:
            wait_first(down_copies[:1])
            down = dot(act_blocks(0, cut), w2[:cut, :])
            wait_first(down_copies[1:])
            down = down + dot(act_blocks(cut, ffn), w2[cut:, :])
        else:
            down = dot(act_blocks(0, ffn), w2[...])
        acts = (acts.astype(F32) + down).astype(BF16)

        def send_rows():
            xin[m] = acts
            x_send(m).start()

        def send_final():
            ends = [acts[dec_rows + e - 8:dec_rows + e].astype(F32) for e in range(seg_micro, seg_len + 1, seg_micro)]
            row = lax.broadcasted_iota(jnp.int32, (8, hidden), 0)
            kept = ends[-1]
            for i, rows in enumerate(ends[:-1]):
                shift = len(ends) - 1 - i
                kept = jnp.where(row == 7 - shift, pltpu.roll(rows, 8 - shift, 0), kept)
            tail = jnp.concatenate([acts[:dec_rows], kept.astype(BF16)], axis=0)
            fin[m] = rms_norm(tail, g_final[...].astype(F32)[None, :])
            for target in fin_first:
                fin_send(m, target).start()

        if loading:
            send_rows()
        else:
            pl.when(stage < last)(send_rows)
            pl.when(stage == last)(send_final)
        return carry

    @pl.when(stage == 0)
    def _():
        tick(True, 0, 0)
        for m in range(1, n_micro):
            for copy in x_copies(m) + (k_copy(m), v_copy(m)):
                copy.wait()

    @pl.when(stage > 0)
    def _():
        for copy in qkv_copies + pre_copies + wo_copies + up_copies[0] + up_copies[1] + down_copies:
            copy.wait()
        for m in range(n_micro):
            k_copy(m).wait()
            v_copy(m).wait()

    lax.fori_loop(jnp.maximum(1 - stage, 0), n_micro, functools.partial(tick, False), 0)

    for copy in head_copies:
        copy.start()

    pre_out = (pltpu.make_async_copy(kp, kp_out, o_sem.at[0]), pltpu.make_async_copy(vp, vp_out, o_sem.at[1]))
    for copy in pre_out:
        copy.start()

    col_full = lax.broadcasted_iota(jnp.int32, (kv_width, cache_len), 1)

    def patch(m, carry):
        for new, cache in ((kn, kc), (vn, vc)):
            cols = jnp.transpose(new[m])
            for b in range(dec_rows):
                pos = dec_len[m * (dec_rows // per_micro) + b // per_micro, b % per_micro]
                column = jnp.broadcast_to(cols[:, b:b + 1], (kv_width, cache_len)).astype(BF16)
                cache[m, b] = jnp.where(col_full == pos, column, cache[m, b])
        return carry

    lax.fori_loop(0, n_micro, patch, 0)

    @pl.when(stage < last)
    def _():
        for m in range(n_micro):
            x_send(m).wait_send()

    def fin_next(m):
        return pltpu.make_async_remote_copy(
            src_ref=fin.at[m], dst_ref=fin.at[m], send_sem=fnext_sem.at[m], recv_sem=frecv_sem.at[m],
            device_id={'stage': jnp.maximum(stage - 1, 0)}, device_id_type=MESH)

    @pl.when(passes_on)
    def _():
        for m in range(n_micro):
            fin_next(m).wait_recv()
            fin_next(m).start()
        for m in range(n_micro):
            fin_next(m).wait_send()

    @pl.when((stage < last) & jnp.logical_not(passes_on))
    def _():
        for m in range(n_micro):
            fin_next(m).wait_recv()

    @pl.when(stage == last)
    def _():
        for m in range(n_micro):
            for target in fin_first:
                fin_send(m, target).wait_send()

    fin_copy = pltpu.make_async_copy(fin, fin_out, o_sem.at[2])
    fin_copy.start()
    for copy in pre_out:
        copy.wait()
    fin_copy.wait()
    for copy in head_copies:
        copy.wait()


def output_kernel(micros, vocab, kc, vc, w_low, w_high, fin_in, kp_in, vp_in, logits, kc_out, vc_out, kp_out, vp_out, fin, kp, vp, rows, stage_buf, i_sem, c_sem, l_sem):
    n_chunk = fin.shape[0]
    n_kept = logits.shape[0]
    join = micros // n_chunk
    n_slot, _, _, v_blk = stage_buf.shape
    copies = [pltpu.make_async_copy(src, dst, c_sem.at[i]) for i, (src, dst) in enumerate(((kc, kc_out), (vc, vc_out), (kp, kp_out), (vp, vp_out)))]
    loads = [pltpu.make_async_copy(src, dst, i_sem.at[i]) for i, (src, dst) in enumerate(((fin_in, fin), (kp_in, kp), (vp_in, vp)))]
    low = w_low.shape[1]
    for copy in loads + copies[:2]:
        copy.start()
    for copy in loads:
        copy.wait()
    for copy in copies[2:]:
        copy.start()

    for m in range(micros):
        kept = fin[m // join].astype(F32)
        first = (m % join) * (n_kept - 1)
        last = fin.shape[1] - join + m % join
        for t in range(rows.shape[0]):
            tile = kept[:, t * 128:(t + 1) * 128]
            rows[t, pl.ds(m, n_kept - 1, stride=micros), :] = tile[first:first + n_kept - 1]
            rows[t, (n_kept - 1) * micros + m:(n_kept - 1) * micros + m + 1, :] = tile[last:last + 1]
    lhs = jnp.concatenate([rows[t].astype(BF16) for t in range(rows.shape[0])], axis=1)

    blocks = [(w_low, 0, n, min(v_blk, low - n)) for n in range(0, low, v_blk)]
    blocks += [(w_high, low, n, min(v_blk, vocab - low - n)) for n in range(0, vocab - low, v_blk)]

    def store(i):
        _, base, n, width = blocks[i]
        return pltpu.make_async_copy(
            stage_buf.at[i % n_slot, :, :, pl.ds(0, width)], logits.at[:, :, pl.ds(base + n, width)], l_sem.at[i % n_slot])

    for i, (w_ref, base, n, width) in enumerate(blocks):
        if i >= n_slot:
            store(i - n_slot).wait()
        out = dot(lhs, w_ref[:, n:n + width])
        for r in range(n_kept):
            stage_buf[i % n_slot, r, :, :width] = out[r * micros:(r + 1) * micros]
        store(i).start()
    for i in range(len(blocks) - n_slot, len(blocks)):
        store(i).wait()
    for copy in copies:
        copy.wait()


def solution(mesh):
    n_stages = mesh.shape['stage']
    part_spec = P('replica')
    layer_spec = P('stage')
    cache_spec = P('stage', 'replica')
    in_specs = (part_spec,) * 4 + (layer_spec,) * 9 + (P(), P()) + (cache_spec,) * 4
    out_specs = (part_spec,) + (cache_spec,) * 4

    def device_fn(x_dec, x_pre, dec_len, pre_len, g_attn, w_q, w_k, w_v, w_o, g_mlp, w_gate, w_up, w_down, g_final, w_head, k_dec, v_dec, k_pre, v_pre):
        micros, micro_rows, hidden = x_dec.shape
        n_micro = micros // JOIN
        dec_rows = micro_rows * JOIN
        seg_len = x_pre.shape[1] * JOIN
        x_dec = x_dec.reshape(n_micro, dec_rows, hidden)
        x_pre = x_pre.reshape(n_micro, seg_len, hidden)
        n_rows = dec_rows + seg_len
        _, cache_len, kv_count, head_dim = k_pre.shape
        kv_width = kv_count * head_dim
        q_width = w_q.shape[2]
        ffn = w_gate.shape[2]
        vocab = w_head.shape[1]
        fin_rows = dec_rows + 8

        kd = jnp.transpose(k_dec[0], (0, 1, 3, 4, 2)).reshape(n_micro, dec_rows, kv_width, cache_len)
        vd = jnp.transpose(v_dec[0], (0, 1, 3, 4, 2)).reshape(n_micro, dec_rows, kv_width, cache_len)
        kpre = jnp.transpose(k_pre[0], (1, 2, 0)).reshape(kv_width, cache_len)
        vpre = jnp.transpose(v_pre[0], (1, 2, 0)).reshape(kv_width, cache_len)

        lanes = np.arange(128) % (head_dim // 2)
        inv_freq = jnp.asarray((ROPE_BASE ** (-lanes * (2.0 / head_dim))).astype(np.float32)[None, :])

        def spec(space):
            return pl.BlockSpec(memory_space=space)

        kc, vc, w1, w3, fin, kp, vp = pl.pallas_call(
            functools.partial(pipeline_kernel, n_stages),
            out_shape=(
                VMEM((n_micro, dec_rows, kv_width, cache_len), BF16),
                VMEM((n_micro, dec_rows, kv_width, cache_len), BF16),
                VMEM((hidden, ffn), BF16),
                VMEM((hidden, ffn), BF16),
                pltpu.HBM((n_micro, fin_rows, hidden), BF16),
                pltpu.HBM((kv_width, cache_len), BF16),
                pltpu.HBM((kv_width, cache_len), BF16),
            ),
            in_specs=[spec(SMEM)] * 2 + [spec(HBM)] * 18,
            out_specs=(spec(VMEM),) * 4 + (spec(pltpu.HBM),) * 3,
            scratch_shapes=[
                VMEM((1, 128), F32),
                VMEM((1, hidden), BF16),
                VMEM((1, hidden), BF16),
                VMEM((hidden,), BF16),
                VMEM((hidden, q_width + 2 * kv_width), BF16),
                VMEM((q_width, hidden), BF16),
                VMEM((ffn, hidden), BF16),
                VMEM((kv_width, cache_len), BF16),
                VMEM((kv_width, cache_len), BF16),
                VMEM((n_micro, n_rows, hidden), BF16),
                VMEM((n_micro, fin_rows, hidden), BF16),
                VMEM((dec_rows * 16, 128), F32),
                VMEM((n_micro, dec_rows, kv_width), F32),
                VMEM((n_micro, dec_rows, kv_width), F32),
                VMEM((n_micro, n_rows, 128), F32),
                VMEM((n_micro, n_rows, 128), F32),
                VMEM((ffn // 256 * n_rows, 256), BF16),
                VMEM((q_width // head_dim * seg_len, cache_len), F32),
                pltpu.SemaphoreType.DMA((12,)),
                pltpu.SemaphoreType.DMA((n_micro, 2)),
                pltpu.SemaphoreType.DMA((2,)),
                pltpu.SemaphoreType.DMA((n_micro, 2)),
                pltpu.SemaphoreType.DMA((3,)),
                pltpu.SemaphoreType.DMA((4,)),
                pltpu.SemaphoreType.DMA((n_micro,)),
                pltpu.SemaphoreType.DMA((n_micro,)),
                pltpu.SemaphoreType.DMA((n_micro, n_stages - 1)),
                pltpu.SemaphoreType.DMA((n_micro,)),
                pltpu.SemaphoreType.DMA((n_micro,)),
            ],
            compiler_params=pltpu.CompilerParams(collective_id=0, has_side_effects=True, vmem_limit_bytes=int(R1_MB * 1024 * 1024)),
            name='pipeline',
        )(dec_len, pre_len, *(pltpu.with_memory_space_constraint(arr, pltpu.HBM) for arr in (
              inv_freq, g_attn, g_mlp, g_final, x_dec, x_pre, w_q[0], w_k[0], w_v[0], w_o[0], w_gate[0], w_up[0], w_down[0], kd, vd, kpre, vpre, w_head)))

        v_blk = 512
        n_slot = -(-ffn // v_blk) - (ffn - vocab) // v_blk
        logits, kd_out, vd_out, kp_out, vp_out = pl.pallas_call(
            functools.partial(output_kernel, micros, vocab),
            out_shape=(
                jax.ShapeDtypeStruct((micro_rows + 1, micros, vocab), F32),
                jax.ShapeDtypeStruct(kd.shape, BF16),
                jax.ShapeDtypeStruct(vd.shape, BF16),
                jax.ShapeDtypeStruct(kpre.shape, BF16),
                jax.ShapeDtypeStruct(vpre.shape, BF16),
            ),
            in_specs=[spec(VMEM)] * 4 + [spec(HBM)] * 3,
            out_specs=(spec(HBM),) * 5,
            scratch_shapes=[
                VMEM((n_micro, fin_rows, hidden), BF16),
                VMEM((kv_width, cache_len), BF16),
                VMEM((kv_width, cache_len), BF16),
                VMEM((hidden // 128, (micro_rows + 1) * micros, 128), F32),
                VMEM((n_slot, micro_rows + 1, micros, v_blk), F32),
                pltpu.SemaphoreType.DMA((4,)),
                pltpu.SemaphoreType.DMA((4,)),
                pltpu.SemaphoreType.DMA((n_slot,)),
            ],
            compiler_params=pltpu.CompilerParams(vmem_limit_bytes=7 * 1024 * 1024),
            name='output',
        )(kc, vc, w1, w3, *(pltpu.with_memory_space_constraint(arr, pltpu.HBM) for arr in (fin, kp, vp)))

        def dec_cache(arr):
            return jnp.transpose(arr.reshape(micros, micro_rows, kv_count, head_dim, cache_len), (0, 1, 4, 2, 3))[None]

        def pre_cache(arr):
            return jnp.transpose(arr.reshape(kv_count, head_dim, cache_len), (2, 0, 1))[None]

        return jnp.transpose(logits, (1, 0, 2)), dec_cache(kd_out), dec_cache(vd_out), pre_cache(kp_out), pre_cache(vp_out)

    return jax.shard_map(device_fn, mesh=mesh, in_specs=in_specs, out_specs=out_specs, check_vma=False)
```

```python
import functools

import jax
import jax.numpy as jnp
import numpy as np
from jax import lax
from jax.experimental import pallas as pl
from jax.experimental.pallas import tpu as pltpu
from jax.sharding import PartitionSpec as P

NORM_EPS = 1e-6
ROPE_BASE = 10000.0
F32 = jnp.float32
BF16 = jnp.bfloat16
NEG = -1e30
HBM = pl.ANY
VMEM = pltpu.VMEM
SMEM = pltpu.SMEM
MESH = pl.DeviceIdType.MESH
R1_MB = 21.5
JOIN = 2


def rms_norm(acts, gain):
    acts_f = acts.astype(F32)
    inv_rms = lax.rsqrt(jnp.mean(acts_f * acts_f, axis=-1, keepdims=True) + NORM_EPS)
    return (acts_f * inv_rms * gain.astype(F32)).astype(BF16)


def dot(lhs, rhs):
    return jnp.dot(lhs, rhs, preferred_element_type=F32)


def dot_t(lhs, rhs):
    return lax.dot_general(lhs, rhs, (((1,), (1,)), ((), ())), preferred_element_type=F32)


def softmax(scores):
    expd = jnp.exp(scores - jnp.max(scores, axis=-1, keepdims=True))
    return expd * (1.0 / jnp.sum(expd, axis=-1, keepdims=True))


def pipeline_kernel(
    n_stages,
    dec_len, pre_len, inv_freq_in, g_attn_in, g_mlp_in, g_final_in,
    x_dec, x_pre, w_q, w_k, w_v, w_o, w_gate, w_up, w_down, k_dec, v_dec, k_pre, v_pre, w_head,
    kc, vc, w1, w3, fin_out, kp_out, vp_out,
    inv_freq, g_attn, g_mlp, g_final, wqkv, wo, w2, kp, vp, xin, fin, qd, kn, vn, cosv, sinv, hid, sp,
    w_sem, kv_sem, p_sem, x_sem, o_sem, g_sem, send_sem, recv_sem, fsend_sem, frecv_sem, fnext_sem,
):
    n_micro, n_rows, hidden = xin.shape
    dec_rows = x_dec.shape[1]
    seg_len = x_pre.shape[1]
    per_micro = dec_len.shape[1]
    kv_width, cache_len = kp.shape
    q_width = wo.shape[0]
    ffn = w2.shape[0]
    head_dim = 64
    kv_count = kv_width // head_dim
    q_heads = q_width // head_dim
    group = q_heads // kv_count
    stage = lax.axis_index('stage')
    last = n_stages - 1
    half = ffn // 2
    seg_micro = seg_len * per_micro // dec_rows

    barrier = pltpu.get_barrier_semaphore()

    def x_copies(m):
        return (
            pltpu.make_async_copy(x_dec.at[m], xin.at[m, pl.ds(0, dec_rows)], x_sem.at[m, 0]),
            pltpu.make_async_copy(x_pre.at[m], xin.at[m, pl.ds(dec_rows, seg_len)], x_sem.at[m, 1]),
        )

    def k_copy(m):
        return pltpu.make_async_copy(k_dec.at[m], kc.at[m], kv_sem.at[m, 0])

    def v_copy(m):
        return pltpu.make_async_copy(v_dec.at[m], vc.at[m], kv_sem.at[m, 1])

    qkv_copies = (
        pltpu.make_async_copy(w_q, wqkv.at[:, pl.ds(0, q_width)], w_sem.at[0]),
        pltpu.make_async_copy(w_k, wqkv.at[:, pl.ds(q_width, kv_width)], w_sem.at[1]),
        pltpu.make_async_copy(w_v, wqkv.at[:, pl.ds(q_width + kv_width, kv_width)], w_sem.at[2]),
    )
    pre_copies = (
        pltpu.make_async_copy(k_pre, kp, p_sem.at[0]),
        pltpu.make_async_copy(v_pre, vp, p_sem.at[1]),
    )
    wo_copies = (pltpu.make_async_copy(w_o, wo, w_sem.at[3]),)
    up_copies = tuple(
        (
            pltpu.make_async_copy(w_gate.at[:, pl.ds(i * half, half)], w1.at[:, pl.ds(i * half, half)], w_sem.at[4 + 2 * i]),
            pltpu.make_async_copy(w_up.at[:, pl.ds(i * half, half)], w3.at[:, pl.ds(i * half, half)], w_sem.at[5 + 2 * i]),
        )
        for i in range(2)
    )
    rest = w_head.shape[1] - ffn
    head_copies = (
        pltpu.make_async_copy(w_head.at[:, pl.ds(0, ffn)], w1, w_sem.at[9]),
        pltpu.make_async_copy(w_head.at[:, pl.ds(ffn, rest)], w3.at[:, pl.ds(0, rest)], w_sem.at[10]),
    )
    cut = ffn // 512 * 256 + 256
    down_copies = tuple(
        pltpu.make_async_copy(w_down.at[pl.ds(lo, size)], w2.at[pl.ds(lo, size)], w_sem.at[sem])
        for lo, size, sem in ((0, cut, 8), (cut, ffn - cut, 11)))

    gain_copies = [pltpu.make_async_copy(src, dst, g_sem.at[i]) for i, (src, dst) in enumerate((
        (inv_freq_in, inv_freq), (g_attn_in, g_attn), (g_mlp_in, g_mlp), (g_final_in, g_final)))]
    for copy in gain_copies:
        copy.start()

    @pl.when(stage == 0)
    def _():
        for copy in x_copies(0):
            copy.start()
    for copy in qkv_copies + pre_copies + (k_copy(0),):
        copy.start()
    later = [(v_copy(0),) + wo_copies + up_copies[0], up_copies[1], down_copies, (k_copy(1), v_copy(1)) if n_micro > 1 else ()]
    later[-1] += tuple(copy for m in range(2, n_micro) for copy in (k_copy(m), v_copy(m)))

    def start_later(i):
        for copy in later[i]:
            copy.start()

    @pl.when(stage == 0)
    def _():
        for m in range(1, n_micro):
            for copy in x_copies(m):
                copy.start()

    @pl.when(stage > 0)
    def _():
        for i in range(len(later)):
            start_later(i)

    @pl.when(stage > 0)
    def _():
        pl.semaphore_signal(barrier, inc=1, device_id={'stage': stage - 1}, device_id_type=MESH)

    n_chips = n_stages // 2
    hops = {t: min((last - t) // 2, n_chips - (last - t) // 2) for t in range(1, last, 2)}
    fin_first = sorted(hops, key=lambda t: -hops[t]) + [last - 1]
    passes_on = (stage % 2 == 1) & (stage < last)
    ends_chain = (stage % 2 == 0) & (stage < last - 1)

    @pl.when(ends_chain)
    def _():
        pl.semaphore_signal(barrier, inc=1, device_id={'stage': stage + 1}, device_id_type=MESH)

    @pl.when((stage < last) & jnp.logical_not(ends_chain))
    def _():
        pl.semaphore_signal(barrier, inc=1, device_id={'stage': last}, device_id_type=MESH)

    for copy in gain_copies:
        copy.wait()

    lane = lax.broadcasted_iota(jnp.int32, (8, 128), 1)
    row8 = lax.broadcasted_iota(jnp.int32, (8, 128), 0)
    freq = inv_freq[...]
    sign = jnp.where((lane % head_dim) < head_dim // 2, -1.0, 1.0)

    def table_body(m, carry):
        for g in range(n_rows // 8):
            if g < dec_rows // 8:
                pos = jnp.zeros((8, 128), jnp.int32)
                for r in range(8):
                    pos = jnp.where(row8 == r, dec_len[m * (dec_rows // per_micro) + (g * 8 + r) // per_micro, (g * 8 + r) % per_micro], pos)
            else:
                pos = pre_len[0] + m * seg_len + (g * 8 - dec_rows) + row8
            angle = pos.astype(F32) * freq
            cosv[m, pl.ds(g * 8, 8), :] = jnp.cos(angle)
            sinv[m, pl.ds(g * 8, 8), :] = jnp.sin(angle) * sign
        return carry

    lax.fori_loop(0, n_micro, table_body, 0)
    qd[...] = jnp.zeros(qd.shape, F32)

    @pl.when((stage < last) & jnp.logical_not(passes_on))
    def _():
        pl.semaphore_wait(barrier, 1)

    @pl.when(passes_on)
    def _():
        pl.semaphore_wait(barrier, 2)

    @pl.when(stage == last)
    def _():
        pl.semaphore_wait(barrier, len(fin_first))

    def x_send(m):
        return pltpu.make_async_remote_copy(
            src_ref=xin.at[m], dst_ref=xin.at[m], send_sem=send_sem.at[m], recv_sem=recv_sem.at[m],
            device_id={'stage': jnp.minimum(stage + 1, last)}, device_id_type=MESH)

    def fin_send(m, target):
        return pltpu.make_async_remote_copy(
            src_ref=fin.at[m], dst_ref=fin.at[m], send_sem=fsend_sem.at[m, target], recv_sem=frecv_sem.at[m],
            device_id={'stage': target}, device_id_type=MESH)

    def tick(loading, m, carry):
        def wait_first(copies):
            if loading:
                for copy in copies:
                    copy.wait()

        if loading:
            for copy in x_copies(m):
                copy.wait()
        else:
            @pl.when(stage > 0)
            def _():
                x_send(m).wait_recv()
        wait_first(qkv_copies + pre_copies)
        if loading:
            start_later(0)

        acts = xin[m]
        normed = rms_norm(acts, g_attn[...])
        cosine = cosv[m]
        sine = sinv[m]
        lane_q = lax.broadcasted_iota(jnp.int32, (n_rows, 128), 1)
        low32 = (lane_q % head_dim) < head_dim // 2
        low_half = lax.broadcasted_iota(jnp.int32, (dec_rows, 128), 1) < head_dim

        def rotate(tile):
            swapped = jnp.where(low32, pltpu.roll(tile, 128 - head_dim // 2, 1), pltpu.roll(tile, head_dim // 2, 1))
            return tile * cosine + swapped * sine

        proj = dot(normed, wqkv[...])
        q_tiles = [rotate(proj[:, t * 128:(t + 1) * 128]).astype(BF16).astype(F32) for t in range(q_width // 128)]
        k_new = rotate(proj[:, q_width:q_width + kv_width]).astype(BF16)
        v_new = proj[:, q_width + kv_width:].astype(BF16)
        kn[m] = k_new[:dec_rows].astype(F32)
        vn[m] = v_new[:dec_rows].astype(F32)

        for j in range(q_heads):
            tile = q_tiles[j // 2][:dec_rows]
            if j % 2 != j // group:
                tile = pltpu.roll(tile, head_dim, 1)
            keep = low_half if j // group == 0 else jnp.logical_not(low_half)
            qd[pl.ds(j, dec_rows, stride=16), :] = jnp.where(keep, tile, 0.0)

        pre_begin = pre_len[0] + m * seg_len
        seg_row = lax.broadcasted_iota(jnp.int32, (seg_len, cache_len), 0)
        seg_col = lax.broadcasted_iota(jnp.int32, (seg_len, cache_len), 1)
        spread = (seg_col == seg_row + pre_begin).astype(F32).astype(BF16)
        col = lax.broadcasted_iota(jnp.int32, (kv_width, cache_len), 1)
        written = (col >= pre_begin) & (col < pre_begin + seg_len)
        contract0 = (((0,), (0,)), ((), ()))
        k_put = lax.dot_general(k_new[dec_rows:], spread, contract0, preferred_element_type=F32)
        v_put = lax.dot_general(v_new[dec_rows:], spread, contract0, preferred_element_type=F32)
        kp_f = jnp.where(written, k_put, kp[...].astype(F32)).astype(BF16)
        vp_f = jnp.where(written, v_put, vp[...].astype(F32)).astype(BF16)
        kp[...] = kp_f
        vp[...] = vp_f

        scale = head_dim ** -0.5
        pre_valid = seg_col <= seg_row + pre_begin
        span = group * seg_len
        pd_base = q_heads * seg_len
        for g in range(kv_count):
            rows = []
            for j in range(g * group, (g + 1) * group):
                keep = low_half if j % 2 == 0 else jnp.logical_not(low_half)
                rows.append(jnp.where(keep, q_tiles[j // 2][dec_rows:], 0.0).astype(BF16))
            k_g = kp_f[g * head_dim:(g + 1) * head_dim]
            sp[g * span:(g + 1) * span, :] = dot(jnp.concatenate(rows, axis=0), jnp.concatenate([k_g, k_g], axis=0))

        if loading:
            k_copy(m).wait()
            start_later(1)
        pos_lane = lax.broadcasted_iota(jnp.int32, (16, cache_len), 1)
        for b in range(dec_rows):
            pos = dec_len[m * (dec_rows // per_micro) + b // per_micro, b % per_micro]
            q_b = qd[b * 16:(b + 1) * 16, :]
            s_old = jnp.where(pos_lane < pos, dot(q_b.astype(BF16), kc[m, b]) * scale, NEG)
            s_new = jnp.sum(q_b * kn[m, b:b + 1, :], axis=-1, keepdims=True) * scale
            peak = jnp.maximum(jnp.max(s_old, axis=-1, keepdims=True), s_new)
            expd = jnp.exp(s_old - peak)
            e_new = jnp.exp(s_new - peak)
            inv = 1.0 / (jnp.sum(expd, axis=-1, keepdims=True) + e_new)
            hid[pd_base + b * 16:pd_base + (b + 1) * 16, :] = (expd * inv).astype(BF16)
            p_new = (e_new * inv).astype(BF16).astype(F32)
            qd[b * 16:(b + 1) * 16, :] = p_new * vn[m, b:b + 1, :]

        if loading:
            v_copy(m).wait()
            start_later(2)
        for j in range(q_heads):
            scores = sp[j * seg_len:(j + 1) * seg_len, :] * scale
            hid[j * seg_len:(j + 1) * seg_len, :] = softmax(jnp.where(pre_valid, scores, NEG)).astype(BF16)
        for b in range(dec_rows):
            qd[b * 16:(b + 1) * 16, :] += dot_t(hid[pd_base + b * 16:pd_base + (b + 1) * 16, :], vc[m, b])
        pre_heads = []
        for g in range(kv_count):
            v_g = vp_f[g * head_dim:(g + 1) * head_dim]
            mixed = dot_t(hid[g * span:(g + 1) * span, :], jnp.concatenate([v_g, v_g], axis=0))
            pre_heads += [mixed[i * seg_len:(i + 1) * seg_len] for i in range(group)]


        att_tiles = []
        for t in range(q_width // 128):
            parts = []
            for j in (2 * t, 2 * t + 1):
                part = qd[pl.ds(j, dec_rows, stride=16), :]
                if j % 2 != j // group:
                    part = pltpu.roll(part, head_dim, 1)
                parts.append(part)
            dec_tile = jnp.where(low_half, parts[0], parts[1])
            pre_tile = jnp.where(low_half, pre_heads[2 * t], pre_heads[2 * t + 1])
            att_tiles.append(jnp.concatenate([dec_tile, pre_tile], axis=0).astype(BF16))
        att = jnp.concatenate(att_tiles, axis=1)

        wait_first(wo_copies)

        acts = (acts.astype(F32) + dot(att, wo[...])).astype(BF16)
        normed = rms_norm(acts, g_mlp[...])

        n_blk = 256
        for i in range(2):
            wait_first(up_copies[i])
            if loading and i == 1:
                start_later(3)
            lo = 0 if i == 0 else half // n_blk * n_blk
            hi = half // n_blk * n_blk if i == 0 else ffn
            for n in range(lo, hi, n_blk):
                gate = dot(normed, w1[:, n:n + n_blk])
                up = dot(normed, w3[:, n:n + n_blk])
                k = n // n_blk
                hid[k * n_rows:(k + 1) * n_rows, :] = (jax.nn.silu(gate) * up).astype(BF16)

        def act_blocks(lo, hi):
            return jnp.concatenate([hid[k * n_rows:(k + 1) * n_rows, :] for k in range(lo // n_blk, hi // n_blk)], axis=1)

        if loading:
            wait_first(down_copies[:1])
            down = dot(act_blocks(0, cut), w2[:cut, :])
            wait_first(down_copies[1:])
            down = down + dot(act_blocks(cut, ffn), w2[cut:, :])
        else:
            down = dot(act_blocks(0, ffn), w2[...])
        acts = (acts.astype(F32) + down).astype(BF16)

        def send_rows():
            xin[m] = acts
            x_send(m).start()

        def send_final():
            ends = [acts[dec_rows + e - 8:dec_rows + e].astype(F32) for e in range(seg_micro, seg_len + 1, seg_micro)]
            row = lax.broadcasted_iota(jnp.int32, (8, hidden), 0)
            kept = ends[-1]
            for i, rows in enumerate(ends[:-1]):
                shift = len(ends) - 1 - i
                kept = jnp.where(row == 7 - shift, pltpu.roll(rows, 8 - shift, 0), kept)
            tail = jnp.concatenate([acts[:dec_rows], kept.astype(BF16)], axis=0)
            fin[m] = rms_norm(tail, g_final[...].astype(F32)[None, :])
            for target in fin_first:
                fin_send(m, target).start()

        if loading:
            send_rows()
        else:
            pl.when(stage < last)(send_rows)
            pl.when(stage == last)(send_final)
        return carry

    @pl.when(stage == 0)
    def _():
        tick(True, 0, 0)
        for m in range(1, n_micro):
            for copy in x_copies(m) + (k_copy(m), v_copy(m)):
                copy.wait()

    @pl.when(stage > 0)
    def _():
        for copy in qkv_copies + pre_copies + wo_copies + up_copies[0] + up_copies[1] + down_copies:
            copy.wait()
        for m in range(n_micro):
            k_copy(m).wait()
            v_copy(m).wait()

    lax.fori_loop(jnp.maximum(1 - stage, 0), n_micro, functools.partial(tick, False), 0)

    for copy in head_copies:
        copy.start()

    pre_out = (pltpu.make_async_copy(kp, kp_out, o_sem.at[0]), pltpu.make_async_copy(vp, vp_out, o_sem.at[1]))
    for copy in pre_out:
        copy.start()

    col_full = lax.broadcasted_iota(jnp.int32, (kv_width, cache_len), 1)

    def patch(m, carry):
        for new, cache in ((kn, kc), (vn, vc)):
            cols = jnp.transpose(new[m])
            for b in range(dec_rows):
                pos = dec_len[m * (dec_rows // per_micro) + b // per_micro, b % per_micro]
                column = jnp.broadcast_to(cols[:, b:b + 1], (kv_width, cache_len)).astype(BF16)
                cache[m, b] = jnp.where(col_full == pos, column, cache[m, b])
        return carry

    lax.fori_loop(0, n_micro, patch, 0)

    @pl.when(stage < last)
    def _():
        for m in range(n_micro):
            x_send(m).wait_send()

    def fin_next(m):
        return pltpu.make_async_remote_copy(
            src_ref=fin.at[m], dst_ref=fin.at[m], send_sem=fnext_sem.at[m], recv_sem=frecv_sem.at[m],
            device_id={'stage': jnp.maximum(stage - 1, 0)}, device_id_type=MESH)

    @pl.when(passes_on)
    def _():
        for m in range(n_micro):
            fin_next(m).wait_recv()
            fin_next(m).start()
        for m in range(n_micro):
            fin_next(m).wait_send()

    @pl.when((stage < last) & jnp.logical_not(passes_on))
    def _():
        for m in range(n_micro):
            fin_next(m).wait_recv()

    @pl.when(stage == last)
    def _():
        for m in range(n_micro):
            for target in fin_first:
                fin_send(m, target).wait_send()

    fin_copy = pltpu.make_async_copy(fin, fin_out, o_sem.at[2])
    fin_copy.start()
    for copy in pre_out:
        copy.wait()
    fin_copy.wait()
    for copy in head_copies:
        copy.wait()


def output_kernel(micros, vocab, kc, vc, w_low, w_high, fin_in, kp_in, vp_in, logits, kc_out, vc_out, kp_out, vp_out, fin, kp, vp, rows, stage_buf, i_sem, c_sem, l_sem):
    n_chunk = fin.shape[0]
    n_kept = logits.shape[0]
    join = micros // n_chunk
    n_slot, _, _, v_blk = stage_buf.shape
    copies = [pltpu.make_async_copy(src, dst, c_sem.at[i]) for i, (src, dst) in enumerate(((kc, kc_out), (vc, vc_out), (kp, kp_out), (vp, vp_out)))]
    loads = [pltpu.make_async_copy(src, dst, i_sem.at[i]) for i, (src, dst) in enumerate(((fin_in, fin), (kp_in, kp), (vp_in, vp)))]
    low = w_low.shape[1]
    for copy in loads + copies[:2]:
        copy.start()
    for copy in loads:
        copy.wait()
    for copy in copies[2:]:
        copy.start()

    for m in range(micros):
        kept = fin[m // join].astype(F32)
        first = (m % join) * (n_kept - 1)
        last = fin.shape[1] - join + m % join
        for t in range(rows.shape[0]):
            tile = kept[:, t * 128:(t + 1) * 128]
            rows[t, pl.ds(m, n_kept - 1, stride=micros), :] = tile[first:first + n_kept - 1]
            rows[t, (n_kept - 1) * micros + m:(n_kept - 1) * micros + m + 1, :] = tile[last:last + 1]
    lhs = jnp.concatenate([rows[t].astype(BF16) for t in range(rows.shape[0])], axis=1)

    blocks = [(w_low, 0, n, min(v_blk, low - n)) for n in range(0, low, v_blk)]
    blocks += [(w_high, low, n, min(v_blk, vocab - low - n)) for n in range(0, vocab - low, v_blk)]

    def store(i):
        _, base, n, width = blocks[i]
        return pltpu.make_async_copy(
            stage_buf.at[i % n_slot, :, :, pl.ds(0, width)], logits.at[:, :, pl.ds(base + n, width)], l_sem.at[i % n_slot])

    for i, (w_ref, base, n, width) in enumerate(blocks):
        if i >= n_slot:
            store(i - n_slot).wait()
        out = dot(lhs, w_ref[:, n:n + width])
        for r in range(n_kept):
            stage_buf[i % n_slot, r, :, :width] = out[r * micros:(r + 1) * micros]
        store(i).start()
    for i in range(len(blocks) - n_slot, len(blocks)):
        store(i).wait()
    for copy in copies:
        copy.wait()


def solution(mesh):
    n_stages = mesh.shape['stage']
    part_spec = P('replica')
    layer_spec = P('stage')
    cache_spec = P('stage', 'replica')
    in_specs = (part_spec,) * 4 + (layer_spec,) * 9 + (P(), P()) + (cache_spec,) * 4
    out_specs = (part_spec,) + (cache_spec,) * 4

    def device_fn(x_dec, x_pre, dec_len, pre_len, g_attn, w_q, w_k, w_v, w_o, g_mlp, w_gate, w_up, w_down, g_final, w_head, k_dec, v_dec, k_pre, v_pre):
        micros, micro_rows, hidden = x_dec.shape
        n_micro = micros // JOIN
        dec_rows = micro_rows * JOIN
        seg_len = x_pre.shape[1] * JOIN
        x_dec = x_dec.reshape(n_micro, dec_rows, hidden)
        x_pre = x_pre.reshape(n_micro, seg_len, hidden)
        n_rows = dec_rows + seg_len
        _, cache_len, kv_count, head_dim = k_pre.shape
        kv_width = kv_count * head_dim
        q_width = w_q.shape[2]
        ffn = w_gate.shape[2]
        vocab = w_head.shape[1]
        fin_rows = dec_rows + 8

        kd = jnp.transpose(k_dec[0], (0, 1, 3, 4, 2)).reshape(n_micro, dec_rows, kv_width, cache_len)
        vd = jnp.transpose(v_dec[0], (0, 1, 3, 4, 2)).reshape(n_micro, dec_rows, kv_width, cache_len)
        kpre = jnp.transpose(k_pre[0], (1, 2, 0)).reshape(kv_width, cache_len)
        vpre = jnp.transpose(v_pre[0], (1, 2, 0)).reshape(kv_width, cache_len)

        lanes = np.arange(128) % (head_dim // 2)
        inv_freq = jnp.asarray((ROPE_BASE ** (-lanes * (2.0 / head_dim))).astype(np.float32)[None, :])

        def spec(space):
            return pl.BlockSpec(memory_space=space)

        kc, vc, w1, w3, fin, kp, vp = pl.pallas_call(
            functools.partial(pipeline_kernel, n_stages),
            out_shape=(
                VMEM((n_micro, dec_rows, kv_width, cache_len), BF16),
                VMEM((n_micro, dec_rows, kv_width, cache_len), BF16),
                VMEM((hidden, ffn), BF16),
                VMEM((hidden, ffn), BF16),
                pltpu.HBM((n_micro, fin_rows, hidden), BF16),
                pltpu.HBM((kv_width, cache_len), BF16),
                pltpu.HBM((kv_width, cache_len), BF16),
            ),
            in_specs=[spec(SMEM)] * 2 + [spec(HBM)] * 18,
            out_specs=(spec(VMEM),) * 4 + (spec(pltpu.HBM),) * 3,
            scratch_shapes=[
                VMEM((1, 128), F32),
                VMEM((1, hidden), BF16),
                VMEM((1, hidden), BF16),
                VMEM((hidden,), BF16),
                VMEM((hidden, q_width + 2 * kv_width), BF16),
                VMEM((q_width, hidden), BF16),
                VMEM((ffn, hidden), BF16),
                VMEM((kv_width, cache_len), BF16),
                VMEM((kv_width, cache_len), BF16),
                VMEM((n_micro, n_rows, hidden), BF16),
                VMEM((n_micro, fin_rows, hidden), BF16),
                VMEM((dec_rows * 16, 128), F32),
                VMEM((n_micro, dec_rows, kv_width), F32),
                VMEM((n_micro, dec_rows, kv_width), F32),
                VMEM((n_micro, n_rows, 128), F32),
                VMEM((n_micro, n_rows, 128), F32),
                VMEM((ffn // 256 * n_rows, 256), BF16),
                VMEM((q_width // head_dim * seg_len, cache_len), F32),
                pltpu.SemaphoreType.DMA((12,)),
                pltpu.SemaphoreType.DMA((n_micro, 2)),
                pltpu.SemaphoreType.DMA((2,)),
                pltpu.SemaphoreType.DMA((n_micro, 2)),
                pltpu.SemaphoreType.DMA((3,)),
                pltpu.SemaphoreType.DMA((4,)),
                pltpu.SemaphoreType.DMA((n_micro,)),
                pltpu.SemaphoreType.DMA((n_micro,)),
                pltpu.SemaphoreType.DMA((n_micro, n_stages - 1)),
                pltpu.SemaphoreType.DMA((n_micro,)),
                pltpu.SemaphoreType.DMA((n_micro,)),
            ],
            compiler_params=pltpu.CompilerParams(collective_id=0, has_side_effects=True, vmem_limit_bytes=int(R1_MB * 1024 * 1024)),
            name='pipeline',
        )(dec_len, pre_len, *(pltpu.with_memory_space_constraint(arr, pltpu.HBM) for arr in (
              inv_freq, g_attn, g_mlp, g_final, x_dec, x_pre, w_q[0], w_k[0], w_v[0], w_o[0], w_gate[0], w_up[0], w_down[0], kd, vd, kpre, vpre, w_head)))

        v_blk = 512
        n_slot = -(-ffn // v_blk) - (ffn - vocab) // v_blk
        logits, kd_out, vd_out, kp_out, vp_out = pl.pallas_call(
            functools.partial(output_kernel, micros, vocab),
            out_shape=(
                jax.ShapeDtypeStruct((micro_rows + 1, micros, vocab), F32),
                jax.ShapeDtypeStruct(kd.shape, BF16),
                jax.ShapeDtypeStruct(vd.shape, BF16),
                jax.ShapeDtypeStruct(kpre.shape, BF16),
                jax.ShapeDtypeStruct(vpre.shape, BF16),
            ),
            in_specs=[spec(VMEM)] * 4 + [spec(HBM)] * 3,
            out_specs=(spec(HBM),) * 5,
            scratch_shapes=[
                VMEM((n_micro, fin_rows, hidden), BF16),
                VMEM((kv_width, cache_len), BF16),
                VMEM((kv_width, cache_len), BF16),
                VMEM((hidden // 128, (micro_rows + 1) * micros, 128), F32),
                VMEM((n_slot, micro_rows + 1, micros, v_blk), F32),
                pltpu.SemaphoreType.DMA((4,)),
                pltpu.SemaphoreType.DMA((4,)),
                pltpu.SemaphoreType.DMA((n_slot,)),
            ],
            compiler_params=pltpu.CompilerParams(vmem_limit_bytes=7 * 1024 * 1024),
            name='output',
        )(kc, vc, w1, w3, *(pltpu.with_memory_space_constraint(arr, pltpu.HBM) for arr in (fin, kp, vp)))

        def dec_cache(arr):
            return jnp.transpose(arr.reshape(micros, micro_rows, kv_count, head_dim, cache_len), (0, 1, 4, 2, 3))[None]

        def pre_cache(arr):
            return jnp.transpose(arr.reshape(kv_count, head_dim, cache_len), (2, 0, 1))[None]

        return jnp.transpose(logits, (1, 0, 2)), dec_cache(kd_out), dec_cache(vd_out), pre_cache(kp_out), pre_cache(vp_out)

    return jax.shard_map(device_fn, mesh=mesh, in_specs=in_specs, out_specs=out_specs, check_vma=False)
```
